32 devices in a mesh: grp: 8 (over z, core), dom: 4 (over y, x).
Axes of the slice: x: 2, y: 2, z: 4, core: 2. Of those that a mesh axis runs over, the one named last changes fastest.
Arguments:
- connect: int32 [20, 4096], P(None, ('grp', 'dom')), may hold values from 0 to 511, as said below
- interface_nodes: int32 [32, 4, 32], P(('grp', 'dom')), may hold values from 0 to 511, as said below
- neighbours: int32 [32, 4], P(('grp', 'dom')), may hold values from 0 to 1, as said below
- point_rank: int32 [32, 2048], P(('grp', 'dom')), may hold values from 0 to 2047, each once within a row
- shape_grad: float32 [48, 20], replicated, may hold values from -1.25 to 1.25
- inverse_jacobian: float32 [9, 4096], P(None, ('grp', 'dom')), may hold values from -0.45 to 2.5
- lame_moduli: float32 [2, 4096], P(None, ('grp', 'dom')), may hold values from 0.5 to 2
- point_weights: float32 [16, 4096], P(None, ('grp', 'dom')), may hold values from 0.003 to 0.02
- mass_elem: float32 [20, 4096], P(None, ('grp', 'dom')), may hold values from 0.5 to 2
- source_pattern: float32 [3, 16384], P(None, ('grp', 'dom')), may hold values from -6 to 6
- wavelet: float32 [16], replicated, may hold values from -6 to 6
Outputs:
- strain_db: bfloat16 [16, 6, 65536], P(None, None, ('grp', 'dom'))
The draws below stay inside these ranges and needn't reach their ends.
Inputs may be any that keep to these rules, and one draw needn't show every extreme that they name: `connect`: every one of a partition's 512 nodes is named by some element of that partition. `interface_nodes`: entry i of list k of a partition and entry i of the opposite list of the partition beside it in direction k are copies of one node; no node stands twice among a partition's four lists. `neighbours`: the entry of a partition in direction k equals that of the partition beside it in the opposite direction; it is 0 where no partition lies in direction k.
All inputs are finite; a program needn't handle non-finite values.
Results may differ from the reference program's by a relative error of at most 0.001.
Values may be sent and summed in bfloat16 or wider, within the bound.
A program may use at most 64 MiB of HBM per device.

```python
import math
import jax
import jax.numpy as jnp
from jax import lax

ELEM_DEV = 128
EL_NODES = 20
POINTS = 16
STRAIN = 6
STEPS = 16
NODE_DEV = 512
FACE_NODES = 32
PT_DEV = 2048
GROUPS = 8
WRITERS = 4
PARTS_SIZE = 32
ELEMS = 4096
NODES = 16384


def draw_connect(key, part):
    streams = jax.random.split(key, PARTS_SIZE)

    def one_partition(stream):
        first_key, second_key = jax.random.split(stream)
        shuffled = jax.random.permutation(first_key, EL_NODES * ELEM_DEV)
        filler = jax.random.randint(second_key, (EL_NODES * ELEM_DEV,), 0, NODE_DEV)
        node_ids = jnp.where(shuffled < NODE_DEV, shuffled, filler)
        return node_ids.reshape(EL_NODES, ELEM_DEV).astype(jnp.int32)
    blocks = jax.vmap(one_partition)(streams)
    return blocks.transpose(1, 0, 2).reshape(EL_NODES, PARTS_SIZE * ELEM_DEV)


def draw_interface_nodes(key, part):
    streams = jax.random.split(jax.random.fold_in(key, 11), PARTS_SIZE)

    def pick_lists(stream):
        shuffled = jax.random.permutation(stream, NODE_DEV)
        return shuffled[:4 * FACE_NODES].reshape(4, FACE_NODES).astype(jnp.int32)
    return jax.vmap(pick_lists)(streams)


def draw_neighbours(key, part):
    first_key, second_key = jax.random.split(jax.random.fold_in(key, 23))
    vertical = (jax.random.randint(first_key, (GROUPS, WRITERS), 0, 4) < 3).astype(jnp.int32)
    vertical = vertical * (jnp.arange(GROUPS) < GROUPS - 1).astype(jnp.int32)[:, None]
    lateral = (jax.random.randint(second_key, (GROUPS, WRITERS), 0, 4) < 3).astype(jnp.int32)
    lateral = lateral * (jnp.arange(WRITERS) < WRITERS - 1).astype(jnp.int32)[None, :]
    toward_lower = jnp.concatenate([jnp.zeros((1, WRITERS), jnp.int32), vertical[:-1]], axis=0)
    toward_left = jnp.concatenate([jnp.zeros((GROUPS, 1), jnp.int32), lateral[:, :-1]], axis=1)
    table = jnp.stack([toward_lower, vertical, toward_left, lateral], axis=2)
    return table.reshape(PARTS_SIZE, 4).astype(jnp.int32)


def draw_inverse_jacobian(key, part):
    first_key, second_key = jax.random.split(jax.random.fold_in(key, 37))
    count = PARTS_SIZE * ELEM_DEV
    diagonal = jnp.exp(jax.random.uniform(first_key, (3, count), jnp.float32, -0.5, 0.5))
    shearing = jnp.clip(0.25 * jax.random.normal(second_key, (3, 3, count), jnp.float32), -0.45, 0.45)
    identity = jnp.eye(3, dtype=jnp.float32)
    matrix = shearing * (1.0 - identity)[:, :, None] + identity[:, :, None] * diagonal[:, None, :]
    return matrix.reshape(9, count).astype(jnp.float32)


def level_of(stream_key, extent, shards, smallest, top_value):
    def one(position, shards_of):
        steps = jax.random.uniform(jax.random.fold_in(jax.random.fold_in(stream_key, 6), position), (shards_of,), jnp.float32, smallest / len(shards), top_value / len(shards))
        return jnp.repeat(jnp.exp(steps), extent[position] // shards_of).reshape((-1,) + (1,) * (len(extent) - position - 1))

    gain = one(*shards[0])
    for cut in shards[1:]:
        gain = gain * one(*cut)
    return gain


def gaussian(rng, dims, spread, bound, pieces=(), kind=jnp.bfloat16):
    loudness = level_of(rng, dims, pieces, -0.22, 0.18) if pieces else 1.0
    values = jax.random.normal(rng, dims, jnp.float32) * spread * loudness
    return jnp.minimum(jnp.maximum(values, -bound), bound).astype(kind)


def setup_inputs(seed: int = 0) -> dict:
    arg_keys = jax.random.split(jax.random.key(seed), 12)
    return {
        "connect": draw_connect(jax.random.fold_in(arg_keys[11], 71), 0),
        "interface_nodes": draw_interface_nodes(jax.random.fold_in(arg_keys[11], 71), 0),
        "neighbours": draw_neighbours(jax.random.fold_in(arg_keys[11], 71), 0),
        "point_rank": jax.vmap(lambda own: jax.random.permutation(own, PT_DEV))(jax.random.split(arg_keys[3], PARTS_SIZE)).reshape((PARTS_SIZE, PT_DEV)).astype(jnp.int32),
        "shape_grad": gaussian(arg_keys[4], (3 * POINTS, EL_NODES), EL_NODES ** -0.5, 1.25, (), jnp.float32),
        "inverse_jacobian": draw_inverse_jacobian(jax.random.fold_in(arg_keys[11], 71), 0),
        "lame_moduli": jnp.clip(jnp.exp(math.log(2.0) - 1.3862944 * jax.random.uniform(arg_keys[6], (2, ELEMS), jnp.float32) ** level_of(arg_keys[6], (2, ELEMS), ((1, 32),), -0.2, 0.2)), 0.5, 2.0),
        "point_weights": jnp.clip(jnp.exp(math.log(0.02) - 1.89712 * jax.random.uniform(arg_keys[7], (POINTS, ELEMS), jnp.float32) ** level_of(arg_keys[7], (POINTS, ELEMS), ((1, 32),), -0.2, 0.2)), 0.003, 0.02),
        "mass_elem": jnp.clip(jnp.exp(math.log(2.0) - 1.3862944 * jax.random.uniform(arg_keys[8], (EL_NODES, ELEMS), jnp.float32) ** level_of(arg_keys[8], (EL_NODES, ELEMS), ((1, 32),), -0.2, 0.2)), 0.5, 2.0),
        "source_pattern": gaussian(arg_keys[9], (3, NODES), 1.0, 6.0, ((1, 32),), jnp.float32),
        "wavelet": gaussian(arg_keys[10], (STEPS,), 1.0, 6.0, (), jnp.float32),
    }


time_step = 0.5


def gradient_at(displace, connect, shape_grad, inverse_jacobian):
    elements = connect.shape[1]
    node_values = jnp.take(displace, connect, axis=1)
    along_ref = jnp.einsum('mn,cne->cme', shape_grad, node_values, precision=lax.Precision.HIGHEST)
    along_ref = along_ref.reshape(3, 3, POINTS, elements)
    jacobian = inverse_jacobian.reshape(3, 3, elements)
    result = along_ref[:, 0, None] * jacobian[0][None, :, None, :]
    result = result + along_ref[:, 1, None] * jacobian[1][None, :, None, :]
    result = result + along_ref[:, 2, None] * jacobian[2][None, :, None, :]
    return result


def strain_of(tensor):
    return jnp.stack([tensor[0, 0], tensor[1, 1], tensor[2, 2],
                      0.5 * (tensor[1, 2] + tensor[2, 1]),
                      0.5 * (tensor[0, 2] + tensor[2, 0]),
                      0.5 * (tensor[0, 1] + tensor[1, 0])], axis=0)


def element_forces(tensor, lame_moduli, point_weights, inverse_jacobian, shape_grad, connect, node_count):
    elements = connect.shape[1]
    jacobian = inverse_jacobian.reshape(3, 3, elements)
    volume_change = tensor[0, 0] + tensor[1, 1] + tensor[2, 2]
    identity = jnp.eye(3, dtype=jnp.float32)
    stress = lame_moduli[1][None, None, None, :] * (tensor + tensor.transpose(1, 0, 2, 3))
    stress = stress + identity[:, :, None, None] * (lame_moduli[0][None, :] * volume_change)[None, None]
    mapped = stress[:, 0][:, None] * jacobian[:, 0][None, :, None, :]
    mapped = mapped + stress[:, 1][:, None] * jacobian[:, 1][None, :, None, :]
    mapped = mapped + stress[:, 2][:, None] * jacobian[:, 2][None, :, None, :]
    mapped = mapped * point_weights[None, None]
    node_values = jnp.einsum('mn,cme->cne', shape_grad, mapped.reshape(3, 3 * POINTS, elements),
                             precision=lax.Precision.HIGHEST)
    return jnp.zeros((3, node_count), jnp.float32).at[:, connect].add(node_values)


def split_parts(array, width):
    return array.reshape(array.shape[0], PARTS_SIZE, width).transpose(1, 0, 2)


def assemble_parts(node_field, interface_nodes, neighbours):
    channels = node_field.shape[1]
    picked = jax.vmap(lambda values, shared: jnp.take(values, shared, axis=1))(node_field, interface_nodes)
    picked = picked.reshape(GROUPS, WRITERS, channels, 4, FACE_NODES)
    zero_row = jnp.zeros((1, WRITERS, channels, FACE_NODES), jnp.float32)
    zero_column = jnp.zeros((GROUPS, 1, channels, FACE_NODES), jnp.float32)
    from_below = jnp.concatenate([zero_row, picked[:-1, :, :, 1]], axis=0)
    from_above = jnp.concatenate([picked[1:, :, :, 0], zero_row], axis=0)
    from_left = jnp.concatenate([zero_column, picked[:, :-1, :, 3]], axis=1)
    from_right = jnp.concatenate([picked[:, 1:, :, 2], zero_column], axis=1)
    received = jnp.stack([from_below, from_above, from_left, from_right], axis=3)
    received = received.reshape(PARTS_SIZE, channels, 4, FACE_NODES)
    received = received * neighbours.astype(jnp.float32)[:, None, :, None]
    return jax.vmap(lambda values, shared, incoming: values.at[:, shared].add(incoming))(
        node_field, interface_nodes, received)


def reference(connect, interface_nodes, neighbours, point_rank, shape_grad, inverse_jacobian,
              lame_moduli, point_weights, mass_elem, source_pattern, wavelet):
    connect_parts = split_parts(connect, ELEM_DEV)
    jacobian_parts = split_parts(inverse_jacobian, ELEM_DEV)
    moduli_parts = split_parts(lame_moduli, ELEM_DEV)
    weight_parts = split_parts(point_weights, ELEM_DEV)
    mass_parts = split_parts(mass_elem, ELEM_DEV)
    pattern_parts = split_parts(source_pattern, NODE_DEV)
    node_mass = jax.vmap(lambda connect_part, mass_part: jnp.zeros((1, NODE_DEV), jnp.float32).at[0, connect_part].add(mass_part))(connect_parts, mass_parts)
    inverse_mass = 1.0 / assemble_parts(node_mass, interface_nodes, neighbours)
    gradient_all = jax.vmap(gradient_at, in_axes=(0, 0, None, 0))
    forces_all = jax.vmap(lambda tensor, moduli, weight_part, jacobian_part, connect_part: element_forces(
        tensor, moduli, weight_part, jacobian_part, shape_grad, connect_part, NODE_DEV))

    def advance(loop_state, wave):
        displace, velocity = loop_state
        tensor = gradient_all(displace, connect_parts, shape_grad, jacobian_parts)
        force = wave * pattern_parts - forces_all(tensor, moduli_parts, weight_parts, jacobian_parts, connect_parts)
        force = assemble_parts(force, interface_nodes, neighbours)
        velocity = velocity + time_step * inverse_mass * force
        displace = displace + time_step * velocity
        snapshot = jax.vmap(strain_of)(gradient_all(displace, connect_parts, shape_grad, jacobian_parts))
        snapshot = snapshot.reshape(PARTS_SIZE, STRAIN, PT_DEV).astype(jnp.bfloat16)
        return (displace, velocity), snapshot

    start = jnp.zeros((PARTS_SIZE, 3, NODE_DEV), jnp.float32)
    unused, snapshots = lax.scan(advance, (start, start), wavelet)
    inverse_rank = jax.vmap(lambda ranking: jnp.zeros((PT_DEV,), jnp.int32).at[ranking].set(
        jnp.arange(PT_DEV, dtype=jnp.int32)))(point_rank)
    ordered = jax.vmap(lambda values, positions: jnp.take(values, positions, axis=2),
                       in_axes=(1, 0), out_axes=1)(snapshots, inverse_rank)
    per_writer = PT_DEV // WRITERS
    ordered = ordered.reshape(STEPS, GROUPS, WRITERS, STRAIN, WRITERS, per_writer).transpose(0, 3, 1, 4, 2, 5)
    return ordered.reshape(STEPS, STRAIN, PARTS_SIZE * PT_DEV)
```

```python
import functools

import jax
import jax.numpy as jnp
from jax import lax
from jax.experimental import pallas as pl
from jax.experimental.pallas import tpu as pltpu
from jax.sharding import PartitionSpec as P

MESH = pl.DeviceIdType.MESH
F32 = jnp.float32
BF16 = jnp.bfloat16
time_step = 0.5
LANES = 128


def split(x):
    hi = x.astype(BF16)
    return hi, (x - hi.astype(F32)).astype(BF16)


def pick_lanes(x, idx):
    return jnp.take_along_axis(x, idx, axis=1, mode="promise_in_bounds")


def kernel(
    groups,
    writers,
    steps,
    nodes_el,
    conn_in,
    faces_in,
    nb_in,
    rank_in,
    jac_in,
    lame_in,
    pw_in,
    mass_in,
    src_in,
    gradt_ref,
    wav_ref,
    out_ref,
    conn_ref,
    faces_ref,
    nb_ref,
    rank_ref,
    jac_ref,
    lame_ref,
    pw_ref,
    mass_ref,
    src_ref,
    conn_own,
    faces_own,
    nb_own,
    rank_own,
    jac_own,
    lame_own,
    pw_own,
    mass_own,
    src_own,
    move_sem,
    move_send_sem,
    move_recv_sem,
    onehot,
    hmask,
    perm,
    w1,
    w2,
    snaps,
    lhs,
    ordered,
    send,
    recv,
    send_sem,
    recv_sem,
    out_send_sem,
    out_recv_sem,
):
    my_g = lax.axis_index("grp")
    my_d = lax.axis_index("dom")
    points = pw_ref.shape[0]
    block = out_ref.shape[2] // writers
    blocks = src_ref.shape[1] // LANES

    def along(w):
        if writers % 4:
            return w
        return w + lax.rem(w // 2, 2) * (1 - 2 * lax.rem(w, 2))

    def across(g, w):
        if groups % 2:
            return g
        return g + lax.rem(w, 2) * (1 - 2 * lax.rem(g, 2))

    def host(g, w):
        return across(g, w), along(w)

    d = along(my_d)
    g = across(my_g, d)
    stays = (g == my_g) & (d == my_d)
    moves = jnp.logical_not(stays)
    other_core = g != my_g
    target = host(my_g, my_d)

    has = (g > 0, g < groups - 1, d > 0, d < writers - 1)
    where_to = (host(g - 1, d), host(g + 1, d), host(g, d - 1), host(g, d + 1))

    arrays = (
        (conn_in, conn_own, conn_ref),
        (mass_in, mass_own, mass_ref),
        (faces_in, faces_own, faces_ref),
        (nb_in, nb_own, nb_ref),
        (src_in, src_own, src_ref),
        (jac_in, jac_own, jac_ref),
        (lame_in, lame_own, lame_ref),
        (pw_in, pw_own, pw_ref),
        (rank_in, rank_own, rank_ref),
    )

    def fetch(i, kept):
        return pltpu.make_async_copy(
            arrays[i][0], arrays[i][2 if kept else 1], move_sem.at[i]
        )

    def move(i):
        return pltpu.make_async_remote_copy(
            src_ref=arrays[i][1],
            dst_ref=arrays[i][2],
            send_sem=move_send_sem.at[i],
            recv_sem=move_recv_sem.at[i],
            device_id=target,
            device_id_type=MESH,
        )

    @pl.when(stays)
    def _():
        for i in range(len(arrays)):
            fetch(i, True).start()

    recv[...] = jnp.zeros_like(recv)
    barrier = pltpu.get_barrier_semaphore()

    @pl.when(moves)
    def _():
        for i in range(len(arrays)):
            fetch(i, False).start()
        pl.semaphore_signal(barrier, inc=1, device_id=(g, d), device_id_type=MESH)

    for k in range(4):

        @pl.when(has[k])
        def _():
            pl.semaphore_signal(barrier, inc=1, device_id=where_to[k], device_id_type=MESH)

    for i in range(writers):
        origin_d = lax.rem(my_d + i, writers)
        origin = (across(my_g, along(origin_d)), origin_d)

        def greet():
            pl.semaphore_signal(barrier, inc=1, device_id=origin, device_id_type=MESH)

        if i:
            greet()
        else:
            pl.when(other_core)(greet)

    expected = moves.astype(jnp.int32) + other_core.astype(jnp.int32) + writers - 1
    for k in range(4):
        expected = expected + has[k].astype(jnp.int32)
    pl.semaphore_wait(barrier, expected)

    @pl.when(moves)
    def _():
        for i in range(len(arrays)):
            fetch(i, False).wait()
            move(i).start()

    def landed(lo, hi):
        @pl.when(stays)
        def _():
            for i in range(lo, hi):
                fetch(i, True).wait()

        @pl.when(moves)
        def _():
            for i in range(lo, hi):
                move(i).wait_recv()
                move(i).wait_send()

    landed(0, 5)

    lane = lax.broadcasted_iota(jnp.int32, (LANES, LANES), 1)
    row16 = lax.broadcasted_iota(jnp.int32, (16, LANES), 0)
    faces = faces_ref[0].astype(F32)
    face_row = jnp.concatenate([faces[k : k + 1, :] for k in range(4)], axis=1)
    face_swap = jnp.concatenate([faces[k ^ 1 : (k ^ 1) + 1, :] for k in range(4)], axis=1)
    face_swap = face_swap.astype(jnp.int32)
    face_low = jnp.broadcast_to(jnp.bitwise_and(face_swap, LANES - 1), (8, LANES))
    face_mask = jnp.where(
        jnp.right_shift(face_swap, 7) == jnp.right_shift(row16, 2), 1.0, 0.0
    )
    face_col = jnp.broadcast_to(face_row, (LANES, LANES)).T
    position = lax.broadcasted_iota(jnp.int32, (LANES, LANES), 0).astype(F32)
    inv_rows = []
    has_rows = []
    for b in range(blocks):
        hit = jnp.where(face_col == (lane + b * LANES).astype(F32), 1.0, 0.0)
        inv_rows.append(
            jnp.broadcast_to(jnp.sum(hit * position, axis=0, keepdims=True), (4, LANES))
        )
        has_rows.append(jnp.broadcast_to(jnp.sum(hit, axis=0, keepdims=True), (4, LANES)))
    inv_idx = jnp.concatenate(inv_rows, axis=0).astype(jnp.int32)
    inv_has = jnp.concatenate(has_rows, axis=0)

    conn_low = jnp.bitwise_and(conn_ref[...], LANES - 1)
    conn_high = jnp.right_shift(conn_ref[...], 7)
    columns = jnp.concatenate(
        [conn_low.astype(F32), jnp.zeros((LANES - nodes_el, LANES), F32)], axis=0
    ).T
    for n in range(nodes_el):
        here = jnp.broadcast_to(columns[:, n : n + 1], (LANES, LANES))
        hit = jnp.where(here == lane.astype(F32), 1.0, 0.0)
        onehot[n * LANES : (n + 1) * LANES, 0:LANES] = hit.astype(BF16)
        hit = jnp.where(here == face_low[0:1, :].astype(F32), 1.0, 0.0)
        onehot[n * LANES : (n + 1) * LANES, LANES:] = hit.astype(BF16)
        hmask[n * 16 : (n + 1) * 16, :] = jnp.where(
            conn_high[n : n + 1, :] == jnp.right_shift(row16, 2), 1.0, 0.0
        ).astype(BF16)
    gradt = gradt_ref[...]
    depth = 3 * points
    hi = gradt.astype(BF16).astype(F32)
    lo = gradt - hi
    gap = jnp.zeros((32 - nodes_el, depth), F32)
    tall = jnp.concatenate([hi, gap, hi, gap, lo, gap, jnp.zeros((32, depth), F32)], axis=0)
    tall = jnp.concatenate([tall, jnp.zeros((LANES, LANES - depth), F32)], axis=1)
    w1[...] = tall.T[0:depth, 0:96].astype(BF16)
    wide = jnp.concatenate([hi] * 6 + [lo] * 3, axis=1)
    col = lax.broadcasted_iota(jnp.int32, (8, 9 * depth), 1)
    rows = jnp.bitwise_and(lax.broadcasted_iota(jnp.int32, (8, 9 * depth), 0), 3)
    own = (col >= rows * depth) & (col < (rows + 1) * depth)
    for piece in (3, 6):
        own = own | ((col >= (rows + piece) * depth) & (col < (rows + piece + 1) * depth))
    own = own & (rows < 3)
    for n in range(0, nodes_el, 2):
        two = [jnp.where(own, wide[m : m + 1, :], 0.0) for m in (n, n + 1)]
        w2[n * 8 : n * 8 + 16, :] = jnp.concatenate(two, axis=0).astype(BF16)

    quarter = jnp.right_shift(lax.broadcasted_iota(jnp.int32, (8, LANES), 1), 5)
    nb = nb_ref[...].astype(F32)
    recv_mask = [jnp.where(quarter == k, nb[:, k : k + 1], 0.0) for k in range(4)]

    def copies(slot):
        return [
            pltpu.make_async_remote_copy(
                src_ref=send.at[slot],
                dst_ref=recv.at[slot, k ^ 1],
                send_sem=send_sem.at[slot, k],
                recv_sem=recv_sem.at[slot, k ^ 1],
                device_id=where_to[k],
                device_id_type=MESH,
            )
            for k in range(4)
        ]

    def arrivals(slot):
        return [
            pltpu.make_async_remote_copy(
                src_ref=send.at[slot],
                dst_ref=recv.at[slot, k],
                send_sem=send_sem.at[slot, k],
                recv_sem=recv_sem.at[slot, k],
                device_id=where_to[k],
                device_id_type=MESH,
            )
            for k in range(4)
        ]

    def send_shared(field, slot):
        part = field[:, LANES:] * face_mask
        part = part[0:8] + part[8:16]
        send[slot] = part + pltpu.roll(part, 4, 0)
        for k, copy in enumerate(copies(slot)):

            @pl.when(has[k])
            def _():
                copy.start()

    def shared_sum(slot):
        for k, copy in enumerate(arrivals(slot)):

            @pl.when(has[k])
            def _():
                copy.wait_recv()
                copy.wait_send()

        got = recv[slot, 0] * recv_mask[0]
        for k in range(1, 4):
            got = got + recv[slot, k] * recv_mask[k]
        return got

    def at_nodes(got):
        added = jnp.concatenate(
            [pick_lanes(got, inv_idx[0:8]), pick_lanes(got, inv_idx[8:16])], axis=0
        )
        return added * inv_has

    def scatter(rows):
        pieces = []
        for n in range(nodes_el):
            v = rows(n)
            hi, lo = split(jnp.concatenate([v, v], axis=0))
            mask = hmask[n * 16 : (n + 1) * 16, :]
            pieces.append(jnp.concatenate([hi * mask, lo * mask], axis=0))
        res = jnp.dot(
            jnp.concatenate(pieces, axis=1), onehot[...], preferred_element_type=F32
        )
        return res[0:16] + res[16:32]

    row8 = lax.broadcasted_iota(jnp.int32, (8, LANES), 0)
    mass_row = jnp.bitwise_and(row8, 3) == 3
    mass = scatter(lambda n: jnp.where(mass_row, mass_ref[n : n + 1, :], 0.0))
    src_rows = []
    for b in range(blocks):
        src_rows.append(src_ref[:, b * LANES : (b + 1) * LANES])
        src_rows.append(jnp.zeros((1, LANES), F32))
    source_rows = jnp.concatenate(src_rows, axis=0)
    source_low = jnp.concatenate(
        [pick_lanes(source_rows[i : i + 8], face_low) for i in (0, 8)], axis=0
    )
    first = mass + jnp.concatenate([source_rows, source_low], axis=1)

    send_shared(first, 0)
    landed(5, len(arrays))

    rank_row = lax.broadcasted_iota(jnp.int32, (perm.shape[0], LANES), 0)

    def build_order(q):
        start = pl.multiple_of(q * LANES, LANES)
        perm[:, pl.ds(start, LANES)] = jnp.where(
            rank_ref[:, pl.ds(start, LANES)] == rank_row, 1.0, 0.0
        ).astype(BF16)

    half = steps // 2
    tables = -(-points // half)
    for q in range(min(tables, points)):
        build_order(q)

    first = first[:, 0:LANES] + at_nodes(shared_sum(0))
    axis_row = jnp.bitwise_and(row16, 3) < 3
    source = jnp.where(axis_row, first, 0.0)
    total = jnp.concatenate(
        [jnp.broadcast_to(first[4 * b + 3 : 4 * b + 4, :], (4, LANES)) for b in range(blocks)],
        axis=0,
    )
    half_inverse = jnp.where(axis_row, time_step / total, 0.0)

    spare = jnp.zeros((24 - nodes_el, LANES), jnp.int32)
    conn_low = jnp.concatenate([conn_low, spare], axis=0)
    conn_high = jnp.concatenate([conn_high, spare], axis=0)
    low = [conn_low[8 * i : 8 * i + 8, :] for i in range(3)]
    high = [conn_high[8 * i : 8 * i + 8, :] for i in range(3)]

    def at_elements(rows_of):
        out = []
        for i in range(3):
            acc = None
            for b in range(blocks):
                val = pick_lanes(jnp.broadcast_to(rows_of(b), (8, LANES)), low[i])
                acc = val if b == 0 else jnp.where(high[i] == b, val, acc)
            out.append(acc)
        return out

    inv_f = inv_idx.astype(F32)
    place = [x.astype(jnp.int32) for x in at_elements(lambda b: inv_f[4 * b : 4 * b + 1, :])]
    coef = (-time_step) * half_inverse * inv_has
    coef = at_elements(lambda b: coef[4 * b : 4 * b + 1, :])

    def gather(u):
        return tuple(
            tuple(at_elements(lambda b: u[4 * b + c : 4 * b + c + 1, :])) for c in range(3)
        )

    def corrected(values, got):
        out = []
        for c in range(3):
            row = jnp.broadcast_to(got[c : c + 1, :], (8, LANES))
            out.append(
                tuple(values[c][i] + pick_lanes(row, place[i]) * coef[i] for i in range(3))
            )
        return tuple(out)

    def gradient(values):
        sides = []
        for c in range(3):
            rows = list(values[c]) + [jnp.zeros((8, LANES), F32)]
            hi, lo = split(jnp.concatenate(rows, axis=0))
            sides.append(jnp.concatenate([hi, lo, hi], axis=0))
        along = jnp.dot(
            w1[...], jnp.concatenate(sides, axis=1), preferred_element_type=F32
        )
        tensor = []
        for c in range(3):
            ref_dir = [
                along[r * points : (r + 1) * points, c * LANES : (c + 1) * LANES]
                for r in range(3)
            ]
            tensor.append(
                [
                    ref_dir[0] * jac_ref[e : e + 1, :]
                    + ref_dir[1] * jac_ref[3 + e : 4 + e, :]
                    + ref_dir[2] * jac_ref[6 + e : 7 + e, :]
                    for e in range(3)
                ]
            )
        return tensor

    def internal_force(t):
        lam = lame_ref[0:1, :]
        mu = lame_ref[1:2, :]
        pressure = lam * (t[0][0] + t[1][1] + t[2][2])
        stress = [[None] * 3 for _ in range(3)]
        for c in range(3):
            for e in range(c, 3):
                s = mu * (t[c][e] + t[e][c])
                if c == e:
                    s = s + pressure
                stress[c][e] = s
                stress[e][c] = s
        weight = pw_ref[...]
        highs = []
        lows = []
        for c in range(3):
            for r in range(3):
                m = stress[c][0] * jac_ref[3 * r : 3 * r + 1, :]
                m = m + stress[c][1] * jac_ref[3 * r + 1 : 3 * r + 2, :]
                m = m + stress[c][2] * jac_ref[3 * r + 2 : 3 * r + 3, :]
                hi, lo = split(m * weight)
                highs.append(hi)
                lows.append(lo)
        side = jnp.concatenate(highs + lows + highs, axis=0)
        values = jnp.dot(w2[...], side, preferred_element_type=F32)
        return scatter(lambda n: values[8 * n : 8 * n + 8, :])

    def record(t, slot_index):
        comps = [
            t[0][0],
            t[1][1],
            t[2][2],
            0.5 * (t[1][2] + t[2][1]),
            0.5 * (t[0][2] + t[2][0]),
            0.5 * (t[0][1] + t[1][0]),
        ]
        for c, value in enumerate(comps):
            start = (slot_index // half) * 6 + c
            start = pl.multiple_of((start * half + lax.rem(slot_index, half)) * points, points)
            snaps[pl.ds(start, points), :] = value

    velocity = wav_ref[0] * source * half_inverse
    displace = time_step * velocity

    def order_for(w):
        start = pl.multiple_of(w * block, block)
        res = lax.dot_general(
            lhs[...],
            perm[pl.ds(start, block), :],
            (((1,), (1,)), ((), ())),
            preferred_element_type=F32,
        )
        return res.astype(BF16).reshape(6, half, block)

    def mine(i):
        return pl.ds(pl.multiple_of(i * block, block), block)

    def parcel(h, i, column, target):
        return pltpu.make_async_remote_copy(
            src_ref=ordered.at[h, i],
            dst_ref=out_ref.at[:, h * half : (h + 1) * half, mine(column)],
            send_sem=out_send_sem.at[h, i],
            recv_sem=out_recv_sem.at[h, i],
            device_id=(g, target),
            device_id_type=MESH,
        )

    def arriving(h, i):
        origin = lax.rem(my_d - i + writers, writers)
        return parcel(h, i, along(origin), origin)

    def ship(h):
        count = 6 * half
        for q in range(points):
            lhs[:, q * LANES : (q + 1) * LANES] = snaps[
                pl.ds(h * count * points + q, count, stride=points), :
            ].astype(BF16)
        for i in range(1, writers):
            w = lax.rem(my_d + i, writers)
            ordered[h, i] = order_for(w)
            parcel(h, i, d, w).start()
        last = order_for(my_d)

        @pl.when(other_core)
        def _():
            ordered[h, 0] = last
            parcel(h, 0, d, my_d).start()

        @pl.when(jnp.logical_not(other_core))
        def _():
            out_ref[:, h * half : (h + 1) * half, mine(d)] = last

    def advance(t, state, extra):
        values, displace, velocity = state
        slot = lax.rem(t, 2)
        tensor = gradient(values)
        inner = internal_force(tensor)
        send_shared(inner, slot)
        velocity = velocity + half_inverse * (wav_ref[t] * source - inner[:, 0:LANES])
        displace = displace + time_step * velocity
        values = gather(displace)
        record(tensor, t - 1)
        extra(t)
        got = shared_sum(slot)
        values = corrected(values, got)
        change = half_inverse * at_nodes(got)
        return values, displace - time_step * change, velocity - change

    def early(t, state):
        def extra(t):
            for i in range(tables):
                build_order(jnp.minimum(t * tables + i, points - 1))

        return advance(t, state, extra)

    state = (gather(displace), displace, velocity)
    state = lax.fori_loop(1, half, early, state)
    state = advance(jnp.int32(half), state, lambda t: ship(0))
    state = lax.fori_loop(
        half + 1, steps, lambda t, held: advance(t, held, lambda t: None), state
    )
    record(gradient(state[0]), jnp.int32(steps - 1))
    ship(1)
    for h in range(2):
        for i in range(1, writers):
            arriving(h, i).wait_recv()
            parcel(h, i, d, lax.rem(my_d + i, writers)).wait_send()

        @pl.when(other_core)
        def _():
            arriving(h, 0).wait_recv()
            parcel(h, 0, d, my_d).wait_send()


def solution(mesh):
    groups, writers = mesh.shape["grp"], mesh.shape["dom"]

    def shards(
        connect,
        interface_nodes,
        neighbours,
        point_rank,
        shape_grad,
        inverse_jacobian,
        lame_moduli,
        point_weights,
        mass_elem,
        source_pattern,
        wavelet,
    ):
        nodes_el, elements = connect.shape
        points = point_weights.shape[0]
        point_count = point_rank.shape[1]
        steps = wavelet.shape[0]
        vmem = pl.BlockSpec(memory_space=pltpu.VMEM)
        smem = pl.BlockSpec(memory_space=pltpu.SMEM)
        hbm = pl.BlockSpec(memory_space=pl.ANY)
        sharded = (
            connect,
            interface_nodes,
            neighbours,
            point_rank,
            inverse_jacobian,
            lame_moduli,
            point_weights,
            mass_elem,
            source_pattern,
        )
        ordered = pl.pallas_call(
            functools.partial(kernel, groups, writers, steps, nodes_el),
            out_shape=jax.ShapeDtypeStruct((6, steps, point_count), BF16),
            in_specs=[hbm] * len(sharded) + [vmem, smem],
            out_specs=vmem,
            scratch_shapes=[pltpu.VMEM(a.shape, a.dtype) for a in sharded] * 2
            + [pltpu.SemaphoreType.DMA((len(sharded),))] * 3
            + [
                pltpu.VMEM((nodes_el * LANES, 2 * LANES), BF16),
                pltpu.VMEM((nodes_el * 16, LANES), BF16),
                pltpu.VMEM((point_count, point_count), BF16),
                pltpu.VMEM((3 * points, 96), BF16),
                pltpu.VMEM((nodes_el * 8, 27 * points), BF16),
                pltpu.VMEM((steps * 6 * points, LANES), F32),
                pltpu.VMEM((steps // 2 * 6, point_count), BF16),
                pltpu.VMEM((2, writers, 6, steps // 2, point_count // writers), BF16),
                pltpu.VMEM((2, 8, LANES), F32),
                pltpu.VMEM((2, 4, 8, LANES), F32),
                pltpu.SemaphoreType.DMA((2, 4)),
                pltpu.SemaphoreType.DMA((2, 4)),
                pltpu.SemaphoreType.DMA((2, writers)),
                pltpu.SemaphoreType.DMA((2, writers)),
            ],
            compiler_params=pltpu.CompilerParams(
                collective_id=0, has_side_effects=True, vmem_limit_bytes=56 * 1024 * 1024
            ),
            name="window",
        )(
            *sharded,
            shape_grad.T,
            wavelet,
        )
        return ordered.transpose(1, 0, 2)

    placed = (
        P(None, ("grp", "dom")),
        P(("grp", "dom"), None, None),
        P(("grp", "dom"), None),
        P(("grp", "dom"), None),
        P(),
        P(None, ("grp", "dom")),
        P(None, ("grp", "dom")),
        P(None, ("grp", "dom")),
        P(None, ("grp", "dom")),
        P(None, ("grp", "dom")),
        P(),
    )
    return jax.shard_map(
        shards, mesh=mesh, in_specs=placed, out_specs=P(None, None, ("grp", "dom")), check_vma=False
    )
```

```python
import functools

import jax
import jax.numpy as jnp
from jax import lax
from jax.experimental import pallas as pl
from jax.experimental.pallas import tpu as pltpu
from jax.sharding import PartitionSpec as P

MESH = pl.DeviceIdType.MESH
F32 = jnp.float32
BF16 = jnp.bfloat16
time_step = 0.5
LANES = 128


def split(x):
    hi = x.astype(BF16)
    return hi, (x - hi.astype(F32)).astype(BF16)


def pick_lanes(x, idx):
    return jnp.take_along_axis(x, idx, axis=1, mode="promise_in_bounds")


def kernel(
    groups,
    writers,
    steps,
    nodes_el,
    conn_in,
    faces_in,
    nb_in,
    rank_in,
    jac_in,
    lame_in,
    pw_in,
    mass_in,
    src_in,
    gradt_ref,
    wav_ref,
    out_ref,
    conn_ref,
    faces_ref,
    nb_ref,
    rank_ref,
    jac_ref,
    lame_ref,
    pw_ref,
    mass_ref,
    src_ref,
    conn_own,
    faces_own,
    nb_own,
    rank_own,
    jac_own,
    lame_own,
    pw_own,
    mass_own,
    src_own,
    move_sem,
    move_send_sem,
    move_recv_sem,
    at_face,
    at_node,
    hmask,
    basis,
    products,
    pww,
    kmat,
    at_el,
    perm,
    w1,
    snaps,
    lhs,
    ordered,
    send,
    recv,
    send_sem,
    recv_sem,
    out_send_sem,
    out_recv_sem,
):
    my_g = lax.axis_index("grp")
    my_d = lax.axis_index("dom")
    points = pw_ref.shape[0]
    block = out_ref.shape[2] // writers
    blocks = src_ref.shape[1] // LANES

    def along(w):
        if writers % 4:
            return w
        return w + lax.rem(w // 2, 2) * (1 - 2 * lax.rem(w, 2))

    def across(g, w):
        if groups % 2:
            return g
        return g + lax.rem(w, 2) * (1 - 2 * lax.rem(g, 2))

    def host(g, w):
        return across(g, w), along(w)

    d = along(my_d)
    g = across(my_g, d)
    stays = (g == my_g) & (d == my_d)
    moves = jnp.logical_not(stays)
    other_core = g != my_g
    target = host(my_g, my_d)

    has = (g > 0, g < groups - 1, d > 0, d < writers - 1)
    where_to = (host(g - 1, d), host(g + 1, d), host(g, d - 1), host(g, d + 1))

    arrays = (
        (conn_in, conn_own, conn_ref),
        (mass_in, mass_own, mass_ref),
        (faces_in, faces_own, faces_ref),
        (nb_in, nb_own, nb_ref),
        (src_in, src_own, src_ref),
        (jac_in, jac_own, jac_ref),
        (lame_in, lame_own, lame_ref),
        (pw_in, pw_own, pw_ref),
        (rank_in, rank_own, rank_ref),
    )

    def fetch(i, kept):
        return pltpu.make_async_copy(
            arrays[i][0], arrays[i][2 if kept else 1], move_sem.at[i]
        )

    def move(i):
        return pltpu.make_async_remote_copy(
            src_ref=arrays[i][1],
            dst_ref=arrays[i][2],
            send_sem=move_send_sem.at[i],
            recv_sem=move_recv_sem.at[i],
            device_id=target,
            device_id_type=MESH,
        )

    @pl.when(stays)
    def _():
        for i in range(len(arrays)):
            fetch(i, True).start()

    recv[...] = jnp.zeros_like(recv)
    barrier = pltpu.get_barrier_semaphore()

    @pl.when(moves)
    def _():
        for i in range(len(arrays)):
            fetch(i, False).start()
        pl.semaphore_signal(barrier, inc=1, device_id=(g, d), device_id_type=MESH)

    for k in range(4):

        @pl.when(has[k])
        def _():
            pl.semaphore_signal(barrier, inc=1, device_id=where_to[k], device_id_type=MESH)

    for i in range(writers):
        origin_d = lax.rem(my_d + i, writers)
        origin = (across(my_g, along(origin_d)), origin_d)

        def greet():
            pl.semaphore_signal(barrier, inc=1, device_id=origin, device_id_type=MESH)

        if i:
            greet()
        else:
            pl.when(other_core)(greet)

    expected = moves.astype(jnp.int32) + other_core.astype(jnp.int32) + writers - 1
    for k in range(4):
        expected = expected + has[k].astype(jnp.int32)
    pl.semaphore_wait(barrier, expected)

    @pl.when(moves)
    def _():
        for i in range(len(arrays)):
            fetch(i, False).wait()
            move(i).start()

    def landed(lo, hi):
        @pl.when(stays)
        def _():
            for i in range(lo, hi):
                fetch(i, True).wait()

        @pl.when(moves)
        def _():
            for i in range(lo, hi):
                move(i).wait_recv()
                move(i).wait_send()


    lane = lax.broadcasted_iota(jnp.int32, (LANES, LANES), 1)
    row8 = lax.broadcasted_iota(jnp.int32, (8, LANES), 0)
    row16 = lax.broadcasted_iota(jnp.int32, (16, LANES), 0)
    pairs_el = nodes_el // 2
    padded = -(-nodes_el // 8) * 8
    tiles = padded // 8

    gradt = gradt_ref[...]
    depth = 3 * points
    hi = gradt.astype(BF16).astype(F32)
    lo = gradt - hi
    gap = jnp.zeros((32 - nodes_el, depth), F32)
    tall = jnp.concatenate([hi, gap, hi, gap, lo, gap, jnp.zeros((32, depth), F32)], axis=0)
    tall = jnp.concatenate([tall, jnp.zeros((LANES, LANES - depth), F32)], axis=1)
    w1[...] = tall.T[0:depth, 0:96].astype(BF16)

    lanes = lax.broadcasted_iota(jnp.int32, (padded, LANES), 1)
    base = jnp.concatenate([gradt, jnp.zeros((padded - nodes_el, depth), F32)], axis=0)
    base = jnp.concatenate([base, jnp.zeros((padded, LANES - depth), F32)], axis=1)
    own_dir = []
    for r in range(3):
        x = pltpu.roll(base, LANES - r * points, 1) if r else base
        x = jnp.where(lanes < points, x, 0.0)
        x = x + pltpu.roll(x, points, 1) + pltpu.roll(x, 2 * points, 1)
        own_dir.append(x)
        basis[r] = x

    def multiply_pairs(m, carry):
        for rp in range(3):
            parts = []
            for p in range(2):
                other = basis[rp, pl.ds(2 * m + p, 1), :]
                for r in range(3):
                    product = own_dir[r] * other
                    high = product.astype(BF16).astype(F32)
                    parts.append(jnp.where(lanes < 2 * points, high, product - high))
            rows = 6 * padded
            products[m, rp * rows : (rp + 1) * rows, :] = jnp.concatenate(
                parts, axis=0
            ).astype(BF16)
        return carry

    lax.fori_loop(0, pairs_el, multiply_pairs, 0)

    def clear(m, carry):
        kmat[m] = jnp.zeros(kmat.shape[1:], F32)
        return carry

    lax.fori_loop(0, pairs_el, clear, 0)

    landed(0, 5)
    faces = faces_ref[0].astype(F32)
    face_row = jnp.concatenate([faces[k : k + 1, :] for k in range(4)], axis=1)
    face_swap = jnp.concatenate([faces[k ^ 1 : (k ^ 1) + 1, :] for k in range(4)], axis=1)
    face_swap = jnp.broadcast_to(face_swap.astype(jnp.int32), (LANES, LANES))
    face_low = jnp.bitwise_and(face_swap[0:8], LANES - 1)
    face_high = jnp.right_shift(face_swap[0:8], 7)

    columns = jnp.concatenate(
        [conn_ref[...].astype(F32), jnp.zeros((LANES - nodes_el, LANES), F32)], axis=0
    ).T.astype(jnp.int32)

    def column(n):
        return jnp.broadcast_to(columns[:, n : n + 1], (LANES, LANES))

    def spot(n):
        j, p = n // 2, n % 2
        return slice(j * LANES, (j + 1) * LANES), slice(p * LANES, (p + 1) * LANES)

    for n in range(nodes_el):
        at_face[spot(n)] = jnp.where(column(n) == face_swap, 1.0, 0.0).astype(BF16)

    def pack(x):
        high = x.astype(BF16).astype(F32)
        return jnp.concatenate([high, x - high], axis=0).astype(BF16)

    def face_forces(packs):
        res = jnp.dot(
            jnp.concatenate(packs, axis=1), at_face[...], preferred_element_type=F32
        )
        res = res[0:8] + res[8:16]
        mixed = jnp.where(row8 < 4, res[:, 0:LANES], res[:, LANES:])
        return mixed + pltpu.roll(mixed, 4, 0)

    def node_forces(packs):
        sides = []
        for b in range(blocks):
            sides.append(
                jnp.concatenate(
                    [
                        packs[j] * hmask[(j * blocks + b) * 16 : (j * blocks + b + 1) * 16, :]
                        for j in range(pairs_el)
                    ],
                    axis=1,
                )
            )
        res = jnp.dot(
            jnp.concatenate(sides, axis=0), at_node[...], preferred_element_type=F32
        )
        halves = []
        for b in range(blocks):
            one = res[16 * b : 16 * b + 8] + res[16 * b + 8 : 16 * b + 16]
            even, odd = one[:, 0:LANES], one[:, LANES:]
            if b % 2:
                halves.append(pltpu.roll(even, 4, 0) + odd)
            else:
                halves.append(even + pltpu.roll(odd, 4, 0))
        return jnp.concatenate(
            [jnp.where(row8 < 4, halves[b], halves[b + 1]) for b in range(0, blocks, 2)],
            axis=0,
        )

    quarter = jnp.right_shift(lax.broadcasted_iota(jnp.int32, (8, LANES), 1), 5)
    nb = nb_ref[...].astype(F32)
    recv_mask = [jnp.where(quarter == k, nb[:, k : k + 1], 0.0) for k in range(4)]

    def copies(slot):
        return [
            pltpu.make_async_remote_copy(
                src_ref=send.at[slot, 0:4],
                dst_ref=recv.at[slot, k ^ 1, 0:4],
                send_sem=send_sem.at[slot, k],
                recv_sem=recv_sem.at[slot, k ^ 1],
                device_id=where_to[k],
                device_id_type=MESH,
            )
            for k in range(4)
        ]

    def arrivals(slot):
        return [
            pltpu.make_async_remote_copy(
                src_ref=send.at[slot, 0:4],
                dst_ref=recv.at[slot, k, 0:4],
                send_sem=send_sem.at[slot, k],
                recv_sem=recv_sem.at[slot, k],
                device_id=where_to[k],
                device_id_type=MESH,
            )
            for k in range(4)
        ]

    def send_shared(message, slot):
        send[slot] = message
        for k, copy in enumerate(copies(slot)):

            @pl.when(has[k])
            def _():
                copy.start()

    def shared_sum(slot):
        for k, copy in enumerate(arrivals(slot)):

            @pl.when(has[k])
            def _():
                copy.wait_recv()
                copy.wait_send()

        got = recv[slot, 0] * recv_mask[0]
        for k in range(1, 4):
            got = got + recv[slot, k] * recv_mask[k]
        return got

    masses = []
    for n in range(0, nodes_el, 2):
        mass = jnp.where(row8 == 3, mass_ref[n : n + 1, :], 0.0)
        masses.append(pack(mass + jnp.where(row8 == 7, mass_ref[n + 1 : n + 2, :], 0.0)))
    src_rows = []
    for b in range(blocks):
        src_rows.append(src_ref[:, b * LANES : (b + 1) * LANES])
        src_rows.append(jnp.zeros((1, LANES), F32))
    at_faces = jnp.zeros((8, LANES), F32)
    for b in range(blocks):
        rows = jnp.concatenate([src_rows[2 * b], jnp.zeros((5, LANES), F32)], axis=0)
        at_faces = jnp.where(face_high == b, pick_lanes(rows, face_low), at_faces)
    send_shared(face_forces(masses) + at_faces, 0)

    conn_low = jnp.bitwise_and(conn_ref[...], LANES - 1)
    conn_high = jnp.right_shift(conn_ref[...], 7)
    for n in range(nodes_el):
        low_column = jnp.bitwise_and(column(n), LANES - 1)
        at_node[spot(n)] = jnp.where(low_column == lane, 1.0, 0.0).astype(BF16)
    for j in range(pairs_el):
        two = [
            jnp.broadcast_to(conn_high[n : n + 1, :], (4, LANES)) for n in (2 * j, 2 * j + 1)
        ]
        two = jnp.concatenate(two * 2, axis=0)
        for b in range(blocks):
            hmask[(j * blocks + b) * 16 : (j * blocks + b + 1) * 16, :] = jnp.where(
                two == b, 1.0, 0.0
            ).astype(BF16)
    first = node_forces(masses) + jnp.concatenate(src_rows, axis=0)

    face_col = jnp.broadcast_to(face_row, (LANES, LANES)).T
    position = lax.broadcasted_iota(jnp.int32, (LANES, LANES), 0).astype(F32)
    inv_rows = []
    has_rows = []
    for b in range(blocks):
        hit = jnp.where(face_col == (lane + b * LANES).astype(F32), 1.0, 0.0)
        inv_rows.append(
            jnp.broadcast_to(jnp.sum(hit * position, axis=0, keepdims=True), (4, LANES))
        )
        has_rows.append(jnp.broadcast_to(jnp.sum(hit, axis=0, keepdims=True), (4, LANES)))
    inv_idx = jnp.concatenate(inv_rows, axis=0).astype(jnp.int32)
    inv_has = jnp.concatenate(has_rows, axis=0)

    def at_nodes(got):
        got = got + pltpu.roll(got, 4, 0)
        added = jnp.concatenate(
            [pick_lanes(got, inv_idx[0:8]), pick_lanes(got, inv_idx[8:16])], axis=0
        )
        return added * inv_has

    landed(5, len(arrays))
    weight = pw_ref[...]
    hi = weight.astype(BF16).astype(F32)
    pww[...] = jnp.concatenate(
        [hi, weight - hi, hi, jnp.zeros((LANES - depth, LANES), F32)], axis=0
    ).astype(BF16)
    jac = [jnp.broadcast_to(jac_ref[i : i + 1, :], (8, LANES)) for i in range(9)]
    lam = jnp.broadcast_to(lame_ref[0:1, :], (8, LANES))
    mu = jnp.broadcast_to(lame_ref[1:2, :], (8, LANES))

    def form_stiffness(m, carry):
        moments = jnp.dot(products[m], pww[...], preferred_element_type=F32)
        for p in range(2):
            for i in range(tiles):

                def moment(r, rp):
                    start = ((rp * 2 + p) * 3 + r) * padded + 8 * i
                    return moments[start : start + 8]

                half = [
                    [
                        jac[a] * moment(0, rp) + jac[3 + a] * moment(1, rp) + jac[6 + a] * moment(2, rp)
                        for rp in range(3)
                    ]
                    for a in range(3)
                ]
                full = [
                    [
                        jac[b] * half[a][0] + jac[3 + b] * half[a][1] + jac[6 + b] * half[a][2]
                        for b in range(3)
                    ]
                    for a in range(3)
                ]
                trace = mu * (full[0][0] + full[1][1] + full[2][2])
                for c in range(3):
                    for cp in range(3):
                        value = mu * full[cp][c] + lam * full[c][cp]
                        if c == cp:
                            value = value + trace
                        start = (p * 3 + cp) * 4 * padded + 32 * i + c
                        kmat[m, pl.ds(start, 8, stride=4), :] = value
        return carry

    lax.fori_loop(0, pairs_el, form_stiffness, 0)

    rank_row = lax.broadcasted_iota(jnp.int32, (perm.shape[0], LANES), 0)

    def build_order(q):
        start = pl.multiple_of(q * LANES, LANES)
        perm[:, pl.ds(start, LANES)] = jnp.where(
            rank_ref[:, pl.ds(start, LANES)] == rank_row, 1.0, 0.0
        ).astype(BF16)

    half = steps // 2
    tables = -(-points // half)
    for q in range(min(tables, points)):
        build_order(q)

    first = first + at_nodes(shared_sum(0))
    axis_row = jnp.bitwise_and(row16, 3) < 3
    source = jnp.where(axis_row, first, 0.0)
    total = jnp.concatenate(
        [jnp.broadcast_to(first[4 * b + 3 : 4 * b + 4, :], (4, LANES)) for b in range(blocks)],
        axis=0,
    )
    half_inverse = jnp.where(axis_row, time_step / total, 0.0)

    spare = jnp.zeros((24 - nodes_el, LANES), jnp.int32)
    conn_low = jnp.concatenate([conn_low, spare], axis=0)
    conn_high = jnp.concatenate([conn_high, spare], axis=0)
    low = [conn_low[8 * i : 8 * i + 8, :] for i in range(3)]
    high = [conn_high[8 * i : 8 * i + 8, :] for i in range(3)]

    def at_elements(rows_of):
        out = []
        for i in range(3):
            acc = None
            for b in range(blocks):
                val = pick_lanes(jnp.broadcast_to(rows_of(b), (8, LANES)), low[i])
                acc = val if b == 0 else jnp.where(high[i] == b, val, acc)
            out.append(acc)
        return out

    inv_f = inv_idx.astype(F32)
    place = [x.astype(jnp.int32) for x in at_elements(lambda b: inv_f[4 * b : 4 * b + 1, :])]
    coef = (-time_step) * half_inverse * inv_has
    coef = at_elements(lambda b: coef[4 * b : 4 * b + 1, :])

    def gather(u):
        return tuple(
            tuple(at_elements(lambda b: u[4 * b + c : 4 * b + c + 1, :])) for c in range(3)
        )

    def corrected(values, got):
        out = []
        for c in range(3):
            row = jnp.broadcast_to(got[c : c + 1, :], (8, LANES))
            out.append(
                tuple(values[c][i] + pick_lanes(row, place[i]) * coef[i] for i in range(3))
            )
        return tuple(out)

    def gradient(values):
        sides = []
        for c in range(3):
            rows = list(values[c]) + [jnp.zeros((8, LANES), F32)]
            hi, lo = split(jnp.concatenate(rows, axis=0))
            sides.append(jnp.concatenate([hi, lo, hi], axis=0))
        along = jnp.dot(
            w1[...], jnp.concatenate(sides, axis=1), preferred_element_type=F32
        )
        tensor = []
        for c in range(3):
            ref_dir = [
                along[r * points : (r + 1) * points, c * LANES : (c + 1) * LANES]
                for r in range(3)
            ]
            tensor.append(
                [
                    ref_dir[0] * jac_ref[e : e + 1, :]
                    + ref_dir[1] * jac_ref[3 + e : 4 + e, :]
                    + ref_dir[2] * jac_ref[6 + e : 7 + e, :]
                    for e in range(3)
                ]
            )
        return tensor

    def stiffness(values):
        for c in range(3):
            for i in range(tiles):
                start = c * padded + 8 * i
                at_el[start : start + 8, :] = values[c][i]
        sums = [None] * pairs_el
        for n in range(nodes_el):
            for cp in range(3):
                here = c_row(cp * padded + n)
                for j in range(pairs_el):
                    start = ((n % 2) * 3 + cp) * 4 * padded + 8 * j
                    term = kmat[n // 2, start : start + 8, :] * here
                    sums[j] = term if sums[j] is None else sums[j] + term
        return [pack(x) for x in sums]

    def c_row(i):
        return jnp.broadcast_to(at_el[i : i + 1, :], (8, LANES))

    def record(t, slot_index):
        comps = [
            t[0][0],
            t[1][1],
            t[2][2],
            0.5 * (t[1][2] + t[2][1]),
            0.5 * (t[0][2] + t[2][0]),
            0.5 * (t[0][1] + t[1][0]),
        ]
        for c, value in enumerate(comps):
            start = (slot_index // half) * 6 + c
            start = pl.multiple_of((start * half + lax.rem(slot_index, half)) * points, points)
            snaps[pl.ds(start, points), :] = value

    velocity = wav_ref[0] * source * half_inverse
    displace = time_step * velocity

    def order_for(w):
        start = pl.multiple_of(w * block, block)
        res = lax.dot_general(
            lhs[...],
            perm[pl.ds(start, block), :],
            (((1,), (1,)), ((), ())),
            preferred_element_type=F32,
        )
        return res.astype(BF16).reshape(6, half, block)

    def mine(i):
        return pl.ds(pl.multiple_of(i * block, block), block)

    def parcel(h, i, column, target):
        return pltpu.make_async_remote_copy(
            src_ref=ordered.at[h, i],
            dst_ref=out_ref.at[:, h * half : (h + 1) * half, mine(column)],
            send_sem=out_send_sem.at[h, i],
            recv_sem=out_recv_sem.at[h, i],
            device_id=(g, target),
            device_id_type=MESH,
        )

    def arriving(h, i):
        origin = lax.rem(my_d - i + writers, writers)
        return parcel(h, i, along(origin), origin)

    def ship(h):
        count = 6 * half
        for q in range(points):
            lhs[:, q * LANES : (q + 1) * LANES] = snaps[
                pl.ds(h * count * points + q, count, stride=points), :
            ].astype(BF16)
        for i in range(1, writers):
            w = lax.rem(my_d + i, writers)
            ordered[h, i] = order_for(w)
            parcel(h, i, d, w).start()
        last = order_for(my_d)

        @pl.when(other_core)
        def _():
            ordered[h, 0] = last
            parcel(h, 0, d, my_d).start()

        @pl.when(jnp.logical_not(other_core))
        def _():
            out_ref[:, h * half : (h + 1) * half, mine(d)] = last

    def launch(t, values, got, displace, velocity, extra):
        packs = stiffness(values)
        send_shared(face_forces(packs), lax.rem(t, 2))
        record(gradient(values), t - 1)
        if got is not None:
            change = half_inverse * at_nodes(got)
            velocity = velocity - change
            displace = displace - time_step * change
        velocity = velocity + half_inverse * (wav_ref[t] * source - node_forces(packs))
        displace = displace + time_step * velocity
        values = gather(displace)
        extra(t)
        return values, displace, velocity

    def advance(t, state, extra):
        values, displace, velocity = state
        got = shared_sum(lax.rem(t - 1, 2))
        return launch(t, corrected(values, got), got, displace, velocity, extra)

    def order_some(t):
        for i in range(tables):
            build_order(jnp.minimum(t * tables + i, points - 1))

    state = launch(jnp.int32(1), gather(displace), None, displace, velocity, order_some)
    state = lax.fori_loop(2, half, lambda t, held: advance(t, held, order_some), state)
    state = advance(jnp.int32(half), state, lambda t: ship(0))
    state = lax.fori_loop(
        half + 1, steps, lambda t, held: advance(t, held, lambda t: None), state
    )
    got = shared_sum(lax.rem(jnp.int32(steps - 1), 2))
    record(gradient(corrected(state[0], got)), jnp.int32(steps - 1))
    ship(1)
    for h in range(2):
        for i in range(1, writers):
            arriving(h, i).wait_recv()
            parcel(h, i, d, lax.rem(my_d + i, writers)).wait_send()

        @pl.when(other_core)
        def _():
            arriving(h, 0).wait_recv()
            parcel(h, 0, d, my_d).wait_send()


def solution(mesh):
    groups, writers = mesh.shape["grp"], mesh.shape["dom"]

    def shards(
        connect,
        interface_nodes,
        neighbours,
        point_rank,
        shape_grad,
        inverse_jacobian,
        lame_moduli,
        point_weights,
        mass_elem,
        source_pattern,
        wavelet,
    ):
        nodes_el, elements = connect.shape
        points = point_weights.shape[0]
        point_count = point_rank.shape[1]
        steps = wavelet.shape[0]
        padded = -(-nodes_el // 8) * 8
        vmem = pl.BlockSpec(memory_space=pltpu.VMEM)
        smem = pl.BlockSpec(memory_space=pltpu.SMEM)
        hbm = pl.BlockSpec(memory_space=pl.ANY)
        sharded = (
            connect,
            interface_nodes,
            neighbours,
            point_rank,
            inverse_jacobian,
            lame_moduli,
            point_weights,
            mass_elem,
            source_pattern,
        )
        ordered = pl.pallas_call(
            functools.partial(kernel, groups, writers, steps, nodes_el),
            out_shape=jax.ShapeDtypeStruct((6, steps, point_count), BF16),
            in_specs=[hbm] * len(sharded) + [vmem, smem],
            out_specs=vmem,
            scratch_shapes=[pltpu.VMEM(a.shape, a.dtype) for a in sharded] * 2
            + [pltpu.SemaphoreType.DMA((len(sharded),))] * 3
            + [
                pltpu.VMEM((nodes_el // 2 * LANES, 2 * LANES), BF16),
                pltpu.VMEM((nodes_el // 2 * LANES, 2 * LANES), BF16),
                pltpu.VMEM((nodes_el // 2 * (source_pattern.shape[1] // LANES) * 16, LANES), BF16),
                pltpu.VMEM((3, padded, LANES), F32),
                pltpu.VMEM((nodes_el // 2, 18 * padded, LANES), BF16),
                pltpu.VMEM((LANES, LANES), BF16),
                pltpu.VMEM((nodes_el // 2, 24 * padded, LANES), F32),
                pltpu.VMEM((3 * padded, LANES), F32),
                pltpu.VMEM((point_count, point_count), BF16),
                pltpu.VMEM((3 * points, 96), BF16),
                pltpu.VMEM((steps * 6 * points, LANES), F32),
                pltpu.VMEM((steps // 2 * 6, point_count), BF16),
                pltpu.VMEM((2, writers, 6, steps // 2, point_count // writers), BF16),
                pltpu.VMEM((2, 8, LANES), F32),
                pltpu.VMEM((2, 4, 8, LANES), F32),
                pltpu.SemaphoreType.DMA((2, 4)),
                pltpu.SemaphoreType.DMA((2, 4)),
                pltpu.SemaphoreType.DMA((2, writers)),
                pltpu.SemaphoreType.DMA((2, writers)),
            ],
            compiler_params=pltpu.CompilerParams(
                collective_id=0, has_side_effects=True, vmem_limit_bytes=56 * 1024 * 1024
            ),
            name="window",
        )(
            *sharded,
            shape_grad.T,
            wavelet,
        )
        return ordered.transpose(1, 0, 2)

    placed = (
        P(None, ("grp", "dom")),
        P(("grp", "dom"), None, None),
        P(("grp", "dom"), None),
        P(("grp", "dom"), None),
        P(),
        P(None, ("grp", "dom")),
        P(None, ("grp", "dom")),
        P(None, ("grp", "dom")),
        P(None, ("grp", "dom")),
        P(None, ("grp", "dom")),
        P(),
    )
    return jax.shard_map(
        shards, mesh=mesh, in_specs=placed, out_specs=P(None, None, ("grp", "dom")), check_vma=False
    )
```

```python
import functools

import jax
import jax.numpy as jnp
from jax import lax
from jax.experimental import pallas as pl
from jax.experimental.pallas import tpu as pltpu
from jax.sharding import PartitionSpec as P

MESH = pl.DeviceIdType.MESH
F32 = jnp.float32
BF16 = jnp.bfloat16
time_step = 0.5
LANES = 128


def split(x):
    hi = x.astype(BF16)
    return hi, (x - hi.astype(F32)).astype(BF16)


def pick_lanes(x, idx):
    return jnp.take_along_axis(x, idx, axis=1, mode="promise_in_bounds")


def kernel(
    groups,
    writers,
    steps,
    nodes_el,
    conn_in,
    faces_in,
    nb_in,
    rank_in,
    jac_in,
    lame_in,
    pw_in,
    mass_in,
    src_in,
    gradt_ref,
    wav_ref,
    out_ref,
    conn_ref,
    faces_ref,
    nb_ref,
    rank_ref,
    jac_ref,
    lame_ref,
    pw_ref,
    mass_ref,
    src_ref,
    conn_own,
    faces_own,
    nb_own,
    rank_own,
    jac_own,
    lame_own,
    pw_own,
    mass_own,
    src_own,
    move_sem,
    move_send_sem,
    move_recv_sem,
    at_face,
    at_node,
    hmask,
    basis,
    products,
    pww,
    kmat,
    at_el,
    w1,
    snap,
    spread,
    route,
    stage,
    mixed,
    pair,
    pair_in,
    ordered,
    send,
    recv,
    send_sem,
    recv_sem,
    out_send_sem,
    out_recv_sem,
):
    my_g = lax.axis_index("grp")
    my_d = lax.axis_index("dom")
    points = pw_ref.shape[0]
    block = out_ref.shape[2] // writers
    blocks = src_ref.shape[1] // LANES

    def along(w):
        if writers % 4:
            return w
        return w + lax.rem(w // 2, 2) * (1 - 2 * lax.rem(w, 2))

    def across(g, w):
        if groups % 2:
            return g
        return g + lax.rem(w, 2) * (1 - 2 * lax.rem(g, 2))

    def host(g, w):
        return across(g, w), along(w)

    d = along(my_d)
    g = across(my_g, d)
    stays = (g == my_g) & (d == my_d)
    moves = jnp.logical_not(stays)
    other_core = g != my_g
    target = host(my_g, my_d)

    has = (g > 0, g < groups - 1, d > 0, d < writers - 1)
    where_to = (host(g - 1, d), host(g + 1, d), host(g, d - 1), host(g, d + 1))

    arrays = (
        (conn_in, conn_own, conn_ref),
        (faces_in, faces_own, faces_ref),
        (mass_in, mass_own, mass_ref),
        (src_in, src_own, src_ref),
        (nb_in, nb_own, nb_ref),
        (pw_in, pw_own, pw_ref),
        (jac_in, jac_own, jac_ref),
        (lame_in, lame_own, lame_ref),
        (rank_in, rank_own, rank_ref),
    )

    def fetch(i, kept):
        return pltpu.make_async_copy(
            arrays[i][0], arrays[i][2 if kept else 1], move_sem.at[i]
        )

    def move(i):
        return pltpu.make_async_remote_copy(
            src_ref=arrays[i][1],
            dst_ref=arrays[i][2],
            send_sem=move_send_sem.at[i],
            recv_sem=move_recv_sem.at[i],
            device_id=target,
            device_id_type=MESH,
        )

    @pl.when(stays)
    def _():
        for i in range(len(arrays)):
            fetch(i, True).start()

    recv[...] = jnp.zeros_like(recv)
    barrier = pltpu.get_barrier_semaphore()

    @pl.when(moves)
    def _():
        for i in range(len(arrays)):
            fetch(i, False).start()
        pl.semaphore_signal(barrier, inc=1, device_id=(g, d), device_id_type=MESH)

    for k in range(4):

        @pl.when(has[k])
        def _():
            pl.semaphore_signal(barrier, inc=1, device_id=where_to[k], device_id_type=MESH)

    for i in range(writers):
        origin_d = lax.rem(my_d + i, writers)
        origin = (across(my_g, along(origin_d)), origin_d)

        def greet():
            pl.semaphore_signal(barrier, inc=1, device_id=origin, device_id_type=MESH)

        if i:
            greet()
        else:
            pl.when(other_core)(greet)

    expected = moves.astype(jnp.int32) + other_core.astype(jnp.int32) + writers - 1
    for k in range(4):
        expected = expected + has[k].astype(jnp.int32)
    pl.semaphore_wait(barrier, expected)

    @pl.when(moves)
    def _():
        for i in range(len(arrays)):
            fetch(i, False).wait()
            move(i).start()

    def landed(lo, hi):
        @pl.when(stays)
        def _():
            for i in range(lo, hi):
                fetch(i, True).wait()

        @pl.when(moves)
        def _():
            for i in range(lo, hi):
                move(i).wait_recv()
                move(i).wait_send()


    lane = lax.broadcasted_iota(jnp.int32, (LANES, LANES), 1)
    row8 = lax.broadcasted_iota(jnp.int32, (8, LANES), 0)
    row16 = lax.broadcasted_iota(jnp.int32, (16, LANES), 0)
    pairs_el = nodes_el // 2
    padded = -(-nodes_el // 8) * 8
    tiles = padded // 8

    gradt = gradt_ref[...]
    depth = 3 * points
    hi = gradt.astype(BF16).astype(F32)
    lo = gradt - hi
    gap = jnp.zeros((32 - nodes_el, depth), F32)
    tall = jnp.concatenate([hi, gap, hi, gap, lo, gap, jnp.zeros((32, depth), F32)], axis=0)
    tall = jnp.concatenate([tall, jnp.zeros((LANES, LANES - depth), F32)], axis=1)
    w1[...] = tall.T[0:depth, 0:96].astype(BF16)

    lanes = lax.broadcasted_iota(jnp.int32, (padded, LANES), 1)
    base = jnp.concatenate([gradt, jnp.zeros((padded - nodes_el, depth), F32)], axis=0)
    base = jnp.concatenate([base, jnp.zeros((padded, LANES - depth), F32)], axis=1)
    own_dir = []
    for r in range(3):
        x = pltpu.roll(base, LANES - r * points, 1) if r else base
        x = jnp.where(lanes < points, x, 0.0)
        x = x + pltpu.roll(x, points, 1) + pltpu.roll(x, 2 * points, 1)
        own_dir.append(x)
        basis[r] = x

    def multiply_pairs(m, carry):
        for rp in range(3):
            parts = []
            for p in range(2):
                other = basis[rp, pl.ds(2 * m + p, 1), :]
                for r in range(3):
                    product = own_dir[r] * other
                    high = product.astype(BF16).astype(F32)
                    parts.append(jnp.where(lanes < 2 * points, high, product - high))
            rows = 6 * padded
            products[m, rp * rows : (rp + 1) * rows, :] = jnp.concatenate(
                parts, axis=0
            ).astype(BF16)
        return carry

    lax.fori_loop(0, pairs_el, multiply_pairs, 0)

    def clear(m, carry):
        kmat[m] = jnp.zeros(kmat.shape[1:], F32)
        return carry

    lax.fori_loop(0, pairs_el, clear, 0)

    half = steps // 2
    held = steps * points * 8
    last_rows = 2 * points * 8
    stage[held - last_rows : held, :] = jnp.zeros((last_rows, LANES), F32)
    snap[...] = jnp.zeros_like(snap)

    landed(0, 2)
    faces = faces_ref[0].astype(F32)
    face_row = jnp.concatenate([faces[k : k + 1, :] for k in range(4)], axis=1)
    face_swap = jnp.concatenate([faces[k ^ 1 : (k ^ 1) + 1, :] for k in range(4)], axis=1)
    face_swap = jnp.broadcast_to(face_swap.astype(jnp.int32), (LANES, LANES))
    face_low = jnp.bitwise_and(face_swap[0:8], LANES - 1)
    face_high = jnp.right_shift(face_swap[0:8], 7)

    columns = jnp.concatenate(
        [conn_ref[...].astype(F32), jnp.zeros((LANES - nodes_el, LANES), F32)], axis=0
    ).T.astype(jnp.int32)

    def column(n):
        return jnp.broadcast_to(columns[:, n : n + 1], (LANES, LANES))

    def spot(n):
        j, p = n // 2, n % 2
        return slice(j * LANES, (j + 1) * LANES), slice(p * LANES, (p + 1) * LANES)

    for n in range(nodes_el):
        at_face[spot(n)] = jnp.where(column(n) == face_swap, 1.0, 0.0).astype(BF16)

    def pack(x):
        high = x.astype(BF16).astype(F32)
        return jnp.concatenate([high, x - high], axis=0).astype(BF16)

    def face_forces(packs):
        res = jnp.dot(
            jnp.concatenate(packs, axis=1), at_face[...], preferred_element_type=F32
        )
        res = res[0:8] + res[8:16]
        mixed = jnp.where(row8 < 4, res[:, 0:LANES], res[:, LANES:])
        return mixed + pltpu.roll(mixed, 4, 0)

    def node_forces(packs):
        sides = []
        for b in range(blocks):
            sides.append(
                jnp.concatenate(
                    [
                        packs[j] * hmask[(j * blocks + b) * 16 : (j * blocks + b + 1) * 16, :]
                        for j in range(pairs_el)
                    ],
                    axis=1,
                )
            )
        res = jnp.dot(
            jnp.concatenate(sides, axis=0), at_node[...], preferred_element_type=F32
        )
        halves = []
        for b in range(blocks):
            one = res[16 * b : 16 * b + 8] + res[16 * b + 8 : 16 * b + 16]
            even, odd = one[:, 0:LANES], one[:, LANES:]
            if b % 2:
                halves.append(pltpu.roll(even, 4, 0) + odd)
            else:
                halves.append(even + pltpu.roll(odd, 4, 0))
        return jnp.concatenate(
            [jnp.where(row8 < 4, halves[b], halves[b + 1]) for b in range(0, blocks, 2)],
            axis=0,
        )

    landed(2, 5)
    quarter = jnp.right_shift(lax.broadcasted_iota(jnp.int32, (8, LANES), 1), 5)
    nb = nb_ref[...].astype(F32)
    recv_mask = [jnp.where(quarter == k, nb[:, k : k + 1], 0.0) for k in range(4)]

    def copies(slot):
        return [
            pltpu.make_async_remote_copy(
                src_ref=send.at[slot, 0:4],
                dst_ref=recv.at[slot, k ^ 1, 0:4],
                send_sem=send_sem.at[slot, k],
                recv_sem=recv_sem.at[slot, k ^ 1],
                device_id=where_to[k],
                device_id_type=MESH,
            )
            for k in range(4)
        ]

    def arrivals(slot):
        return [
            pltpu.make_async_remote_copy(
                src_ref=send.at[slot, 0:4],
                dst_ref=recv.at[slot, k, 0:4],
                send_sem=send_sem.at[slot, k],
                recv_sem=recv_sem.at[slot, k],
                device_id=where_to[k],
                device_id_type=MESH,
            )
            for k in range(4)
        ]

    def send_shared(message, slot):
        send[slot] = message
        for k, copy in enumerate(copies(slot)):

            @pl.when(has[k])
            def _():
                copy.start()

    def shared_sum(slot):
        for k, copy in enumerate(arrivals(slot)):

            @pl.when(has[k])
            def _():
                copy.wait_recv()
                copy.wait_send()

        got = recv[slot, 0] * recv_mask[0]
        for k in range(1, 4):
            got = got + recv[slot, k] * recv_mask[k]
        return got

    masses = []
    for n in range(0, nodes_el, 2):
        mass = jnp.where(row8 == 3, mass_ref[n : n + 1, :], 0.0)
        masses.append(pack(mass + jnp.where(row8 == 7, mass_ref[n + 1 : n + 2, :], 0.0)))
    src_rows = []
    for b in range(blocks):
        src_rows.append(src_ref[:, b * LANES : (b + 1) * LANES])
        src_rows.append(jnp.zeros((1, LANES), F32))
    at_faces = jnp.zeros((8, LANES), F32)
    for b in range(blocks):
        rows = jnp.concatenate([src_rows[2 * b], jnp.zeros((5, LANES), F32)], axis=0)
        at_faces = jnp.where(face_high == b, pick_lanes(rows, face_low), at_faces)
    send_shared(face_forces(masses) + at_faces, 0)

    conn_low = jnp.bitwise_and(conn_ref[...], LANES - 1)
    conn_high = jnp.right_shift(conn_ref[...], 7)
    for n in range(nodes_el):
        low_column = jnp.bitwise_and(column(n), LANES - 1)
        at_node[spot(n)] = jnp.where(low_column == lane, 1.0, 0.0).astype(BF16)
    for j in range(pairs_el):
        two = [
            jnp.broadcast_to(conn_high[n : n + 1, :], (4, LANES)) for n in (2 * j, 2 * j + 1)
        ]
        two = jnp.concatenate(two * 2, axis=0)
        for b in range(blocks):
            hmask[(j * blocks + b) * 16 : (j * blocks + b + 1) * 16, :] = jnp.where(
                two == b, 1.0, 0.0
            ).astype(BF16)
    first = node_forces(masses) + jnp.concatenate(src_rows, axis=0)

    face_col = jnp.broadcast_to(face_row, (LANES, LANES)).T
    position = lax.broadcasted_iota(jnp.int32, (LANES, LANES), 0).astype(F32)
    inv_rows = []
    has_rows = []
    for b in range(blocks):
        hit = jnp.where(face_col == (lane + b * LANES).astype(F32), 1.0, 0.0)
        inv_rows.append(
            jnp.broadcast_to(jnp.sum(hit * position, axis=0, keepdims=True), (4, LANES))
        )
        has_rows.append(jnp.broadcast_to(jnp.sum(hit, axis=0, keepdims=True), (4, LANES)))
    inv_idx = jnp.concatenate(inv_rows, axis=0).astype(jnp.int32)
    inv_has = jnp.concatenate(has_rows, axis=0)

    def at_nodes(got):
        got = got + pltpu.roll(got, 4, 0)
        added = jnp.concatenate(
            [pick_lanes(got, inv_idx[0:8]), pick_lanes(got, inv_idx[8:16])], axis=0
        )
        return added * inv_has

    landed(5, len(arrays))
    weight = pw_ref[...]
    hi = weight.astype(BF16).astype(F32)
    pww[...] = jnp.concatenate(
        [hi, weight - hi, hi, jnp.zeros((LANES - depth, LANES), F32)], axis=0
    ).astype(BF16)
    jac = [jnp.broadcast_to(jac_ref[i : i + 1, :], (8, LANES)) for i in range(9)]
    lam = jnp.broadcast_to(lame_ref[0:1, :], (8, LANES))
    mu = jnp.broadcast_to(lame_ref[1:2, :], (8, LANES))

    def form_stiffness(m, carry):
        moments = jnp.dot(products[m], pww[...], preferred_element_type=F32)
        for p in range(2):
            for i in range(tiles):

                def moment(r, rp):
                    start = ((rp * 2 + p) * 3 + r) * padded + 8 * i
                    return moments[start : start + 8]

                half = [
                    [
                        jac[a] * moment(0, rp) + jac[3 + a] * moment(1, rp) + jac[6 + a] * moment(2, rp)
                        for rp in range(3)
                    ]
                    for a in range(3)
                ]
                full = [
                    [
                        jac[b] * half[a][0] + jac[3 + b] * half[a][1] + jac[6 + b] * half[a][2]
                        for b in range(3)
                    ]
                    for a in range(3)
                ]
                trace = mu * (full[0][0] + full[1][1] + full[2][2])
                for c in range(3):
                    for cp in range(3):
                        value = mu * full[cp][c] + lam * full[c][cp]
                        if c == cp:
                            value = value + trace
                        start = (p * 3 + cp) * 4 * padded + 32 * i + c
                        kmat[m, pl.ds(start, 8, stride=4), :] = value
        return carry

    group = 5 if pairs_el % 5 == 0 else 1

    def form_group(i, carry):
        for k in range(group):
            form_stiffness(i * group + k, carry)
        return carry

    lax.fori_loop(0, pairs_el // group, form_group, 0)

    first = first + at_nodes(shared_sum(0))
    axis_row = jnp.bitwise_and(row16, 3) < 3
    source = jnp.where(axis_row, first, 0.0)
    total = jnp.concatenate(
        [jnp.broadcast_to(first[4 * b + 3 : 4 * b + 4, :], (4, LANES)) for b in range(blocks)],
        axis=0,
    )
    half_inverse = jnp.where(axis_row, time_step / total, 0.0)

    spare = jnp.zeros((24 - nodes_el, LANES), jnp.int32)
    conn_low = jnp.concatenate([conn_low, spare], axis=0)
    conn_high = jnp.concatenate([conn_high, spare], axis=0)
    low = [conn_low[8 * i : 8 * i + 8, :] for i in range(3)]
    high = [conn_high[8 * i : 8 * i + 8, :] for i in range(3)]

    def at_elements(rows_of):
        out = []
        for i in range(3):
            acc = None
            for b in range(blocks):
                val = pick_lanes(jnp.broadcast_to(rows_of(b), (8, LANES)), low[i])
                acc = val if b == 0 else jnp.where(high[i] == b, val, acc)
            out.append(acc)
        return out

    def gather(u):
        return tuple(
            tuple(at_elements(lambda b: u[4 * b + c : 4 * b + c + 1, :])) for c in range(3)
        )

    def gradient(values):
        sides = []
        for c in range(3):
            rows = list(values[c]) + [jnp.zeros((8, LANES), F32)]
            hi, lo = split(jnp.concatenate(rows, axis=0))
            sides.append(jnp.concatenate([hi, lo, hi], axis=0))
        along = jnp.dot(
            w1[...], jnp.concatenate(sides, axis=1), preferred_element_type=F32
        )
        tensor = []
        for c in range(3):
            ref_dir = [
                along[r * points : (r + 1) * points, c * LANES : (c + 1) * LANES]
                for r in range(3)
            ]
            tensor.append(
                [
                    ref_dir[0] * jac_ref[e : e + 1, :]
                    + ref_dir[1] * jac_ref[3 + e : 4 + e, :]
                    + ref_dir[2] * jac_ref[6 + e : 7 + e, :]
                    for e in range(3)
                ]
            )
        return tensor

    def stiffness(values):
        for c in range(3):
            for i in range(tiles):
                start = c * padded + 8 * i
                at_el[start : start + 8, :] = values[c][i]
        sums = [None] * pairs_el
        for n in range(nodes_el):
            for cp in range(3):
                here = c_row(cp * padded + n)
                for j in range(pairs_el):
                    start = ((n % 2) * 3 + cp) * 4 * padded + 8 * j
                    term = kmat[n // 2, start : start + 8, :] * here
                    sums[j] = term if sums[j] is None else sums[j] + term
        return [pack(x) for x in sums]

    def c_row(i):
        return jnp.broadcast_to(at_el[i : i + 1, :], (8, LANES))

    def record(t):
        comps = [
            t[0][0],
            t[1][1],
            t[2][2],
            0.5 * (t[1][2] + t[2][1]),
            0.5 * (t[0][2] + t[2][0]),
            0.5 * (t[0][1] + t[1][0]),
        ]
        for c, value in enumerate(comps):
            snap[pl.ds(c, points, stride=8), :] = value

    def build_route():
        ranks = jnp.concatenate(
            [rank_ref[:, q * LANES : (q + 1) * LANES] for q in range(points)], axis=0
        )
        turned = jnp.concatenate(
            [ranks.astype(F32), jnp.zeros((LANES - points, LANES), F32)], axis=0
        ).T.astype(jnp.int32)
        upper = jnp.right_shift(ranks, 7)
        place_row = lax.broadcasted_iota(jnp.int32, (points, LANES), 0)
        lane_value = lax.broadcasted_iota(jnp.int32, (points, LANES), 1).astype(F32)
        sides = []
        for q in range(points):
            low = jnp.broadcast_to(turned[:, q : q + 1], (LANES, LANES))
            low = jnp.bitwise_and(low, LANES - 1)
            spread[q * LANES : (q + 1) * LANES, :] = jnp.where(low == lane, 1.0, 0.0).astype(BF16)
            mine_here = place_row == jnp.broadcast_to(upper[q : q + 1, :], (points, LANES))
            sides.append(
                jnp.concatenate(
                    [jnp.where(mine_here, float(q), 0.0), jnp.where(mine_here, lane_value, 0.0)],
                    axis=0,
                ).astype(BF16)
            )
        route[...] = jnp.dot(
            jnp.concatenate(sides, axis=1), spread[...], preferred_element_type=F32
        ).astype(jnp.int32)

    def in_order():
        sources = [snap[8 * q : 8 * q + 8, :] for q in range(points)]
        out = []
        for k in range(points):
            origin = jnp.broadcast_to(route[k : k + 1, :], (8, LANES))
            at = jnp.broadcast_to(route[points + k : points + k + 1, :], (8, LANES))
            value = pick_lanes(sources[0], at)
            for q in range(1, points):
                value = jnp.where(origin == q, pick_lanes(sources[q], at), value)
            out.append(value)
        return out

    def keep(t):
        for k, value in enumerate(in_order()):
            start = pl.multiple_of(t * (points * 8) + 8 * k, 8)
            stage[pl.ds(start, 8), :] = value

    velocity = wav_ref[0] * source * half_inverse
    displace = time_step * velocity

    def mine(i):
        return pl.ds(pl.multiple_of(i * block, block), block)

    def parcel(h, i, column, target):
        return pltpu.make_async_remote_copy(
            src_ref=ordered.at[h, :, :, mine(target)],
            dst_ref=out_ref.at[:, h * half : (h + 1) * half, mine(column)],
            send_sem=out_send_sem.at[h, i],
            recv_sem=out_recv_sem.at[h, i],
            device_id=(g, target),
            device_id_type=MESH,
        )

    def last_parcel(i, column, target):
        return pltpu.make_async_remote_copy(
            src_ref=pair.at[:, mine(target)],
            dst_ref=pair_in.at[:, mine(column)],
            send_sem=out_send_sem.at[2, i],
            recv_sem=out_recv_sem.at[2, i],
            device_id=(g, target),
            device_id_type=MESH,
        )

    def dispatch(make, local):
        for i in range(1, writers):
            make(i, d, lax.rem(my_d + i, writers)).start()

        @pl.when(other_core)
        def _():
            make(0, d, my_d).start()

        pl.when(jnp.logical_not(other_core))(local)

    def collect(make):
        for i in range(1, writers):
            origin = lax.rem(my_d - i + writers, writers)
            make(i, along(origin), origin).wait_recv()
            make(i, d, lax.rem(my_d + i, writers)).wait_send()

        @pl.when(other_core)
        def _():
            make(0, d, my_d).wait_recv()
            make(0, d, my_d).wait_send()

    def ship(h):
        for k in range(points):
            for c in range(6):
                start = h * half * points * 8 + 8 * k + c
                ordered[h, c, :, k * LANES : (k + 1) * LANES] = stage[
                    pl.ds(start, half, stride=points * 8), :
                ].astype(BF16)

        def local():
            out_ref[:, h * half : (h + 1) * half, mine(d)] = ordered[h, :, :, mine(my_d)]

        dispatch(functools.partial(parcel, h), local)

    def finish():
        for k, value in enumerate(in_order()):
            start = held - last_rows + 8 * k
            mixed[k, pl.ds(0, 8, stride=2), :] = stage[start : start + 8, :]
            mixed[k, pl.ds(1, 8, stride=2), :] = value
            pair[:, k * LANES : (k + 1) * LANES] = mixed[k].astype(BF16)

        def local():
            pair_in[:, mine(d)] = pair[:, mine(my_d)]

        dispatch(last_parcel, local)
        for h in range(2):
            collect(functools.partial(parcel, h))
        collect(last_parcel)
        for c in range(6):
            out_ref[c, steps - 2 : steps, :] = pair_in[2 * c : 2 * c + 2, :]

    def launch(t, values, got, displace, velocity, extra):
        packs = stiffness(values)
        send_shared(face_forces(packs), lax.rem(t, 2))
        record(gradient(values))
        if got is not None:
            change = half_inverse * at_nodes(got)
            velocity = velocity - change
            displace = displace - time_step * change
        velocity = velocity + half_inverse * (wav_ref[t] * source - node_forces(packs))
        displace = displace + time_step * velocity
        values = gather(displace)
        extra()
        keep(t - 1)
        return values, displace, velocity

    state = launch(jnp.int32(1), gather(displace), None, displace, velocity, build_route)

    inv_f = inv_idx.astype(F32)
    place = [x.astype(jnp.int32) for x in at_elements(lambda b: inv_f[4 * b : 4 * b + 1, :])]
    coef = (-time_step) * half_inverse * inv_has
    coef = at_elements(lambda b: coef[4 * b : 4 * b + 1, :])

    def corrected(values, got):
        out = []
        for c in range(3):
            row = jnp.broadcast_to(got[c : c + 1, :], (8, LANES))
            out.append(
                tuple(values[c][i] + pick_lanes(row, place[i]) * coef[i] for i in range(3))
            )
        return tuple(out)

    def advance(t, state):
        values, displace, velocity = state
        got = shared_sum(lax.rem(t - 1, 2))

        def ships():
            for h, when in ((0, half), (1, steps - 2)):
                pl.when(t == when)(functools.partial(ship, h))

        state = launch(t, corrected(values, got), got, displace, velocity, lambda: None)
        ships()
        return state

    state = lax.fori_loop(2, steps, advance, state)
    got = shared_sum(lax.rem(jnp.int32(steps - 1), 2))
    record(gradient(corrected(state[0], got)))
    finish()


def solution(mesh):
    groups, writers = mesh.shape["grp"], mesh.shape["dom"]

    def shards(
        connect,
        interface_nodes,
        neighbours,
        point_rank,
        shape_grad,
        inverse_jacobian,
        lame_moduli,
        point_weights,
        mass_elem,
        source_pattern,
        wavelet,
    ):
        nodes_el, elements = connect.shape
        points = point_weights.shape[0]
        point_count = point_rank.shape[1]
        steps = wavelet.shape[0]
        padded = -(-nodes_el // 8) * 8
        vmem = pl.BlockSpec(memory_space=pltpu.VMEM)
        smem = pl.BlockSpec(memory_space=pltpu.SMEM)
        hbm = pl.BlockSpec(memory_space=pl.ANY)
        sharded = (
            connect,
            interface_nodes,
            neighbours,
            point_rank,
            inverse_jacobian,
            lame_moduli,
            point_weights,
            mass_elem,
            source_pattern,
        )
        ordered = pl.pallas_call(
            functools.partial(kernel, groups, writers, steps, nodes_el),
            out_shape=jax.ShapeDtypeStruct((6, steps, point_count), BF16),
            in_specs=[hbm] * len(sharded) + [vmem, smem],
            out_specs=vmem,
            scratch_shapes=[pltpu.VMEM(a.shape, a.dtype) for a in sharded] * 2
            + [pltpu.SemaphoreType.DMA((len(sharded),))] * 3
            + [
                pltpu.VMEM((nodes_el // 2 * LANES, 2 * LANES), BF16),
                pltpu.VMEM((nodes_el // 2 * LANES, 2 * LANES), BF16),
                pltpu.VMEM((nodes_el // 2 * (source_pattern.shape[1] // LANES) * 16, LANES), BF16),
                pltpu.VMEM((3, padded, LANES), F32),
                pltpu.VMEM((nodes_el // 2, 18 * padded, LANES), BF16),
                pltpu.VMEM((LANES, LANES), BF16),
                pltpu.VMEM((nodes_el // 2, 24 * padded, LANES), F32),
                pltpu.VMEM((3 * padded, LANES), F32),
                pltpu.VMEM((3 * points, 96), BF16),
                pltpu.VMEM((8 * points, LANES), F32),
                pltpu.VMEM((points * LANES, LANES), BF16),
                pltpu.VMEM((2 * points, LANES), jnp.int32),
                pltpu.VMEM((steps * 8 * points, LANES), F32),
                pltpu.VMEM((points, 16, LANES), F32),
                pltpu.VMEM((16, point_count), BF16),
                pltpu.VMEM((16, point_count), BF16),
                pltpu.VMEM((2, 6, steps // 2, point_count), BF16),
                pltpu.VMEM((2, 8, LANES), F32),
                pltpu.VMEM((2, 4, 8, LANES), F32),
                pltpu.SemaphoreType.DMA((2, 4)),
                pltpu.SemaphoreType.DMA((2, 4)),
                pltpu.SemaphoreType.DMA((3, writers)),
                pltpu.SemaphoreType.DMA((3, writers)),
            ],
            compiler_params=pltpu.CompilerParams(
                collective_id=0, has_side_effects=True, vmem_limit_bytes=56 * 1024 * 1024
            ),
            name="window",
        )(
            *sharded,
            shape_grad.T,
            wavelet,
        )
        return ordered.transpose(1, 0, 2)

    placed = (
        P(None, ("grp", "dom")),
        P(("grp", "dom"), None, None),
        P(("grp", "dom"), None),
        P(("grp", "dom"), None),
        P(),
        P(None, ("grp", "dom")),
        P(None, ("grp", "dom")),
        P(None, ("grp", "dom")),
        P(None, ("grp", "dom")),
        P(None, ("grp", "dom")),
        P(),
    )
    return jax.shard_map(
        shards, mesh=mesh, in_specs=placed, out_specs=P(None, None, ("grp", "dom")), check_vma=False
    )
```

```python
import functools

import jax
import jax.numpy as jnp
from jax import lax
from jax.experimental import pallas as pl
from jax.experimental.pallas import tpu as pltpu
from jax.sharding import PartitionSpec as P

MESH = pl.DeviceIdType.MESH
F32 = jnp.float32
BF16 = jnp.bfloat16
time_step = 0.5
LANES = 128


def split(x):
    hi = x.astype(BF16)
    return hi, (x - hi.astype(F32)).astype(BF16)


def pick_lanes(x, idx):
    return jnp.take_along_axis(x, idx, axis=1, mode="promise_in_bounds")


def kernel(
    groups,
    writers,
    steps,
    nodes_el,
    conn_in,
    faces_in,
    nb_in,
    rank_in,
    jac_in,
    lame_in,
    pw_in,
    mass_in,
    src_in,
    gradt_ref,
    wav_ref,
    out_ref,
    conn_ref,
    faces_ref,
    nb_ref,
    rank_ref,
    jac_ref,
    lame_ref,
    pw_ref,
    mass_ref,
    src_ref,
    conn_own,
    faces_own,
    nb_own,
    rank_own,
    jac_own,
    lame_own,
    pw_own,
    mass_own,
    src_own,
    move_sem,
    move_send_sem,
    move_recv_sem,
    at_face,
    at_node,
    hmask,
    basis,
    products,
    pww,
    kmat,
    at_el,
    w1,
    snap,
    spread,
    route,
    mixed,
    pair,
    pair_in,
    send,
    recv,
    send_sem,
    recv_sem,
    out_send_sem,
    out_recv_sem,
):
    my_g = lax.axis_index("grp")
    my_d = lax.axis_index("dom")
    points = pw_ref.shape[0]
    block = out_ref.shape[2] // writers
    blocks = src_ref.shape[1] // LANES

    def along(w):
        if writers % 4:
            return w
        return w + lax.rem(w // 2, 2) * (1 - 2 * lax.rem(w, 2))

    def across(g, w):
        if groups % 2:
            return g
        return g + lax.rem(w, 2) * (1 - 2 * lax.rem(g, 2))

    def host(g, w):
        return across(g, w), along(w)

    d = along(my_d)
    g = across(my_g, d)
    stays = (g == my_g) & (d == my_d)
    moves = jnp.logical_not(stays)
    other_core = g != my_g
    target = host(my_g, my_d)

    has = (g > 0, g < groups - 1, d > 0, d < writers - 1)
    where_to = (host(g - 1, d), host(g + 1, d), host(g, d - 1), host(g, d + 1))

    arrays = (
        (conn_in, conn_own, conn_ref),
        (faces_in, faces_own, faces_ref),
        (mass_in, mass_own, mass_ref),
        (src_in, src_own, src_ref),
        (nb_in, nb_own, nb_ref),
        (pw_in, pw_own, pw_ref),
        (jac_in, jac_own, jac_ref),
        (lame_in, lame_own, lame_ref),
        (rank_in, rank_own, rank_ref),
    )

    def fetch(i, kept):
        return pltpu.make_async_copy(
            arrays[i][0], arrays[i][2 if kept else 1], move_sem.at[i]
        )

    def move(i):
        return pltpu.make_async_remote_copy(
            src_ref=arrays[i][1],
            dst_ref=arrays[i][2],
            send_sem=move_send_sem.at[i],
            recv_sem=move_recv_sem.at[i],
            device_id=target,
            device_id_type=MESH,
        )

    recv[...] = jnp.zeros_like(recv)
    barrier = pltpu.get_barrier_semaphore()

    @pl.when(moves)
    def _():
        pl.semaphore_signal(barrier, inc=1, device_id=(g, d), device_id_type=MESH)

    for k in range(4):

        @pl.when(has[k])
        def _():
            pl.semaphore_signal(barrier, inc=1, device_id=where_to[k], device_id_type=MESH)

    for i in range(writers):
        origin_d = lax.rem(my_d + i, writers)
        origin = (across(my_g, along(origin_d)), origin_d)

        def greet():
            pl.semaphore_signal(barrier, inc=1, device_id=origin, device_id_type=MESH)

        if i:
            greet()
        else:
            pl.when(other_core)(greet)

    @pl.when(stays)
    def _():
        for i in range(len(arrays)):
            fetch(i, True).start()

    @pl.when(moves)
    def _():
        for i in range(len(arrays)):
            fetch(i, False).start()

    expected = moves.astype(jnp.int32) + other_core.astype(jnp.int32) + writers - 1
    for k in range(4):
        expected = expected + has[k].astype(jnp.int32)
    pl.semaphore_wait(barrier, expected)

    @pl.when(moves)
    def _():
        for i in range(len(arrays)):
            fetch(i, False).wait()
            move(i).start()

    def landed(lo, hi):
        @pl.when(stays)
        def _():
            for i in range(lo, hi):
                fetch(i, True).wait()

        @pl.when(moves)
        def _():
            for i in range(lo, hi):
                move(i).wait_recv()
                move(i).wait_send()


    lane = lax.broadcasted_iota(jnp.int32, (LANES, LANES), 1)
    row8 = lax.broadcasted_iota(jnp.int32, (8, LANES), 0)
    row16 = lax.broadcasted_iota(jnp.int32, (16, LANES), 0)
    pairs_el = nodes_el // 2
    padded = -(-nodes_el // 8) * 8
    tiles = padded // 8

    gradt = gradt_ref[...]
    depth = 3 * points
    hi = gradt.astype(BF16).astype(F32)
    lo = gradt - hi
    gap = jnp.zeros((32 - nodes_el, depth), F32)
    tall = jnp.concatenate([hi, gap, hi, gap, lo, gap, jnp.zeros((32, depth), F32)], axis=0)
    tall = jnp.concatenate([tall, jnp.zeros((LANES, LANES - depth), F32)], axis=1)
    w1[...] = tall.T[0:depth, 0:96].astype(BF16)

    lanes = lax.broadcasted_iota(jnp.int32, (padded, LANES), 1)
    base = jnp.concatenate([gradt, jnp.zeros((padded - nodes_el, depth), F32)], axis=0)
    base = jnp.concatenate([base, jnp.zeros((padded, LANES - depth), F32)], axis=1)
    own_dir = []
    for r in range(3):
        x = pltpu.roll(base, LANES - r * points, 1) if r else base
        x = jnp.where(lanes < points, x, 0.0)
        x = x + pltpu.roll(x, points, 1) + pltpu.roll(x, 2 * points, 1)
        own_dir.append(x)
        basis[r] = x

    def multiply_pairs(m, carry):
        for rp in range(3):
            parts = []
            for p in range(2):
                other = basis[rp, pl.ds(2 * m + p, 1), :]
                for r in range(3):
                    product = own_dir[r] * other
                    high = product.astype(BF16).astype(F32)
                    parts.append(jnp.where(lanes < 2 * points, high, product - high))
            rows = 6 * padded
            products[m, rp * rows : (rp + 1) * rows, :] = jnp.concatenate(
                parts, axis=0
            ).astype(BF16)
        return carry

    lax.fori_loop(0, pairs_el, multiply_pairs, 0)

    def clear(m, carry):
        kmat[m] = jnp.zeros(kmat.shape[1:], F32)
        return carry

    lax.fori_loop(0, pairs_el, clear, 0)

    chunks = steps // 2
    snap[...] = jnp.zeros_like(snap)

    landed(0, 2)
    faces = faces_ref[0].astype(F32)
    face_row = jnp.concatenate([faces[k : k + 1, :] for k in range(4)], axis=1)
    face_swap = jnp.concatenate([faces[k ^ 1 : (k ^ 1) + 1, :] for k in range(4)], axis=1)
    face_swap = jnp.broadcast_to(face_swap.astype(jnp.int32), (LANES, LANES))
    face_low = jnp.bitwise_and(face_swap[0:8], LANES - 1)
    face_high = jnp.right_shift(face_swap[0:8], 7)

    columns = jnp.concatenate(
        [conn_ref[...].astype(F32), jnp.zeros((LANES - nodes_el, LANES), F32)], axis=0
    ).T.astype(jnp.int32)

    def column(n):
        return jnp.broadcast_to(columns[:, n : n + 1], (LANES, LANES))

    def spot(n):
        j, p = n // 2, n % 2
        return slice(j * LANES, (j + 1) * LANES), slice(p * LANES, (p + 1) * LANES)

    for n in range(nodes_el):
        at_face[spot(n)] = jnp.where(column(n) == face_swap, 1.0, 0.0).astype(BF16)

    def pack(x):
        high = x.astype(BF16).astype(F32)
        return jnp.concatenate([high, x - high], axis=0).astype(BF16)

    def face_forces(packs):
        res = jnp.dot(
            jnp.concatenate(packs, axis=1), at_face[...], preferred_element_type=F32
        )
        res = res[0:8] + res[8:16]
        mixed = jnp.where(row8 < 4, res[:, 0:LANES], res[:, LANES:])
        return mixed + pltpu.roll(mixed, 4, 0)

    def node_forces(packs):
        sides = []
        for b in range(blocks):
            sides.append(
                jnp.concatenate(
                    [
                        packs[j] * hmask[(j * blocks + b) * 16 : (j * blocks + b + 1) * 16, :]
                        for j in range(pairs_el)
                    ],
                    axis=1,
                )
            )
        res = jnp.dot(
            jnp.concatenate(sides, axis=0), at_node[...], preferred_element_type=F32
        )
        halves = []
        for b in range(blocks):
            one = res[16 * b : 16 * b + 8] + res[16 * b + 8 : 16 * b + 16]
            even, odd = one[:, 0:LANES], one[:, LANES:]
            if b % 2:
                halves.append(pltpu.roll(even, 4, 0) + odd)
            else:
                halves.append(even + pltpu.roll(odd, 4, 0))
        return jnp.concatenate(
            [jnp.where(row8 < 4, halves[b], halves[b + 1]) for b in range(0, blocks, 2)],
            axis=0,
        )

    landed(2, 5)
    quarter = jnp.right_shift(lax.broadcasted_iota(jnp.int32, (8, LANES), 1), 5)
    nb = nb_ref[...].astype(F32)
    recv_mask = [jnp.where(quarter == k, nb[:, k : k + 1], 0.0) for k in range(4)]

    def copies(slot):
        return [
            pltpu.make_async_remote_copy(
                src_ref=send.at[slot, 0:4],
                dst_ref=recv.at[slot, k ^ 1, 0:4],
                send_sem=send_sem.at[slot, k],
                recv_sem=recv_sem.at[slot, k ^ 1],
                device_id=where_to[k],
                device_id_type=MESH,
            )
            for k in range(4)
        ]

    def arrivals(slot):
        return [
            pltpu.make_async_remote_copy(
                src_ref=send.at[slot, 0:4],
                dst_ref=recv.at[slot, k, 0:4],
                send_sem=send_sem.at[slot, k],
                recv_sem=recv_sem.at[slot, k],
                device_id=where_to[k],
                device_id_type=MESH,
            )
            for k in range(4)
        ]

    def send_shared(message, slot):
        send[slot] = message
        for k, copy in enumerate(copies(slot)):

            @pl.when(has[k])
            def _():
                copy.start()

    def shared_sum(slot):
        for k, copy in enumerate(arrivals(slot)):

            @pl.when(has[k])
            def _():
                copy.wait_recv()
                copy.wait_send()

        got = recv[slot, 0] * recv_mask[0]
        for k in range(1, 4):
            got = got + recv[slot, k] * recv_mask[k]
        return got

    masses = []
    for n in range(0, nodes_el, 2):
        mass = jnp.where(row8 == 3, mass_ref[n : n + 1, :], 0.0)
        masses.append(pack(mass + jnp.where(row8 == 7, mass_ref[n + 1 : n + 2, :], 0.0)))
    src_rows = []
    for b in range(blocks):
        src_rows.append(src_ref[:, b * LANES : (b + 1) * LANES])
        src_rows.append(jnp.zeros((1, LANES), F32))
    at_faces = jnp.zeros((8, LANES), F32)
    for b in range(blocks):
        rows = jnp.concatenate([src_rows[2 * b], jnp.zeros((5, LANES), F32)], axis=0)
        at_faces = jnp.where(face_high == b, pick_lanes(rows, face_low), at_faces)
    send_shared(face_forces(masses) + at_faces, 0)

    conn_low = jnp.bitwise_and(conn_ref[...], LANES - 1)
    conn_high = jnp.right_shift(conn_ref[...], 7)
    for n in range(nodes_el):
        low_column = jnp.bitwise_and(column(n), LANES - 1)
        at_node[spot(n)] = jnp.where(low_column == lane, 1.0, 0.0).astype(BF16)
    for j in range(pairs_el):
        two = [
            jnp.broadcast_to(conn_high[n : n + 1, :], (4, LANES)) for n in (2 * j, 2 * j + 1)
        ]
        two = jnp.concatenate(two * 2, axis=0)
        for b in range(blocks):
            hmask[(j * blocks + b) * 16 : (j * blocks + b + 1) * 16, :] = jnp.where(
                two == b, 1.0, 0.0
            ).astype(BF16)
    first = node_forces(masses) + jnp.concatenate(src_rows, axis=0)

    face_col = jnp.broadcast_to(face_row, (LANES, LANES)).T
    position = lax.broadcasted_iota(jnp.int32, (LANES, LANES), 0).astype(F32)
    inv_rows = []
    has_rows = []
    for b in range(blocks):
        hit = jnp.where(face_col == (lane + b * LANES).astype(F32), 1.0, 0.0)
        inv_rows.append(
            jnp.broadcast_to(jnp.sum(hit * position, axis=0, keepdims=True), (4, LANES))
        )
        has_rows.append(jnp.broadcast_to(jnp.sum(hit, axis=0, keepdims=True), (4, LANES)))
    inv_idx = jnp.concatenate(inv_rows, axis=0).astype(jnp.int32)
    inv_has = jnp.concatenate(has_rows, axis=0)

    def at_nodes(got):
        got = got + pltpu.roll(got, 4, 0)
        added = jnp.concatenate(
            [pick_lanes(got, inv_idx[0:8]), pick_lanes(got, inv_idx[8:16])], axis=0
        )
        return added * inv_has

    landed(5, len(arrays))
    weight = pw_ref[...]
    hi = weight.astype(BF16).astype(F32)
    pww[...] = jnp.concatenate(
        [hi, weight - hi, hi, jnp.zeros((LANES - depth, LANES), F32)], axis=0
    ).astype(BF16)
    jac = [jnp.broadcast_to(jac_ref[i : i + 1, :], (8, LANES)) for i in range(9)]
    lam = jnp.broadcast_to(lame_ref[0:1, :], (8, LANES))
    mu = jnp.broadcast_to(lame_ref[1:2, :], (8, LANES))

    def form_stiffness(m, carry):
        moments = jnp.dot(products[m], pww[...], preferred_element_type=F32)
        for p in range(2):
            for i in range(tiles):

                def moment(r, rp):
                    start = ((rp * 2 + p) * 3 + r) * padded + 8 * i
                    return moments[start : start + 8]

                half = [
                    [
                        jac[a] * moment(0, rp) + jac[3 + a] * moment(1, rp) + jac[6 + a] * moment(2, rp)
                        for rp in range(3)
                    ]
                    for a in range(3)
                ]
                full = [
                    [
                        jac[b] * half[a][0] + jac[3 + b] * half[a][1] + jac[6 + b] * half[a][2]
                        for b in range(3)
                    ]
                    for a in range(3)
                ]
                trace = mu * (full[0][0] + full[1][1] + full[2][2])
                for c in range(3):
                    for cp in range(3):
                        value = mu * full[cp][c] + lam * full[c][cp]
                        if c == cp:
                            value = value + trace
                        start = (p * 3 + cp) * 4 * padded + 32 * i + c
                        kmat[m, pl.ds(start, 8, stride=4), :] = value
        return carry

    group = 5 if pairs_el % 5 == 0 else 1

    def form_group(i, carry):
        for k in range(group):
            form_stiffness(i * group + k, carry)
        return carry

    lax.fori_loop(0, pairs_el // group, form_group, 0)

    first = first + at_nodes(shared_sum(0))
    axis_row = jnp.bitwise_and(row16, 3) < 3
    source = jnp.where(axis_row, first, 0.0)
    total = jnp.concatenate(
        [jnp.broadcast_to(first[4 * b + 3 : 4 * b + 4, :], (4, LANES)) for b in range(blocks)],
        axis=0,
    )
    half_inverse = jnp.where(axis_row, time_step / total, 0.0)

    spare = jnp.zeros((24 - nodes_el, LANES), jnp.int32)
    conn_low = jnp.concatenate([conn_low, spare], axis=0)
    conn_high = jnp.concatenate([conn_high, spare], axis=0)
    low = [conn_low[8 * i : 8 * i + 8, :] for i in range(3)]
    high = [conn_high[8 * i : 8 * i + 8, :] for i in range(3)]

    def at_elements(rows_of):
        out = []
        for i in range(3):
            acc = None
            for b in range(blocks):
                val = pick_lanes(jnp.broadcast_to(rows_of(b), (8, LANES)), low[i])
                acc = val if b == 0 else jnp.where(high[i] == b, val, acc)
            out.append(acc)
        return out

    def gather(u):
        return tuple(
            tuple(at_elements(lambda b: u[4 * b + c : 4 * b + c + 1, :])) for c in range(3)
        )

    def gradient(values):
        sides = []
        for c in range(3):
            rows = list(values[c]) + [jnp.zeros((8, LANES), F32)]
            hi, lo = split(jnp.concatenate(rows, axis=0))
            sides.append(jnp.concatenate([hi, lo, hi], axis=0))
        along = jnp.dot(
            w1[...], jnp.concatenate(sides, axis=1), preferred_element_type=F32
        )
        tensor = []
        for c in range(3):
            ref_dir = [
                along[r * points : (r + 1) * points, c * LANES : (c + 1) * LANES]
                for r in range(3)
            ]
            tensor.append(
                [
                    ref_dir[0] * jac_ref[e : e + 1, :]
                    + ref_dir[1] * jac_ref[3 + e : 4 + e, :]
                    + ref_dir[2] * jac_ref[6 + e : 7 + e, :]
                    for e in range(3)
                ]
            )
        return tensor

    def stiffness(values):
        for c in range(3):
            for i in range(tiles):
                start = c * padded + 8 * i
                at_el[start : start + 8, :] = values[c][i]
        sums = [None] * pairs_el
        for n in range(nodes_el):
            for cp in range(3):
                here = c_row(cp * padded + n)
                for j in range(pairs_el):
                    start = ((n % 2) * 3 + cp) * 4 * padded + 8 * j
                    term = kmat[n // 2, start : start + 8, :] * here
                    sums[j] = term if sums[j] is None else sums[j] + term
        return [pack(x) for x in sums]

    def c_row(i):
        return jnp.broadcast_to(at_el[i : i + 1, :], (8, LANES))

    def record(t):
        comps = [
            t[0][0],
            t[1][1],
            t[2][2],
            0.5 * (t[1][2] + t[2][1]),
            0.5 * (t[0][2] + t[2][0]),
            0.5 * (t[0][1] + t[1][0]),
        ]
        for c, value in enumerate(comps):
            snap[pl.ds(c, points, stride=8), :] = value

    def build_route():
        ranks = jnp.concatenate(
            [rank_ref[:, q * LANES : (q + 1) * LANES] for q in range(points)], axis=0
        )
        turned = jnp.concatenate(
            [ranks.astype(F32), jnp.zeros((LANES - points, LANES), F32)], axis=0
        ).T.astype(jnp.int32)
        upper = jnp.right_shift(ranks, 7)
        place_row = lax.broadcasted_iota(jnp.int32, (points, LANES), 0)
        lane_value = lax.broadcasted_iota(jnp.int32, (points, LANES), 1).astype(F32)
        sides = []
        for q in range(points):
            low = jnp.broadcast_to(turned[:, q : q + 1], (LANES, LANES))
            low = jnp.bitwise_and(low, LANES - 1)
            spread[q * LANES : (q + 1) * LANES, :] = jnp.where(low == lane, 1.0, 0.0).astype(BF16)
            mine_here = place_row == jnp.broadcast_to(upper[q : q + 1, :], (points, LANES))
            sides.append(
                jnp.concatenate(
                    [jnp.where(mine_here, float(q), 0.0), jnp.where(mine_here, lane_value, 0.0)],
                    axis=0,
                ).astype(BF16)
            )
        route[...] = jnp.dot(
            jnp.concatenate(sides, axis=1), spread[...], preferred_element_type=F32
        ).astype(jnp.int32)

    def in_order():
        sources = [snap[8 * q : 8 * q + 8, :] for q in range(points)]
        out = []
        for k in range(points):
            origin = jnp.broadcast_to(route[k : k + 1, :], (8, LANES))
            at = jnp.broadcast_to(route[points + k : points + k + 1, :], (8, LANES))
            value = pick_lanes(sources[0], at)
            for q in range(1, points):
                value = jnp.where(origin == q, pick_lanes(sources[q], at), value)
            out.append(value)
        return out

    def keep(parity):
        for k, value in enumerate(in_order()):
            mixed[k, pl.ds(parity, 8, stride=2), :] = value

    velocity = wav_ref[0] * source * half_inverse
    displace = time_step * velocity

    def mine(i):
        return pl.ds(pl.multiple_of(i * block, block), block)

    def parcel(chunk, i, column, target):
        return pltpu.make_async_remote_copy(
            src_ref=pair.at[chunk, :, mine(target)],
            dst_ref=pair_in.at[chunk, :, mine(column)],
            send_sem=out_send_sem.at[chunk, i],
            recv_sem=out_recv_sem.at[chunk, i],
            device_id=(g, target),
            device_id_type=MESH,
        )

    def dispatch(make, local):
        for i in range(1, writers):
            make(i, d, lax.rem(my_d + i, writers)).start()

        @pl.when(other_core)
        def _():
            make(0, d, my_d).start()

        pl.when(jnp.logical_not(other_core))(local)

    def collect(make):
        for i in range(1, writers):
            origin = lax.rem(my_d - i + writers, writers)
            make(i, along(origin), origin).wait_recv()
            make(i, d, lax.rem(my_d + i, writers)).wait_send()

        @pl.when(other_core)
        def _():
            make(0, d, my_d).wait_recv()
            make(0, d, my_d).wait_send()

    def send_pair(chunk):
        for k in range(points):
            pair[chunk, :, k * LANES : (k + 1) * LANES] = mixed[k].astype(BF16)

        def local():
            pair_in[chunk, :, mine(d)] = pair[chunk, :, mine(my_d)]

        dispatch(functools.partial(parcel, chunk), local)

    def merge(chunk):
        collect(functools.partial(parcel, chunk))
        for c in range(6):
            out_ref[c, 2 * chunk : 2 * chunk + 2, :] = pair_in[chunk, 2 * c : 2 * c + 2, :]

    def launch(t, odd, values, got, displace, velocity, extra):
        packs = stiffness(values)
        send_shared(face_forces(packs), odd)
        record(gradient(values))
        if got is not None:
            change = half_inverse * at_nodes(got)
            velocity = velocity - change
            displace = displace - time_step * change
        velocity = velocity + half_inverse * (wav_ref[t] * source - node_forces(packs))
        displace = displace + time_step * velocity
        values = gather(displace)
        extra()
        keep(1 - odd)
        return values, displace, velocity

    state = launch(1, 1, gather(displace), None, displace, velocity, build_route)

    inv_f = inv_idx.astype(F32)
    place = [x.astype(jnp.int32) for x in at_elements(lambda b: inv_f[4 * b : 4 * b + 1, :])]
    coef = (-time_step) * half_inverse * inv_has
    coef = at_elements(lambda b: coef[4 * b : 4 * b + 1, :])

    def corrected(values, got):
        out = []
        for c in range(3):
            row = jnp.broadcast_to(got[c : c + 1, :], (8, LANES))
            out.append(
                tuple(values[c][i] + pick_lanes(row, place[i]) * coef[i] for i in range(3))
            )
        return tuple(out)

    def advance(t, odd, state):
        values, displace, velocity = state
        got = shared_sum(1 - odd)
        return launch(t, odd, corrected(values, got), got, displace, velocity, lambda: None)

    def two_steps(i, state):
        state = advance(2 * i, 0, state)
        send_pair(i - 1)
        return advance(2 * i + 1, 1, state)

    state = lax.fori_loop(1, chunks, two_steps, state)
    for chunk in range(chunks - 2):
        merge(chunk)
    got = shared_sum(1)
    record(gradient(corrected(state[0], got)))
    keep(1)
    send_pair(chunks - 1)
    merge(chunks - 2)
    merge(chunks - 1)


def solution(mesh):
    groups, writers = mesh.shape["grp"], mesh.shape["dom"]

    def shards(
        connect,
        interface_nodes,
        neighbours,
        point_rank,
        shape_grad,
        inverse_jacobian,
        lame_moduli,
        point_weights,
        mass_elem,
        source_pattern,
        wavelet,
    ):
        nodes_el, elements = connect.shape
        points = point_weights.shape[0]
        point_count = point_rank.shape[1]
        steps = wavelet.shape[0]
        padded = -(-nodes_el // 8) * 8
        vmem = pl.BlockSpec(memory_space=pltpu.VMEM)
        smem = pl.BlockSpec(memory_space=pltpu.SMEM)
        hbm = pl.BlockSpec(memory_space=pl.ANY)
        sharded = (
            connect,
            interface_nodes,
            neighbours,
            point_rank,
            inverse_jacobian,
            lame_moduli,
            point_weights,
            mass_elem,
            source_pattern,
        )
        ordered = pl.pallas_call(
            functools.partial(kernel, groups, writers, steps, nodes_el),
            out_shape=pltpu.VMEM((6, steps, point_count), BF16),
            in_specs=[hbm] * len(sharded) + [vmem, smem],
            out_specs=vmem,
            scratch_shapes=[pltpu.VMEM(a.shape, a.dtype) for a in sharded] * 2
            + [pltpu.SemaphoreType.DMA((len(sharded),))] * 3
            + [
                pltpu.VMEM((nodes_el // 2 * LANES, 2 * LANES), BF16),
                pltpu.VMEM((nodes_el // 2 * LANES, 2 * LANES), BF16),
                pltpu.VMEM((nodes_el // 2 * (source_pattern.shape[1] // LANES) * 16, LANES), BF16),
                pltpu.VMEM((3, padded, LANES), F32),
                pltpu.VMEM((nodes_el // 2, 18 * padded, LANES), BF16),
                pltpu.VMEM((LANES, LANES), BF16),
                pltpu.VMEM((nodes_el // 2, 24 * padded, LANES), F32),
                pltpu.VMEM((3 * padded, LANES), F32),
                pltpu.VMEM((3 * points, 96), BF16),
                pltpu.VMEM((8 * points, LANES), F32),
                pltpu.VMEM((points * LANES, LANES), BF16),
                pltpu.VMEM((2 * points, LANES), jnp.int32),
                pltpu.VMEM((points, 16, LANES), F32),
                pltpu.VMEM((steps // 2, 16, point_count), BF16),
                pltpu.VMEM((steps // 2, 16, point_count), BF16),
                pltpu.VMEM((2, 8, LANES), F32),
                pltpu.VMEM((2, 4, 8, LANES), F32),
                pltpu.SemaphoreType.DMA((2, 4)),
                pltpu.SemaphoreType.DMA((2, 4)),
                pltpu.SemaphoreType.DMA((steps // 2, writers)),
                pltpu.SemaphoreType.DMA((steps // 2, writers)),
            ],
            compiler_params=pltpu.CompilerParams(
                collective_id=0, has_side_effects=True, vmem_limit_bytes=56 * 1024 * 1024
            ),
            name="window",
        )(
            *sharded,
            shape_grad.T,
            wavelet,
        )
        return ordered.transpose(1, 0, 2)

    placed = (
        P(None, ("grp", "dom")),
        P(("grp", "dom"), None, None),
        P(("grp", "dom"), None),
        P(("grp", "dom"), None),
        P(),
        P(None, ("grp", "dom")),
        P(None, ("grp", "dom")),
        P(None, ("grp", "dom")),
        P(None, ("grp", "dom")),
        P(None, ("grp", "dom")),
        P(),
    )
    return jax.shard_map(
        shards, mesh=mesh, in_specs=placed, out_specs=P(None, None, ("grp", "dom")), check_vma=False
    )
```

```python
import functools

import jax
import jax.numpy as jnp
from jax import lax
from jax.experimental import pallas as pl
from jax.experimental.pallas import tpu as pltpu
from jax.sharding import PartitionSpec as P

MESH = pl.DeviceIdType.MESH
F32 = jnp.float32
BF16 = jnp.bfloat16
time_step = 0.5
LANES = 128


def split(x):
    hi = x.astype(BF16)
    return hi, (x - hi.astype(F32)).astype(BF16)


def pick_lanes(x, idx):
    return jnp.take_along_axis(x, idx, axis=1, mode="promise_in_bounds")


def kernel(
    groups,
    writers,
    steps,
    nodes_el,
    conn_in,
    faces_in,
    nb_in,
    rank_in,
    jac_in,
    lame_in,
    pw_in,
    mass_in,
    src_in,
    gradt_in,
    wav_in,
    out_ref,
    conn_ref,
    faces_ref,
    nb_ref,
    rank_ref,
    jac_ref,
    lame_ref,
    pw_ref,
    mass_ref,
    src_ref,
    conn_own,
    faces_own,
    nb_own,
    rank_own,
    jac_own,
    lame_own,
    pw_own,
    mass_own,
    src_own,
    gradt_ref,
    wav_ref,
    move_sem,
    move_send_sem,
    move_recv_sem,
    at_face,
    at_node,
    hmask,
    basis,
    products,
    pww,
    kmat,
    at_el,
    w1,
    snap,
    spread,
    route,
    mixed,
    pair,
    pair_in,
    send,
    recv,
    send_sem,
    recv_sem,
    out_send_sem,
    out_recv_sem,
):
    my_g = lax.axis_index("grp")
    my_d = lax.axis_index("dom")
    points = pw_ref.shape[0]
    block = out_ref.shape[2] // writers
    blocks = src_ref.shape[1] // LANES

    def along(w):
        if writers % 4:
            return w
        return w + lax.rem(w // 2, 2) * (1 - 2 * lax.rem(w, 2))

    def across(g, w):
        if groups % 2:
            return g
        return g + lax.rem(w, 2) * (1 - 2 * lax.rem(g, 2))

    def host(g, w):
        return across(g, w), along(w)

    d = along(my_d)
    g = across(my_g, d)
    stays = (g == my_g) & (d == my_d)
    moves = jnp.logical_not(stays)
    other_core = g != my_g
    target = host(my_g, my_d)

    has = (g > 0, g < groups - 1, d > 0, d < writers - 1)
    where_to = (host(g - 1, d), host(g + 1, d), host(g, d - 1), host(g, d + 1))

    arrays = (
        (conn_in, conn_own, conn_ref),
        (faces_in, faces_own, faces_ref),
        (mass_in, mass_own, mass_ref),
        (src_in, src_own, src_ref),
        (nb_in, nb_own, nb_ref),
        (pw_in, pw_own, pw_ref),
        (jac_in, jac_own, jac_ref),
        (lame_in, lame_own, lame_ref),
        (rank_in, rank_own, rank_ref),
    )

    def fetch(i, kept):
        return pltpu.make_async_copy(
            arrays[i][0], arrays[i][2 if kept else 1], move_sem.at[i]
        )

    def move(i):
        return pltpu.make_async_remote_copy(
            src_ref=arrays[i][1],
            dst_ref=arrays[i][2],
            send_sem=move_send_sem.at[i],
            recv_sem=move_recv_sem.at[i],
            device_id=target,
            device_id_type=MESH,
        )

    recv[...] = jnp.zeros_like(recv)
    barrier = pltpu.get_barrier_semaphore()
    shared = (
        pltpu.make_async_copy(gradt_in, gradt_ref, move_sem.at[len(arrays)]),
        pltpu.make_async_copy(wav_in, wav_ref, move_sem.at[len(arrays) + 1]),
    )

    @pl.when(moves)
    def _():
        pl.semaphore_signal(barrier, inc=1, device_id=(g, d), device_id_type=MESH)

    for k in range(4):

        @pl.when(has[k])
        def _():
            pl.semaphore_signal(barrier, inc=1, device_id=where_to[k], device_id_type=MESH)

    near = writers <= 4
    for i in range(0 if near else writers):
        origin_d = lax.rem(my_d + i, writers)
        origin = (across(my_g, along(origin_d)), origin_d)

        def greet():
            pl.semaphore_signal(barrier, inc=1, device_id=origin, device_id_type=MESH)

        if i:
            greet()
        else:
            pl.when(other_core)(greet)

    @pl.when(stays)
    def _():
        for i in range(len(arrays)):
            fetch(i, True).start()

    @pl.when(moves)
    def _():
        for i in range(len(arrays)):
            fetch(i, False).start()

    for copy in shared:
        copy.start()
    expected = moves.astype(jnp.int32)
    if not near:
        expected = expected + other_core.astype(jnp.int32) + writers - 1
    for k in range(4):
        expected = expected + has[k].astype(jnp.int32)
    pl.semaphore_wait(barrier, expected)

    @pl.when(moves)
    def _():
        for i in range(len(arrays)):
            fetch(i, False).wait()
            move(i).start()

    def landed(lo, hi):
        @pl.when(stays)
        def _():
            for i in range(lo, hi):
                fetch(i, True).wait()

        @pl.when(moves)
        def _():
            for i in range(lo, hi):
                move(i).wait_recv()
                move(i).wait_send()


    lane = lax.broadcasted_iota(jnp.int32, (LANES, LANES), 1)
    row8 = lax.broadcasted_iota(jnp.int32, (8, LANES), 0)
    row16 = lax.broadcasted_iota(jnp.int32, (16, LANES), 0)
    pairs_el = nodes_el // 2
    padded = -(-nodes_el // 8) * 8
    tiles = padded // 8

    for copy in shared:
        copy.wait()
    gradt = gradt_ref[...]
    depth = 3 * points
    hi = gradt.astype(BF16).astype(F32)
    lo = gradt - hi
    gap = jnp.zeros((32 - nodes_el, depth), F32)
    tall = jnp.concatenate([hi, gap, hi, gap, lo, gap, jnp.zeros((32, depth), F32)], axis=0)
    tall = jnp.concatenate([tall, jnp.zeros((LANES, LANES - depth), F32)], axis=1)
    w1[...] = tall.T[0:depth, 0:96].astype(BF16)

    lanes = lax.broadcasted_iota(jnp.int32, (padded, LANES), 1)
    base = jnp.concatenate([gradt, jnp.zeros((padded - nodes_el, depth), F32)], axis=0)
    base = jnp.concatenate([base, jnp.zeros((padded, LANES - depth), F32)], axis=1)
    own_dir = []
    for r in range(3):
        x = pltpu.roll(base, LANES - r * points, 1) if r else base
        x = jnp.where(lanes < points, x, 0.0)
        x = x + pltpu.roll(x, points, 1) + pltpu.roll(x, 2 * points, 1)
        own_dir.append(x)
        basis[r] = x

    def multiply_pairs(m, carry):
        for rp in range(3):
            parts = []
            for p in range(2):
                other = basis[rp, pl.ds(2 * m + p, 1), :]
                for r in range(3):
                    product = own_dir[r] * other
                    high = product.astype(BF16).astype(F32)
                    parts.append(jnp.where(lanes < 2 * points, high, product - high))
            rows = 6 * padded
            products[m, rp * rows : (rp + 1) * rows, :] = jnp.concatenate(
                parts, axis=0
            ).astype(BF16)
        return carry

    lax.fori_loop(0, pairs_el, multiply_pairs, 0)

    def clear(m, carry):
        kmat[m] = jnp.zeros(kmat.shape[1:], F32)
        return carry

    lax.fori_loop(0, pairs_el, clear, 0)

    chunks = steps // 2
    snap[...] = jnp.zeros_like(snap)

    landed(0, 2)
    faces = faces_ref[0].astype(F32)
    face_row = jnp.concatenate([faces[k : k + 1, :] for k in range(4)], axis=1)
    face_swap = jnp.concatenate([faces[k ^ 1 : (k ^ 1) + 1, :] for k in range(4)], axis=1)
    face_swap = jnp.broadcast_to(face_swap.astype(jnp.int32), (LANES, LANES))
    face_low = jnp.bitwise_and(face_swap[0:8], LANES - 1)
    face_high = jnp.right_shift(face_swap[0:8], 7)

    columns = jnp.concatenate(
        [conn_ref[...].astype(F32), jnp.zeros((LANES - nodes_el, LANES), F32)], axis=0
    ).T.astype(jnp.int32)

    def column(n):
        return jnp.broadcast_to(columns[:, n : n + 1], (LANES, LANES))

    def spot(n):
        j, p = n // 2, n % 2
        return slice(j * LANES, (j + 1) * LANES), slice(p * LANES, (p + 1) * LANES)

    for n in range(nodes_el):
        at_face[spot(n)] = jnp.where(column(n) == face_swap, 1.0, 0.0).astype(BF16)

    def pack(x):
        high = x.astype(BF16).astype(F32)
        return jnp.concatenate([high, x - high], axis=0).astype(BF16)

    def face_forces(packs):
        res = jnp.dot(
            jnp.concatenate(packs, axis=1), at_face[...], preferred_element_type=F32
        )
        res = res[0:8] + res[8:16]
        mixed = jnp.where(row8 < 4, res[:, 0:LANES], res[:, LANES:])
        return mixed + pltpu.roll(mixed, 4, 0)

    def node_forces(packs):
        sides = []
        for b in range(blocks):
            sides.append(
                jnp.concatenate(
                    [
                        packs[j] * hmask[(j * blocks + b) * 16 : (j * blocks + b + 1) * 16, :]
                        for j in range(pairs_el)
                    ],
                    axis=1,
                )
            )
        res = jnp.dot(
            jnp.concatenate(sides, axis=0), at_node[...], preferred_element_type=F32
        )
        halves = []
        for b in range(blocks):
            one = res[16 * b : 16 * b + 8] + res[16 * b + 8 : 16 * b + 16]
            even, odd = one[:, 0:LANES], one[:, LANES:]
            if b % 2:
                halves.append(pltpu.roll(even, 4, 0) + odd)
            else:
                halves.append(even + pltpu.roll(odd, 4, 0))
        return jnp.concatenate(
            [jnp.where(row8 < 4, halves[b], halves[b + 1]) for b in range(0, blocks, 2)],
            axis=0,
        )

    landed(2, 5)
    quarter = jnp.right_shift(lax.broadcasted_iota(jnp.int32, (8, LANES), 1), 5)
    nb = nb_ref[...].astype(F32)
    recv_mask = [jnp.where(quarter == k, nb[:, k : k + 1], 0.0) for k in range(4)]

    def copies(slot):
        return [
            pltpu.make_async_remote_copy(
                src_ref=send.at[slot, 0:4],
                dst_ref=recv.at[slot, k ^ 1, 0:4],
                send_sem=send_sem.at[slot, k],
                recv_sem=recv_sem.at[slot, k ^ 1],
                device_id=where_to[k],
                device_id_type=MESH,
            )
            for k in range(4)
        ]

    def arrivals(slot):
        return [
            pltpu.make_async_remote_copy(
                src_ref=send.at[slot, 0:4],
                dst_ref=recv.at[slot, k, 0:4],
                send_sem=send_sem.at[slot, k],
                recv_sem=recv_sem.at[slot, k],
                device_id=where_to[k],
                device_id_type=MESH,
            )
            for k in range(4)
        ]

    def send_shared(message, slot):
        send[slot] = message
        for k, copy in enumerate(copies(slot)):

            @pl.when(has[k])
            def _():
                copy.start()

    def shared_sum(slot):
        for k, copy in enumerate(arrivals(slot)):

            @pl.when(has[k])
            def _():
                copy.wait_recv()
                copy.wait_send()

        got = recv[slot, 0] * recv_mask[0]
        for k in range(1, 4):
            got = got + recv[slot, k] * recv_mask[k]
        return got

    masses = []
    for n in range(0, nodes_el, 2):
        mass = jnp.where(row8 == 3, mass_ref[n : n + 1, :], 0.0)
        masses.append(pack(mass + jnp.where(row8 == 7, mass_ref[n + 1 : n + 2, :], 0.0)))
    src_rows = []
    for b in range(blocks):
        src_rows.append(src_ref[:, b * LANES : (b + 1) * LANES])
        src_rows.append(jnp.zeros((1, LANES), F32))
    at_faces = jnp.zeros((8, LANES), F32)
    for b in range(blocks):
        rows = jnp.concatenate([src_rows[2 * b], jnp.zeros((5, LANES), F32)], axis=0)
        at_faces = jnp.where(face_high == b, pick_lanes(rows, face_low), at_faces)
    send_shared(face_forces(masses) + at_faces, 0)

    conn_low = jnp.bitwise_and(conn_ref[...], LANES - 1)
    conn_high = jnp.right_shift(conn_ref[...], 7)
    for n in range(nodes_el):
        low_column = jnp.bitwise_and(column(n), LANES - 1)
        at_node[spot(n)] = jnp.where(low_column == lane, 1.0, 0.0).astype(BF16)
    for j in range(pairs_el):
        two = [
            jnp.broadcast_to(conn_high[n : n + 1, :], (4, LANES)) for n in (2 * j, 2 * j + 1)
        ]
        two = jnp.concatenate(two * 2, axis=0)
        for b in range(blocks):
            hmask[(j * blocks + b) * 16 : (j * blocks + b + 1) * 16, :] = jnp.where(
                two == b, 1.0, 0.0
            ).astype(BF16)
    first = node_forces(masses) + jnp.concatenate(src_rows, axis=0)

    face_col = jnp.broadcast_to(face_row, (LANES, LANES)).T
    position = lax.broadcasted_iota(jnp.int32, (LANES, LANES), 0).astype(F32)
    inv_rows = []
    has_rows = []
    for b in range(blocks):
        hit = jnp.where(face_col == (lane + b * LANES).astype(F32), 1.0, 0.0)
        inv_rows.append(
            jnp.broadcast_to(jnp.sum(hit * position, axis=0, keepdims=True), (4, LANES))
        )
        has_rows.append(jnp.broadcast_to(jnp.sum(hit, axis=0, keepdims=True), (4, LANES)))
    inv_idx = jnp.concatenate(inv_rows, axis=0).astype(jnp.int32)
    inv_has = jnp.concatenate(has_rows, axis=0)

    def at_nodes(got):
        got = got + pltpu.roll(got, 4, 0)
        added = jnp.concatenate(
            [pick_lanes(got, inv_idx[0:8]), pick_lanes(got, inv_idx[8:16])], axis=0
        )
        return added * inv_has

    landed(5, len(arrays))
    weight = pw_ref[...]
    hi = weight.astype(BF16).astype(F32)
    pww[...] = jnp.concatenate(
        [hi, weight - hi, hi, jnp.zeros((LANES - depth, LANES), F32)], axis=0
    ).astype(BF16)
    jac = [jnp.broadcast_to(jac_ref[i : i + 1, :], (8, LANES)) for i in range(9)]
    lam = jnp.broadcast_to(lame_ref[0:1, :], (8, LANES))
    mu = jnp.broadcast_to(lame_ref[1:2, :], (8, LANES))

    def form_stiffness(m, carry):
        moments = jnp.dot(products[m], pww[...], preferred_element_type=F32)
        for p in range(2):
            for i in range(tiles):

                def moment(r, rp):
                    start = ((rp * 2 + p) * 3 + r) * padded + 8 * i
                    return moments[start : start + 8]

                half = [
                    [
                        jac[a] * moment(0, rp) + jac[3 + a] * moment(1, rp) + jac[6 + a] * moment(2, rp)
                        for rp in range(3)
                    ]
                    for a in range(3)
                ]
                full = [
                    [
                        jac[b] * half[a][0] + jac[3 + b] * half[a][1] + jac[6 + b] * half[a][2]
                        for b in range(3)
                    ]
                    for a in range(3)
                ]
                trace = mu * (full[0][0] + full[1][1] + full[2][2])
                for c in range(3):
                    for cp in range(3):
                        value = mu * full[cp][c] + lam * full[c][cp]
                        if c == cp:
                            value = value + trace
                        start = (p * 3 + cp) * 4 * padded + 32 * i + c
                        kmat[m, pl.ds(start, 8, stride=4), :] = value
        return carry

    group = 5 if pairs_el % 5 == 0 else 1

    def form_group(i, carry):
        for k in range(group):
            form_stiffness(i * group + k, carry)
        return carry

    lax.fori_loop(0, pairs_el // group, form_group, 0)

    first = first + at_nodes(shared_sum(0))
    axis_row = jnp.bitwise_and(row16, 3) < 3
    source = jnp.where(axis_row, first, 0.0)
    total = jnp.concatenate(
        [jnp.broadcast_to(first[4 * b + 3 : 4 * b + 4, :], (4, LANES)) for b in range(blocks)],
        axis=0,
    )
    half_inverse = jnp.where(axis_row, time_step / total, 0.0)

    spare = jnp.zeros((24 - nodes_el, LANES), jnp.int32)
    conn_low = jnp.concatenate([conn_low, spare], axis=0)
    conn_high = jnp.concatenate([conn_high, spare], axis=0)
    low = [conn_low[8 * i : 8 * i + 8, :] for i in range(3)]
    high = [conn_high[8 * i : 8 * i + 8, :] for i in range(3)]

    def at_elements(rows_of):
        out = []
        for i in range(3):
            acc = None
            for b in range(blocks):
                val = pick_lanes(jnp.broadcast_to(rows_of(b), (8, LANES)), low[i])
                acc = val if b == 0 else jnp.where(high[i] == b, val, acc)
            out.append(acc)
        return out

    def gather(u):
        return tuple(
            tuple(at_elements(lambda b: u[4 * b + c : 4 * b + c + 1, :])) for c in range(3)
        )

    def gradient(values):
        sides = []
        for c in range(3):
            rows = list(values[c]) + [jnp.zeros((8, LANES), F32)]
            hi, lo = split(jnp.concatenate(rows, axis=0))
            sides.append(jnp.concatenate([hi, lo, hi], axis=0))
        along = jnp.dot(
            w1[...], jnp.concatenate(sides, axis=1), preferred_element_type=F32
        )
        tensor = []
        for c in range(3):
            ref_dir = [
                along[r * points : (r + 1) * points, c * LANES : (c + 1) * LANES]
                for r in range(3)
            ]
            tensor.append(
                [
                    ref_dir[0] * jac_ref[e : e + 1, :]
                    + ref_dir[1] * jac_ref[3 + e : 4 + e, :]
                    + ref_dir[2] * jac_ref[6 + e : 7 + e, :]
                    for e in range(3)
                ]
            )
        return tensor

    def stiffness(values):
        for c in range(3):
            for i in range(tiles):
                start = c * padded + 8 * i
                at_el[start : start + 8, :] = values[c][i]
        sums = [None] * pairs_el
        for n in range(nodes_el):
            for cp in range(3):
                here = c_row(cp * padded + n)
                for j in range(pairs_el):
                    start = ((n % 2) * 3 + cp) * 4 * padded + 8 * j
                    term = kmat[n // 2, start : start + 8, :] * here
                    sums[j] = term if sums[j] is None else sums[j] + term
        return [pack(x) for x in sums]

    def c_row(i):
        return jnp.broadcast_to(at_el[i : i + 1, :], (8, LANES))

    def record(t):
        comps = [
            t[0][0],
            t[1][1],
            t[2][2],
            0.5 * (t[1][2] + t[2][1]),
            0.5 * (t[0][2] + t[2][0]),
            0.5 * (t[0][1] + t[1][0]),
        ]
        for c, value in enumerate(comps):
            snap[pl.ds(c, points, stride=8), :] = value

    def build_route():
        ranks = jnp.concatenate(
            [rank_ref[:, q * LANES : (q + 1) * LANES] for q in range(points)], axis=0
        )
        turned = jnp.concatenate(
            [ranks.astype(F32), jnp.zeros((LANES - points, LANES), F32)], axis=0
        ).T.astype(jnp.int32)
        upper = jnp.right_shift(ranks, 7)
        place_row = lax.broadcasted_iota(jnp.int32, (points, LANES), 0)
        lane_value = lax.broadcasted_iota(jnp.int32, (points, LANES), 1).astype(F32)
        sides = []
        for q in range(points):
            low = jnp.broadcast_to(turned[:, q : q + 1], (LANES, LANES))
            low = jnp.bitwise_and(low, LANES - 1)
            spread[q * LANES : (q + 1) * LANES, :] = jnp.where(low == lane, 1.0, 0.0).astype(BF16)
            mine_here = place_row == jnp.broadcast_to(upper[q : q + 1, :], (points, LANES))
            sides.append(
                jnp.concatenate(
                    [jnp.where(mine_here, float(q), 0.0), jnp.where(mine_here, lane_value, 0.0)],
                    axis=0,
                ).astype(BF16)
            )
        route[...] = jnp.dot(
            jnp.concatenate(sides, axis=1), spread[...], preferred_element_type=F32
        ).astype(jnp.int32)

    def in_order():
        sources = [snap[8 * q : 8 * q + 8, :] for q in range(points)]
        out = []
        for k in range(points):
            origin = jnp.broadcast_to(route[k : k + 1, :], (8, LANES))
            at = jnp.broadcast_to(route[points + k : points + k + 1, :], (8, LANES))
            value = pick_lanes(sources[0], at)
            for q in range(1, points):
                value = jnp.where(origin == q, pick_lanes(sources[q], at), value)
            out.append(value)
        return out

    def keep(parity):
        for k, value in enumerate(in_order()):
            mixed[k, pl.ds(parity, 8, stride=2), :] = value

    velocity = wav_ref[0] * source * half_inverse
    displace = time_step * velocity

    def mine(i):
        return pl.ds(pl.multiple_of(i * block, block), block)

    def parcel(chunk, i, column, target):
        return pltpu.make_async_remote_copy(
            src_ref=pair.at[chunk, :, mine(target)],
            dst_ref=pair_in.at[chunk, :, mine(column)],
            send_sem=out_send_sem.at[chunk, i],
            recv_sem=out_recv_sem.at[chunk, i],
            device_id=(g, target),
            device_id_type=MESH,
        )

    def dispatch(make, local):
        for i in range(1, writers):
            make(i, d, lax.rem(my_d + i, writers)).start()

        @pl.when(other_core)
        def _():
            make(0, d, my_d).start()

        pl.when(jnp.logical_not(other_core))(local)

    def collect(make):
        for i in range(1, writers):
            origin = lax.rem(my_d - i + writers, writers)
            make(i, along(origin), origin).wait_recv()
            make(i, d, lax.rem(my_d + i, writers)).wait_send()

        @pl.when(other_core)
        def _():
            make(0, d, my_d).wait_recv()
            make(0, d, my_d).wait_send()

    def close_pair(chunk):
        for k in range(points):
            pair[chunk, :, k * LANES : (k + 1) * LANES] = mixed[k].astype(BF16)

    def send_pair(chunk):
        def local():
            pair_in[chunk, :, mine(d)] = pair[chunk, :, mine(my_d)]

        dispatch(functools.partial(parcel, chunk), local)

    def merge(chunk):
        collect(functools.partial(parcel, chunk))
        for c in range(6):
            out_ref[c, 2 * chunk : 2 * chunk + 2, :] = pair_in[chunk, 2 * c : 2 * c + 2, :]

    def launch(t, odd, values, got, displace, velocity, early, extra):
        packs = stiffness(values)
        send_shared(face_forces(packs), odd)
        early()
        record(gradient(values))
        if got is not None:
            change = half_inverse * at_nodes(got)
            velocity = velocity - change
            displace = displace - time_step * change
        velocity = velocity + half_inverse * (wav_ref[t] * source - node_forces(packs))
        displace = displace + time_step * velocity
        values = gather(displace)
        extra()
        keep(1 - odd)
        return values, displace, velocity

    def nothing():
        return None

    state = launch(
        1, 1, gather(displace), None, displace, velocity, nothing, build_route
    )

    inv_f = inv_idx.astype(F32)
    place = [x.astype(jnp.int32) for x in at_elements(lambda b: inv_f[4 * b : 4 * b + 1, :])]
    coef = (-time_step) * half_inverse * inv_has
    coef = at_elements(lambda b: coef[4 * b : 4 * b + 1, :])

    def corrected(values, got):
        out = []
        for c in range(3):
            row = jnp.broadcast_to(got[c : c + 1, :], (8, LANES))
            out.append(
                tuple(values[c][i] + pick_lanes(row, place[i]) * coef[i] for i in range(3))
            )
        return tuple(out)

    def advance(t, odd, state, early):
        values, displace, velocity = state
        got = shared_sum(1 - odd)
        return launch(t, odd, corrected(values, got), got, displace, velocity, early, nothing)

    def two_steps(i, state):
        def early():
            pl.when(i >= 2)(lambda: send_pair(i - 2))

        state = advance(2 * i, 0, state, early)
        close_pair(i - 1)
        return advance(2 * i + 1, 1, state, nothing)

    state = lax.fori_loop(1, chunks, two_steps, state)
    send_pair(chunks - 2)
    for chunk in range(chunks - 2):
        merge(chunk)
    got = shared_sum(1)
    record(gradient(corrected(state[0], got)))
    keep(1)
    close_pair(chunks - 1)
    send_pair(chunks - 1)
    merge(chunks - 2)
    merge(chunks - 1)


def solution(mesh):
    groups, writers = mesh.shape["grp"], mesh.shape["dom"]

    def shards(
        connect,
        interface_nodes,
        neighbours,
        point_rank,
        shape_grad,
        inverse_jacobian,
        lame_moduli,
        point_weights,
        mass_elem,
        source_pattern,
        wavelet,
    ):
        nodes_el, elements = connect.shape
        points = point_weights.shape[0]
        point_count = point_rank.shape[1]
        steps = wavelet.shape[0]
        padded = -(-nodes_el // 8) * 8
        vmem = pl.BlockSpec(memory_space=pltpu.VMEM)
        hbm = pl.BlockSpec(memory_space=pl.ANY)
        sharded = (
            connect,
            interface_nodes,
            neighbours,
            point_rank,
            inverse_jacobian,
            lame_moduli,
            point_weights,
            mass_elem,
            source_pattern,
        )
        ordered = pl.pallas_call(
            functools.partial(kernel, groups, writers, steps, nodes_el),
            out_shape=pltpu.VMEM((6, steps, point_count), BF16),
            in_specs=[hbm] * (len(sharded) + 2),
            out_specs=vmem,
            scratch_shapes=[pltpu.VMEM(a.shape, a.dtype) for a in sharded] * 2
            + [pltpu.VMEM(shape_grad.shape[::-1], F32), pltpu.SMEM(wavelet.shape, F32)]
            + [pltpu.SemaphoreType.DMA((len(sharded) + 2,))] * 3
            + [
                pltpu.VMEM((nodes_el // 2 * LANES, 2 * LANES), BF16),
                pltpu.VMEM((nodes_el // 2 * LANES, 2 * LANES), BF16),
                pltpu.VMEM((nodes_el // 2 * (source_pattern.shape[1] // LANES) * 16, LANES), BF16),
                pltpu.VMEM((3, padded, LANES), F32),
                pltpu.VMEM((nodes_el // 2, 18 * padded, LANES), BF16),
                pltpu.VMEM((LANES, LANES), BF16),
                pltpu.VMEM((nodes_el // 2, 24 * padded, LANES), F32),
                pltpu.VMEM((3 * padded, LANES), F32),
                pltpu.VMEM((3 * points, 96), BF16),
                pltpu.VMEM((8 * points, LANES), F32),
                pltpu.VMEM((points * LANES, LANES), BF16),
                pltpu.VMEM((2 * points, LANES), jnp.int32),
                pltpu.VMEM((points, 16, LANES), F32),
                pltpu.VMEM((steps // 2, 16, point_count), BF16),
                pltpu.VMEM((steps // 2, 16, point_count), BF16),
                pltpu.VMEM((2, 8, LANES), F32),
                pltpu.VMEM((2, 4, 8, LANES), F32),
                pltpu.SemaphoreType.DMA((2, 4)),
                pltpu.SemaphoreType.DMA((2, 4)),
                pltpu.SemaphoreType.DMA((steps // 2, writers)),
                pltpu.SemaphoreType.DMA((steps // 2, writers)),
            ],
            compiler_params=pltpu.CompilerParams(
                collective_id=0, has_side_effects=True, vmem_limit_bytes=56 * 1024 * 1024
            ),
            name="window",
        )(
            *sharded,
            shape_grad.T,
            wavelet,
        )
        return ordered.transpose(1, 0, 2)

    placed = (
        P(None, ("grp", "dom")),
        P(("grp", "dom"), None, None),
        P(("grp", "dom"), None),
        P(("grp", "dom"), None),
        P(),
        P(None, ("grp", "dom")),
        P(None, ("grp", "dom")),
        P(None, ("grp", "dom")),
        P(None, ("grp", "dom")),
        P(None, ("grp", "dom")),
        P(),
    )
    return jax.shard_map(
        shards, mesh=mesh, in_specs=placed, out_specs=P(None, None, ("grp", "dom")), check_vma=False
    )
```

```python
import functools

import jax
import jax.numpy as jnp
from jax import lax
from jax.experimental import pallas as pl
from jax.experimental.pallas import tpu as pltpu
from jax.sharding import PartitionSpec as P

MESH = pl.DeviceIdType.MESH
F32 = jnp.float32
BF16 = jnp.bfloat16
time_step = 0.5
LANES = 128


def split(x):
    hi = x.astype(BF16)
    return hi, (x - hi.astype(F32)).astype(BF16)


def pick_lanes(x, idx):
    return jnp.take_along_axis(x, idx, axis=1, mode="promise_in_bounds")


def kernel(
    groups,
    writers,
    steps,
    nodes_el,
    conn_in,
    faces_in,
    nb_in,
    rank_in,
    jac_in,
    lame_in,
    pw_in,
    mass_in,
    src_in,
    gradt_in,
    wav_in,
    out_ref,
    conn_ref,
    faces_ref,
    nb_ref,
    rank_ref,
    jac_ref,
    lame_ref,
    pw_ref,
    mass_ref,
    src_ref,
    conn_own,
    faces_own,
    nb_own,
    rank_own,
    jac_own,
    lame_own,
    pw_own,
    mass_own,
    src_own,
    gradt_ref,
    wav_ref,
    move_sem,
    move_send_sem,
    move_recv_sem,
    at_face,
    at_node,
    hmask,
    basis,
    products,
    pww,
    kmat,
    at_el,
    w1,
    snap,
    spread,
    route,
    mixed,
    pair,
    pair_in,
    send,
    recv,
    send_sem,
    recv_sem,
    out_send_sem,
    out_recv_sem,
):
    my_g = lax.axis_index("grp")
    my_d = lax.axis_index("dom")
    points = pw_ref.shape[0]
    block = out_ref.shape[2] // writers
    blocks = src_ref.shape[1] // LANES

    def along(w):
        if writers % 4:
            return w
        return w + lax.rem(w // 2, 2) * (1 - 2 * lax.rem(w, 2))

    def across(g, w):
        if groups % 2:
            return g
        return g + lax.rem(w, 2) * (1 - 2 * lax.rem(g, 2))

    def host(g, w):
        return across(g, w), along(w)

    d = along(my_d)
    g = across(my_g, d)
    stays = (g == my_g) & (d == my_d)
    moves = jnp.logical_not(stays)
    other_core = g != my_g
    target = host(my_g, my_d)

    has = (g > 0, g < groups - 1, d > 0, d < writers - 1)
    where_to = (host(g - 1, d), host(g + 1, d), host(g, d - 1), host(g, d + 1))

    arrays = (
        (conn_in, conn_own, conn_ref),
        (faces_in, faces_own, faces_ref),
        (mass_in, mass_own, mass_ref),
        (src_in, src_own, src_ref),
        (nb_in, nb_own, nb_ref),
        (pw_in, pw_own, pw_ref),
        (jac_in, jac_own, jac_ref),
        (lame_in, lame_own, lame_ref),
        (rank_in, rank_own, rank_ref),
    )

    def fetch(i, kept):
        return pltpu.make_async_copy(
            arrays[i][0], arrays[i][2 if kept else 1], move_sem.at[i]
        )

    def move(i):
        return pltpu.make_async_remote_copy(
            src_ref=arrays[i][1],
            dst_ref=arrays[i][2],
            send_sem=move_send_sem.at[i],
            recv_sem=move_recv_sem.at[i],
            device_id=target,
            device_id_type=MESH,
        )

    recv[...] = jnp.zeros_like(recv)
    barrier = pltpu.get_barrier_semaphore()
    shared = (
        pltpu.make_async_copy(gradt_in, gradt_ref, move_sem.at[len(arrays)]),
        pltpu.make_async_copy(wav_in, wav_ref, move_sem.at[len(arrays) + 1]),
    )

    @pl.when(moves)
    def _():
        pl.semaphore_signal(barrier, inc=1, device_id=(g, d), device_id_type=MESH)

    for k in range(4):

        @pl.when(has[k])
        def _():
            pl.semaphore_signal(barrier, inc=1, device_id=where_to[k], device_id_type=MESH)

    near = writers <= 4
    for i in range(0 if near else writers):
        origin_d = lax.rem(my_d + i, writers)
        origin = (across(my_g, along(origin_d)), origin_d)

        def greet():
            pl.semaphore_signal(barrier, inc=1, device_id=origin, device_id_type=MESH)

        if i:
            greet()
        else:
            pl.when(other_core)(greet)

    @pl.when(stays)
    def _():
        for i in range(len(arrays)):
            fetch(i, True).start()

    @pl.when(moves)
    def _():
        for i in range(len(arrays)):
            fetch(i, False).start()

    for copy in shared:
        copy.start()
    expected = moves.astype(jnp.int32)
    if not near:
        expected = expected + other_core.astype(jnp.int32) + writers - 1
    for k in range(4):
        expected = expected + has[k].astype(jnp.int32)
    pl.semaphore_wait(barrier, expected)

    @pl.when(moves)
    def _():
        for i in range(len(arrays)):
            fetch(i, False).wait()
            move(i).start()

    def landed(lo, hi):
        @pl.when(stays)
        def _():
            for i in range(lo, hi):
                fetch(i, True).wait()

        @pl.when(moves)
        def _():
            for i in range(lo, hi):
                move(i).wait_recv()
                move(i).wait_send()


    lane = lax.broadcasted_iota(jnp.int32, (LANES, LANES), 1)
    row8 = lax.broadcasted_iota(jnp.int32, (8, LANES), 0)
    row16 = lax.broadcasted_iota(jnp.int32, (16, LANES), 0)
    pairs_el = nodes_el // 2
    padded = -(-nodes_el // 8) * 8
    tiles = padded // 8

    for copy in shared:
        copy.wait()
    gradt = gradt_ref[...]
    depth = 3 * points
    hi = gradt.astype(BF16).astype(F32)
    lo = gradt - hi
    gap = jnp.zeros((32 - nodes_el, depth), F32)
    tall = jnp.concatenate([hi, gap, hi, gap, lo, gap, jnp.zeros((32, depth), F32)], axis=0)
    tall = jnp.concatenate([tall, jnp.zeros((LANES, LANES - depth), F32)], axis=1)
    w1[...] = tall.T[0:depth, 0:96].astype(BF16)

    lanes = lax.broadcasted_iota(jnp.int32, (padded, LANES), 1)
    base = jnp.concatenate([gradt, jnp.zeros((padded - nodes_el, depth), F32)], axis=0)
    base = jnp.concatenate([base, jnp.zeros((padded, LANES - depth), F32)], axis=1)
    own_dir = []
    for r in range(3):
        x = pltpu.roll(base, LANES - r * points, 1) if r else base
        x = jnp.where(lanes < points, x, 0.0)
        x = x + pltpu.roll(x, points, 1) + pltpu.roll(x, 2 * points, 1)
        own_dir.append(x)
        basis[r] = x

    def multiply_pairs(m, carry):
        for rp in range(3):
            parts = []
            for p in range(2):
                other = basis[rp, pl.ds(2 * m + p, 1), :]
                for r in range(3):
                    product = own_dir[r] * other
                    high = product.astype(BF16).astype(F32)
                    parts.append(jnp.where(lanes < 2 * points, high, product - high))
            rows = 6 * padded
            products[m, rp * rows : (rp + 1) * rows, :] = jnp.concatenate(
                parts, axis=0
            ).astype(BF16)
        return carry

    lax.fori_loop(0, pairs_el, multiply_pairs, 0)

    def clear(m, carry):
        kmat[m] = jnp.zeros(kmat.shape[1:], F32)
        return carry

    lax.fori_loop(0, pairs_el, clear, 0)

    chunks = steps // 2
    snap[...] = jnp.zeros_like(snap)

    landed(0, 2)
    faces = faces_ref[0].astype(F32)
    face_row = jnp.concatenate([faces[k : k + 1, :] for k in range(4)], axis=1)
    face_swap = jnp.concatenate([faces[k ^ 1 : (k ^ 1) + 1, :] for k in range(4)], axis=1)
    face_swap = jnp.broadcast_to(face_swap.astype(jnp.int32), (LANES, LANES))
    face_low = jnp.bitwise_and(face_swap[0:8], LANES - 1)
    face_high = jnp.right_shift(face_swap[0:8], 7)

    columns = jnp.concatenate(
        [conn_ref[...].astype(F32), jnp.zeros((LANES - nodes_el, LANES), F32)], axis=0
    ).T.astype(jnp.int32)

    def column(n):
        return jnp.broadcast_to(columns[:, n : n + 1], (LANES, LANES))

    def spot(n):
        j, p = n // 2, n % 2
        return slice(j * LANES, (j + 1) * LANES), slice(p * LANES, (p + 1) * LANES)

    for n in range(nodes_el):
        at_face[spot(n)] = jnp.where(column(n) == face_swap, 1.0, 0.0).astype(BF16)

    def pack(x):
        high = x.astype(BF16).astype(F32)
        return jnp.concatenate([high, x - high], axis=0).astype(BF16)

    def face_forces(packs):
        res = jnp.dot(
            jnp.concatenate(packs, axis=1), at_face[...], preferred_element_type=F32
        )
        res = res[0:8] + res[8:16]
        mixed = jnp.where(row8 < 4, res[:, 0:LANES], res[:, LANES:])
        return mixed + pltpu.roll(mixed, 4, 0)

    def node_forces(packs):
        sides = []
        for b in range(blocks):
            sides.append(
                jnp.concatenate(
                    [
                        packs[j] * hmask[(j * blocks + b) * 16 : (j * blocks + b + 1) * 16, :]
                        for j in range(pairs_el)
                    ],
                    axis=1,
                )
            )
        res = jnp.dot(
            jnp.concatenate(sides, axis=0), at_node[...], preferred_element_type=F32
        )
        halves = []
        for b in range(blocks):
            one = res[16 * b : 16 * b + 8] + res[16 * b + 8 : 16 * b + 16]
            even, odd = one[:, 0:LANES], one[:, LANES:]
            if b % 2:
                halves.append(pltpu.roll(even, 4, 0) + odd)
            else:
                halves.append(even + pltpu.roll(odd, 4, 0))
        return jnp.concatenate(
            [jnp.where(row8 < 4, halves[b], halves[b + 1]) for b in range(0, blocks, 2)],
            axis=0,
        )

    landed(2, 5)
    quarter = jnp.right_shift(lax.broadcasted_iota(jnp.int32, (8, LANES), 1), 5)
    nb = nb_ref[...].astype(F32)
    recv_mask = [jnp.where(quarter == k, nb[:, k : k + 1], 0.0) for k in range(4)]

    def copies(slot):
        return [
            pltpu.make_async_remote_copy(
                src_ref=send.at[slot, 0:4],
                dst_ref=recv.at[slot, k ^ 1, 0:4],
                send_sem=send_sem.at[slot, k],
                recv_sem=recv_sem.at[slot, k ^ 1],
                device_id=where_to[k],
                device_id_type=MESH,
            )
            for k in range(4)
        ]

    def arrivals(slot):
        return [
            pltpu.make_async_remote_copy(
                src_ref=send.at[slot, 0:4],
                dst_ref=recv.at[slot, k, 0:4],
                send_sem=send_sem.at[slot, k],
                recv_sem=recv_sem.at[slot, k],
                device_id=where_to[k],
                device_id_type=MESH,
            )
            for k in range(4)
        ]

    def send_shared(message, slot):
        send[slot] = message
        for k, copy in enumerate(copies(slot)):

            @pl.when(has[k])
            def _():
                copy.start()

    def shared_sum(slot):
        for k, copy in enumerate(arrivals(slot)):

            @pl.when(has[k])
            def _():
                copy.wait_recv()
                copy.wait_send()

        got = recv[slot, 0] * recv_mask[0]
        for k in range(1, 4):
            got = got + recv[slot, k] * recv_mask[k]
        return got

    masses = []
    for n in range(0, nodes_el, 2):
        mass = jnp.where(row8 == 3, mass_ref[n : n + 1, :], 0.0)
        masses.append(pack(mass + jnp.where(row8 == 7, mass_ref[n + 1 : n + 2, :], 0.0)))
    src_rows = []
    for b in range(blocks):
        src_rows.append(src_ref[:, b * LANES : (b + 1) * LANES])
        src_rows.append(jnp.zeros((1, LANES), F32))
    at_faces = jnp.zeros((8, LANES), F32)
    for b in range(blocks):
        rows = jnp.concatenate([src_rows[2 * b], jnp.zeros((5, LANES), F32)], axis=0)
        at_faces = jnp.where(face_high == b, pick_lanes(rows, face_low), at_faces)
    send_shared(face_forces(masses) + at_faces, 0)

    conn_low = jnp.bitwise_and(conn_ref[...], LANES - 1)
    conn_high = jnp.right_shift(conn_ref[...], 7)
    for n in range(nodes_el):
        low_column = jnp.bitwise_and(column(n), LANES - 1)
        at_node[spot(n)] = jnp.where(low_column == lane, 1.0, 0.0).astype(BF16)
    for j in range(pairs_el):
        two = [
            jnp.broadcast_to(conn_high[n : n + 1, :], (4, LANES)) for n in (2 * j, 2 * j + 1)
        ]
        two = jnp.concatenate(two * 2, axis=0)
        for b in range(blocks):
            hmask[(j * blocks + b) * 16 : (j * blocks + b + 1) * 16, :] = jnp.where(
                two == b, 1.0, 0.0
            ).astype(BF16)
    first = node_forces(masses) + jnp.concatenate(src_rows, axis=0)

    face_col = jnp.broadcast_to(face_row, (LANES, LANES)).T
    position = lax.broadcasted_iota(jnp.int32, (LANES, LANES), 0).astype(F32)
    inv_rows = []
    has_rows = []
    for b in range(blocks):
        hit = jnp.where(face_col == (lane + b * LANES).astype(F32), 1.0, 0.0)
        inv_rows.append(
            jnp.broadcast_to(jnp.sum(hit * position, axis=0, keepdims=True), (4, LANES))
        )
        has_rows.append(jnp.broadcast_to(jnp.sum(hit, axis=0, keepdims=True), (4, LANES)))
    inv_idx = jnp.concatenate(inv_rows, axis=0).astype(jnp.int32)
    inv_has = jnp.concatenate(has_rows, axis=0)

    def at_nodes(got):
        got = got + pltpu.roll(got, 4, 0)
        added = jnp.concatenate(
            [pick_lanes(got, inv_idx[0:8]), pick_lanes(got, inv_idx[8:16])], axis=0
        )
        return added * inv_has

    landed(5, len(arrays))
    weight = pw_ref[...]
    hi = weight.astype(BF16).astype(F32)
    pww[...] = jnp.concatenate(
        [hi, weight - hi, hi, jnp.zeros((LANES - depth, LANES), F32)], axis=0
    ).astype(BF16)
    jac = [jnp.broadcast_to(jac_ref[i : i + 1, :], (8, LANES)) for i in range(9)]
    lam = jnp.broadcast_to(lame_ref[0:1, :], (8, LANES))
    mu = jnp.broadcast_to(lame_ref[1:2, :], (8, LANES))

    def form_stiffness(m, carry):
        moments = jnp.dot(products[m], pww[...], preferred_element_type=F32)
        for p in range(2):
            for i in range(tiles):

                def moment(r, rp):
                    start = ((rp * 2 + p) * 3 + r) * padded + 8 * i
                    return moments[start : start + 8]

                half = [
                    [
                        jac[a] * moment(0, rp) + jac[3 + a] * moment(1, rp) + jac[6 + a] * moment(2, rp)
                        for rp in range(3)
                    ]
                    for a in range(3)
                ]
                full = [
                    [
                        jac[b] * half[a][0] + jac[3 + b] * half[a][1] + jac[6 + b] * half[a][2]
                        for b in range(3)
                    ]
                    for a in range(3)
                ]
                trace = mu * (full[0][0] + full[1][1] + full[2][2])
                for c in range(3):
                    for cp in range(3):
                        value = mu * full[cp][c] + lam * full[c][cp]
                        if c == cp:
                            value = value + trace
                        start = (p * 3 + cp) * 4 * padded + 32 * i + c
                        kmat[m, pl.ds(start, 8, stride=4), :] = value
        return carry

    group = 5 if pairs_el % 5 == 0 else 1

    def form_group(i, carry):
        for k in range(group):
            form_stiffness(i * group + k, carry)
        return carry

    lax.fori_loop(0, pairs_el // group, form_group, 0)

    first = first + at_nodes(shared_sum(0))
    axis_row = jnp.bitwise_and(row16, 3) < 3
    source = jnp.where(axis_row, first, 0.0)
    total = jnp.concatenate(
        [jnp.broadcast_to(first[4 * b + 3 : 4 * b + 4, :], (4, LANES)) for b in range(blocks)],
        axis=0,
    )
    half_inverse = jnp.where(axis_row, time_step / total, 0.0)

    spare = jnp.zeros((24 - nodes_el, LANES), jnp.int32)
    conn_low = jnp.concatenate([conn_low, spare], axis=0)
    conn_high = jnp.concatenate([conn_high, spare], axis=0)
    low = [conn_low[8 * i : 8 * i + 8, :] for i in range(3)]
    high = [conn_high[8 * i : 8 * i + 8, :] for i in range(3)]

    def at_elements(rows_of):
        out = []
        for i in range(3):
            acc = None
            for b in range(blocks):
                val = pick_lanes(jnp.broadcast_to(rows_of(b), (8, LANES)), low[i])
                acc = val if b == 0 else jnp.where(high[i] == b, val, acc)
            out.append(acc)
        return out

    def gather(u):
        return tuple(
            tuple(at_elements(lambda b: u[4 * b + c : 4 * b + c + 1, :])) for c in range(3)
        )

    def gradient(values):
        sides = []
        for c in range(3):
            rows = list(values[c]) + [jnp.zeros((8, LANES), F32)]
            hi, lo = split(jnp.concatenate(rows, axis=0))
            sides.append(jnp.concatenate([hi, lo, hi], axis=0))
        along = jnp.dot(
            w1[...], jnp.concatenate(sides, axis=1), preferred_element_type=F32
        )
        tensor = []
        for c in range(3):
            ref_dir = [
                along[r * points : (r + 1) * points, c * LANES : (c + 1) * LANES]
                for r in range(3)
            ]
            tensor.append(
                [
                    ref_dir[0] * jac_ref[e : e + 1, :]
                    + ref_dir[1] * jac_ref[3 + e : 4 + e, :]
                    + ref_dir[2] * jac_ref[6 + e : 7 + e, :]
                    for e in range(3)
                ]
            )
        return tensor

    def stiffness(values):
        for c in range(3):
            for i in range(tiles):
                start = c * padded + 8 * i
                at_el[start : start + 8, :] = values[c][i]
        sums = [None] * pairs_el
        for n in range(nodes_el):
            for cp in range(3):
                here = c_row(cp * padded + n)
                for j in range(pairs_el):
                    start = ((n % 2) * 3 + cp) * 4 * padded + 8 * j
                    term = kmat[n // 2, start : start + 8, :] * here
                    sums[j] = term if sums[j] is None else sums[j] + term
        return [pack(x) for x in sums]

    def c_row(i):
        return jnp.broadcast_to(at_el[i : i + 1, :], (8, LANES))

    def record(t):
        comps = [
            t[0][0],
            t[1][1],
            t[2][2],
            0.5 * (t[1][2] + t[2][1]),
            0.5 * (t[0][2] + t[2][0]),
            0.5 * (t[0][1] + t[1][0]),
        ]
        for c, value in enumerate(comps):
            snap[pl.ds(c, points, stride=8), :] = value

    def build_route():
        ranks = jnp.concatenate(
            [rank_ref[:, q * LANES : (q + 1) * LANES] for q in range(points)], axis=0
        )
        turned = jnp.concatenate(
            [ranks.astype(F32), jnp.zeros((LANES - points, LANES), F32)], axis=0
        ).T.astype(jnp.int32)
        upper = jnp.right_shift(ranks, 7)
        place_row = lax.broadcasted_iota(jnp.int32, (points, LANES), 0)
        lane_value = lax.broadcasted_iota(jnp.int32, (points, LANES), 1).astype(F32)
        sides = []
        for q in range(points):
            low = jnp.broadcast_to(turned[:, q : q + 1], (LANES, LANES))
            low = jnp.bitwise_and(low, LANES - 1)
            spread[q * LANES : (q + 1) * LANES, :] = jnp.where(low == lane, 1.0, 0.0).astype(BF16)
            mine_here = place_row == jnp.broadcast_to(upper[q : q + 1, :], (points, LANES))
            sides.append(
                jnp.concatenate(
                    [jnp.where(mine_here, float(q), 0.0), jnp.where(mine_here, lane_value, 0.0)],
                    axis=0,
                ).astype(BF16)
            )
        route[...] = jnp.dot(
            jnp.concatenate(sides, axis=1), spread[...], preferred_element_type=F32
        ).astype(jnp.int32)

    def in_order(k):
        origin = jnp.broadcast_to(route[pl.ds(k, 1), :], (8, LANES))
        at = jnp.broadcast_to(route[pl.ds(points + k, 1), :], (8, LANES))
        value = pick_lanes(snap[0:8, :], at)
        for q in range(1, points):
            value = jnp.where(origin == q, pick_lanes(snap[8 * q : 8 * q + 8, :], at), value)
        return value

    def keep(parity):
        for k in range(points):
            mixed[k, pl.ds(parity, 8, stride=2), :] = in_order(k)

    velocity = wav_ref[0] * source * half_inverse
    displace = time_step * velocity

    def mine(i):
        return pl.ds(pl.multiple_of(i * block, block), block)

    def parcel(chunk, i, column, target):
        return pltpu.make_async_remote_copy(
            src_ref=pair.at[chunk, :, mine(target)],
            dst_ref=pair_in.at[chunk, :, mine(column)],
            send_sem=out_send_sem.at[chunk, i],
            recv_sem=out_recv_sem.at[chunk, i],
            device_id=(g, target),
            device_id_type=MESH,
        )

    def dispatch(make, local):
        for i in range(1, writers):
            make(i, d, lax.rem(my_d + i, writers)).start()

        @pl.when(other_core)
        def _():
            make(0, d, my_d).start()

        pl.when(jnp.logical_not(other_core))(local)

    def collect(make):
        for i in range(1, writers):
            origin = lax.rem(my_d - i + writers, writers)
            make(i, along(origin), origin).wait_recv()
            make(i, d, lax.rem(my_d + i, writers)).wait_send()

        @pl.when(other_core)
        def _():
            make(0, d, my_d).wait_recv()
            make(0, d, my_d).wait_send()

    def close_pair(chunk):
        for k in range(points):
            pair[chunk, :, k * LANES : (k + 1) * LANES] = mixed[k].astype(BF16)

    def send_pair(chunk):
        def local():
            pair_in[chunk, :, mine(d)] = pair[chunk, :, mine(my_d)]

        dispatch(functools.partial(parcel, chunk), local)

    def send_last(chunk):
        each = block // LANES
        for i in [*range(1, writers, 2), *range(2, writers, 2), 0]:
            w = lax.rem(my_d + i, writers)
            for k in range(each):
                at = w * each + k
                mixed[at, pl.ds(1, 8, stride=2), :] = in_order(at)
                start = pl.multiple_of(at * LANES, LANES)
                pair[chunk, :, pl.ds(start, LANES)] = mixed[at].astype(BF16)
            if i:
                parcel(chunk, i, d, w).start()

        @pl.when(other_core)
        def _():
            parcel(chunk, 0, d, my_d).start()

        @pl.when(jnp.logical_not(other_core))
        def _():
            pair_in[chunk, :, mine(d)] = pair[chunk, :, mine(my_d)]

    def merge(chunk):
        collect(functools.partial(parcel, chunk))
        for c in range(6):
            out_ref[c, 2 * chunk : 2 * chunk + 2, :] = pair_in[chunk, 2 * c : 2 * c + 2, :]

    def launch(t, odd, values, got, displace, velocity, early, extra):
        packs = stiffness(values)
        send_shared(face_forces(packs), odd)
        record(gradient(values))
        if got is not None:
            change = half_inverse * at_nodes(got)
            velocity = velocity - change
            displace = displace - time_step * change
        velocity = velocity + half_inverse * (wav_ref[t] * source - node_forces(packs))
        displace = displace + time_step * velocity
        values = gather(displace)
        extra()
        early()
        keep(1 - odd)
        return values, displace, velocity

    def nothing():
        return None

    state = launch(
        1, 1, gather(displace), None, displace, velocity, nothing, build_route
    )

    inv_f = inv_idx.astype(F32)
    place = [x.astype(jnp.int32) for x in at_elements(lambda b: inv_f[4 * b : 4 * b + 1, :])]
    coef = (-time_step) * half_inverse * inv_has
    coef = at_elements(lambda b: coef[4 * b : 4 * b + 1, :])

    def corrected(values, got):
        out = []
        for c in range(3):
            row = jnp.broadcast_to(got[c : c + 1, :], (8, LANES))
            out.append(
                tuple(values[c][i] + pick_lanes(row, place[i]) * coef[i] for i in range(3))
            )
        return tuple(out)

    def advance(t, odd, state, early):
        values, displace, velocity = state
        got = shared_sum(1 - odd)
        return launch(t, odd, corrected(values, got), got, displace, velocity, early, nothing)

    def two_steps(i, state):
        def early():
            pl.when(i >= 2)(lambda: send_pair(i - 2))

        state = advance(2 * i, 0, state, early)
        close_pair(i - 1)
        return advance(2 * i + 1, 1, state, nothing)

    state = lax.fori_loop(1, chunks, two_steps, state)
    send_pair(chunks - 2)
    for chunk in range(chunks - 2):
        merge(chunk)
    got = shared_sum(1)
    record(gradient(corrected(state[0], got)))
    if block % LANES:
        keep(1)
        close_pair(chunks - 1)
        send_pair(chunks - 1)
    else:
        send_last(chunks - 1)
    merge(chunks - 2)
    merge(chunks - 1)


def solution(mesh):
    groups, writers = mesh.shape["grp"], mesh.shape["dom"]

    def shards(
        connect,
        interface_nodes,
        neighbours,
        point_rank,
        shape_grad,
        inverse_jacobian,
        lame_moduli,
        point_weights,
        mass_elem,
        source_pattern,
        wavelet,
    ):
        nodes_el, elements = connect.shape
        points = point_weights.shape[0]
        point_count = point_rank.shape[1]
        steps = wavelet.shape[0]
        padded = -(-nodes_el // 8) * 8
        vmem = pl.BlockSpec(memory_space=pltpu.VMEM)
        hbm = pl.BlockSpec(memory_space=pl.ANY)
        sharded = (
            connect,
            interface_nodes,
            neighbours,
            point_rank,
            inverse_jacobian,
            lame_moduli,
            point_weights,
            mass_elem,
            source_pattern,
        )
        ordered = pl.pallas_call(
            functools.partial(kernel, groups, writers, steps, nodes_el),
            out_shape=pltpu.VMEM((6, steps, point_count), BF16),
            in_specs=[hbm] * (len(sharded) + 2),
            out_specs=vmem,
            scratch_shapes=[pltpu.VMEM(a.shape, a.dtype) for a in sharded] * 2
            + [pltpu.VMEM(shape_grad.shape[::-1], F32), pltpu.SMEM(wavelet.shape, F32)]
            + [pltpu.SemaphoreType.DMA((len(sharded) + 2,))] * 3
            + [
                pltpu.VMEM((nodes_el // 2 * LANES, 2 * LANES), BF16),
                pltpu.VMEM((nodes_el // 2 * LANES, 2 * LANES), BF16),
                pltpu.VMEM((nodes_el // 2 * (source_pattern.shape[1] // LANES) * 16, LANES), BF16),
                pltpu.VMEM((3, padded, LANES), F32),
                pltpu.VMEM((nodes_el // 2, 18 * padded, LANES), BF16),
                pltpu.VMEM((LANES, LANES), BF16),
                pltpu.VMEM((nodes_el // 2, 24 * padded, LANES), F32),
                pltpu.VMEM((3 * padded, LANES), F32),
                pltpu.VMEM((3 * points, 96), BF16),
                pltpu.VMEM((8 * points, LANES), F32),
                pltpu.VMEM((points * LANES, LANES), BF16),
                pltpu.VMEM((2 * points, LANES), jnp.int32),
                pltpu.VMEM((points, 16, LANES), F32),
                pltpu.VMEM((steps // 2, 16, point_count), BF16),
                pltpu.VMEM((steps // 2, 16, point_count), BF16),
                pltpu.VMEM((2, 8, LANES), F32),
                pltpu.VMEM((2, 4, 8, LANES), F32),
                pltpu.SemaphoreType.DMA((2, 4)),
                pltpu.SemaphoreType.DMA((2, 4)),
                pltpu.SemaphoreType.DMA((steps // 2, writers)),
                pltpu.SemaphoreType.DMA((steps // 2, writers)),
            ],
            compiler_params=pltpu.CompilerParams(
                collective_id=0, has_side_effects=True, vmem_limit_bytes=56 * 1024 * 1024
            ),
            name="window",
        )(
            *sharded,
            shape_grad.T,
            wavelet,
        )
        return ordered.transpose(1, 0, 2)

    placed = (
        P(None, ("grp", "dom")),
        P(("grp", "dom"), None, None),
        P(("grp", "dom"), None),
        P(("grp", "dom"), None),
        P(),
        P(None, ("grp", "dom")),
        P(None, ("grp", "dom")),
        P(None, ("grp", "dom")),
        P(None, ("grp", "dom")),
        P(None, ("grp", "dom")),
        P(),
    )
    return jax.shard_map(
        shards, mesh=mesh, in_specs=placed, out_specs=P(None, None, ("grp", "dom")), check_vma=False
    )
```

```python
import functools

import jax
import jax.numpy as jnp
from jax import lax
from jax.experimental import pallas as pl
from jax.experimental.pallas import tpu as pltpu
from jax.sharding import PartitionSpec as P

MESH = pl.DeviceIdType.MESH
F32 = jnp.float32
BF16 = jnp.bfloat16
F8 = jnp.float8_e4m3fn
time_step = 0.5
LANES = 128


def split(x):
    hi = x.astype(BF16)
    return hi, (x - hi.astype(F32)).astype(BF16)


def pick_lanes(x, idx):
    return jnp.take_along_axis(x, idx, axis=1, mode="promise_in_bounds")


def kernel(
    groups,
    writers,
    steps,
    nodes_el,
    conn_in,
    faces_in,
    nb_in,
    rank_in,
    jac_in,
    lame_in,
    pw_in,
    mass_in,
    src_in,
    gradt_in,
    wav_in,
    out_ref,
    conn_ref,
    faces_ref,
    nb_ref,
    rank_ref,
    jac_ref,
    lame_ref,
    pw_ref,
    mass_ref,
    src_ref,
    conn_own,
    faces_own,
    nb_own,
    rank_own,
    jac_own,
    lame_own,
    pw_own,
    mass_own,
    src_own,
    gradt_ref,
    wav_ref,
    move_sem,
    move_send_sem,
    move_recv_sem,
    at_face,
    at_node,
    hmask,
    basis,
    products,
    pww,
    kmat,
    at_el,
    w1,
    snap,
    spread,
    route,
    mixed,
    pair,
    pair_in,
    send,
    recv,
    send_sem,
    recv_sem,
    out_send_sem,
    out_recv_sem,
):
    my_g = lax.axis_index("grp")
    my_d = lax.axis_index("dom")
    points = pw_ref.shape[0]
    block = out_ref.shape[2] // writers
    blocks = src_ref.shape[1] // LANES

    def along(w):
        if writers % 4:
            return w
        return w + lax.rem(w // 2, 2) * (1 - 2 * lax.rem(w, 2))

    def across(g, w):
        if groups % 2:
            return g
        return g + lax.rem(w, 2) * (1 - 2 * lax.rem(g, 2))

    def host(g, w):
        return across(g, w), along(w)

    d = along(my_d)
    g = across(my_g, d)
    stays = (g == my_g) & (d == my_d)
    moves = jnp.logical_not(stays)
    other_core = g != my_g
    target = host(my_g, my_d)

    has = (g > 0, g < groups - 1, d > 0, d < writers - 1)
    where_to = (host(g - 1, d), host(g + 1, d), host(g, d - 1), host(g, d + 1))

    arrays = (
        (conn_in, conn_own, conn_ref),
        (faces_in, faces_own, faces_ref),
        (mass_in, mass_own, mass_ref),
        (src_in, src_own, src_ref),
        (nb_in, nb_own, nb_ref),
        (pw_in, pw_own, pw_ref),
        (jac_in, jac_own, jac_ref),
        (lame_in, lame_own, lame_ref),
        (rank_in, rank_own, rank_ref),
    )

    def fetch(i, kept):
        return pltpu.make_async_copy(
            arrays[i][0], arrays[i][2 if kept else 1], move_sem.at[i]
        )

    def move(i):
        return pltpu.make_async_remote_copy(
            src_ref=arrays[i][1],
            dst_ref=arrays[i][2],
            send_sem=move_send_sem.at[i],
            recv_sem=move_recv_sem.at[i],
            device_id=target,
            device_id_type=MESH,
        )

    recv[...] = jnp.zeros_like(recv)
    barrier = pltpu.get_barrier_semaphore()
    shared = (
        pltpu.make_async_copy(gradt_in, gradt_ref, move_sem.at[len(arrays)]),
        pltpu.make_async_copy(wav_in, wav_ref, move_sem.at[len(arrays) + 1]),
    )

    @pl.when(moves)
    def _():
        pl.semaphore_signal(barrier, inc=1, device_id=(g, d), device_id_type=MESH)

    for k in range(4):

        @pl.when(has[k])
        def _():
            pl.semaphore_signal(barrier, inc=1, device_id=where_to[k], device_id_type=MESH)

    near = writers <= 4
    for i in range(0 if near else writers):
        origin_d = lax.rem(my_d + i, writers)
        origin = (across(my_g, along(origin_d)), origin_d)

        def greet():
            pl.semaphore_signal(barrier, inc=1, device_id=origin, device_id_type=MESH)

        if i:
            greet()
        else:
            pl.when(other_core)(greet)

    @pl.when(stays)
    def _():
        for i in range(len(arrays)):
            fetch(i, True).start()

    @pl.when(moves)
    def _():
        for i in range(len(arrays)):
            fetch(i, False).start()

    for copy in shared:
        copy.start()
    expected = moves.astype(jnp.int32)
    if not near:
        expected = expected + other_core.astype(jnp.int32) + writers - 1
    for k in range(4):
        expected = expected + has[k].astype(jnp.int32)
    pl.semaphore_wait(barrier, expected)

    @pl.when(moves)
    def _():
        for i in range(len(arrays)):
            fetch(i, False).wait()
            move(i).start()

    def landed(lo, hi):
        @pl.when(stays)
        def _():
            for i in range(lo, hi):
                fetch(i, True).wait()

        @pl.when(moves)
        def _():
            for i in range(lo, hi):
                move(i).wait_recv()
                move(i).wait_send()


    lane = lax.broadcasted_iota(jnp.int32, (LANES, LANES), 1)
    row8 = lax.broadcasted_iota(jnp.int32, (8, LANES), 0)
    row16 = lax.broadcasted_iota(jnp.int32, (16, LANES), 0)
    pairs_el = nodes_el // 2
    padded = -(-nodes_el // 8) * 8
    tiles = padded // 8

    for copy in shared:
        copy.wait()
    gradt = gradt_ref[...]
    depth = 3 * points
    hi = gradt.astype(BF16).astype(F32)
    lo = gradt - hi
    gap = jnp.zeros((32 - nodes_el, depth), F32)
    tall = jnp.concatenate([hi, gap, hi, gap, lo, gap, jnp.zeros((32, depth), F32)], axis=0)
    tall = jnp.concatenate([tall, jnp.zeros((LANES, LANES - depth), F32)], axis=1)
    w1[...] = tall.T[0:depth, 0:96].astype(BF16)

    lanes = lax.broadcasted_iota(jnp.int32, (padded, LANES), 1)
    base = jnp.concatenate([gradt, jnp.zeros((padded - nodes_el, depth), F32)], axis=0)
    base = jnp.concatenate([base, jnp.zeros((padded, LANES - depth), F32)], axis=1)
    own_dir = []
    for r in range(3):
        x = pltpu.roll(base, LANES - r * points, 1) if r else base
        x = jnp.where(lanes < points, x, 0.0)
        x = x + pltpu.roll(x, points, 1) + pltpu.roll(x, 2 * points, 1)
        own_dir.append(x)
        basis[r] = x

    def multiply_pairs(m, carry):
        for rp in range(3):
            parts = []
            for p in range(2):
                other = basis[rp, pl.ds(2 * m + p, 1), :]
                for r in range(3):
                    product = own_dir[r] * other
                    high = product.astype(BF16).astype(F32)
                    parts.append(jnp.where(lanes < 2 * points, high, product - high))
            rows = 6 * padded
            products[m, rp * rows : (rp + 1) * rows, :] = jnp.concatenate(
                parts, axis=0
            ).astype(BF16)
        return carry

    lax.fori_loop(0, pairs_el, multiply_pairs, 0)

    def clear(m, carry):
        kmat[m] = jnp.zeros(kmat.shape[1:], F32)
        return carry

    lax.fori_loop(0, pairs_el, clear, 0)

    chunks = steps // 2
    snap[...] = jnp.zeros_like(snap)

    landed(0, 2)
    faces = faces_ref[0].astype(F32)
    face_row = jnp.concatenate([faces[k : k + 1, :] for k in range(4)], axis=1)
    face_swap = jnp.concatenate([faces[k ^ 1 : (k ^ 1) + 1, :] for k in range(4)], axis=1)
    face_swap = jnp.broadcast_to(face_swap.astype(jnp.int32), (LANES, LANES))
    face_low = jnp.bitwise_and(face_swap[0:8], LANES - 1)
    face_high = jnp.right_shift(face_swap[0:8], 7)

    columns = jnp.concatenate(
        [conn_ref[...].astype(F32), jnp.zeros((LANES - nodes_el, LANES), F32)], axis=0
    ).T.astype(jnp.int32)

    def column(n):
        return jnp.broadcast_to(columns[:, n : n + 1], (LANES, LANES))

    def spot(n):
        j, p = n // 2, n % 2
        return slice(j * LANES, (j + 1) * LANES), slice(p * LANES, (p + 1) * LANES)

    for n in range(nodes_el):
        at_face[spot(n)] = jnp.where(column(n) == face_swap, 1.0, 0.0).astype(F8)

    def pack(x):
        high = x.astype(BF16).astype(F32)
        return jnp.concatenate([high, x - high], axis=0).astype(BF16)

    def face_forces(packs):
        res = jnp.dot(
            jnp.concatenate(packs, axis=1), at_face[...], preferred_element_type=F32
        )
        res = res[0:8] + res[8:16]
        mixed = jnp.where(row8 < 4, res[:, 0:LANES], res[:, LANES:])
        return mixed + pltpu.roll(mixed, 4, 0)

    def node_forces(packs):
        sides = []
        for b in range(blocks):
            sides.append(
                jnp.concatenate(
                    [
                        packs[j] * hmask[(j * blocks + b) * 16 : (j * blocks + b + 1) * 16, :]
                        for j in range(pairs_el)
                    ],
                    axis=1,
                )
            )
        res = jnp.dot(
            jnp.concatenate(sides, axis=0), at_node[...], preferred_element_type=F32
        )
        halves = []
        for b in range(blocks):
            one = res[16 * b : 16 * b + 8] + res[16 * b + 8 : 16 * b + 16]
            even, odd = one[:, 0:LANES], one[:, LANES:]
            if b % 2:
                halves.append(pltpu.roll(even, 4, 0) + odd)
            else:
                halves.append(even + pltpu.roll(odd, 4, 0))
        return jnp.concatenate(
            [jnp.where(row8 < 4, halves[b], halves[b + 1]) for b in range(0, blocks, 2)],
            axis=0,
        )

    landed(2, 5)
    quarter = jnp.right_shift(lax.broadcasted_iota(jnp.int32, (8, LANES), 1), 5)
    nb = nb_ref[...].astype(F32)
    recv_mask = [jnp.where(quarter == k, nb[:, k : k + 1], 0.0) for k in range(4)]

    def copies(slot):
        return [
            pltpu.make_async_remote_copy(
                src_ref=send.at[slot, 0:4],
                dst_ref=recv.at[slot, k ^ 1, 0:4],
                send_sem=send_sem.at[slot, k],
                recv_sem=recv_sem.at[slot, k ^ 1],
                device_id=where_to[k],
                device_id_type=MESH,
            )
            for k in range(4)
        ]

    def arrivals(slot):
        return [
            pltpu.make_async_remote_copy(
                src_ref=send.at[slot, 0:4],
                dst_ref=recv.at[slot, k, 0:4],
                send_sem=send_sem.at[slot, k],
                recv_sem=recv_sem.at[slot, k],
                device_id=where_to[k],
                device_id_type=MESH,
            )
            for k in range(4)
        ]

    def send_shared(message, slot):
        send[slot] = message
        for k, copy in enumerate(copies(slot)):

            @pl.when(has[k])
            def _():
                copy.start()

    def departed(slot):
        for k, copy in enumerate(copies(slot)):
            pl.when(has[k])(copy.wait_send)

    def shared_sum(slot):
        for k, copy in enumerate(arrivals(slot)):

            @pl.when(has[k])
            def _():
                copy.wait_recv()

        got = recv[slot, 0] * recv_mask[0]
        for k in range(1, 4):
            got = got + recv[slot, k] * recv_mask[k]
        return got

    masses = []
    for n in range(0, nodes_el, 2):
        mass = jnp.where(row8 == 3, mass_ref[n : n + 1, :], 0.0)
        masses.append(pack(mass + jnp.where(row8 == 7, mass_ref[n + 1 : n + 2, :], 0.0)))
    src_rows = []
    for b in range(blocks):
        src_rows.append(src_ref[:, b * LANES : (b + 1) * LANES])
        src_rows.append(jnp.zeros((1, LANES), F32))
    at_faces = jnp.zeros((8, LANES), F32)
    for b in range(blocks):
        rows = jnp.concatenate([src_rows[2 * b], jnp.zeros((5, LANES), F32)], axis=0)
        at_faces = jnp.where(face_high == b, pick_lanes(rows, face_low), at_faces)
    send_shared(face_forces(masses) + at_faces, 0)

    conn_low = jnp.bitwise_and(conn_ref[...], LANES - 1)
    conn_high = jnp.right_shift(conn_ref[...], 7)
    for n in range(nodes_el):
        low_column = jnp.bitwise_and(column(n), LANES - 1)
        at_node[spot(n)] = jnp.where(low_column == lane, 1.0, 0.0).astype(BF16)
    for j in range(pairs_el):
        two = [
            jnp.broadcast_to(conn_high[n : n + 1, :], (4, LANES)) for n in (2 * j, 2 * j + 1)
        ]
        two = jnp.concatenate(two * 2, axis=0)
        for b in range(blocks):
            hmask[(j * blocks + b) * 16 : (j * blocks + b + 1) * 16, :] = jnp.where(
                two == b, 1.0, 0.0
            ).astype(BF16)
    first = node_forces(masses) + jnp.concatenate(src_rows, axis=0)

    face_col = jnp.broadcast_to(face_row, (LANES, LANES)).T
    position = lax.broadcasted_iota(jnp.int32, (LANES, LANES), 0).astype(F32)
    inv_rows = []
    has_rows = []
    for b in range(blocks):
        hit = jnp.where(face_col == (lane + b * LANES).astype(F32), 1.0, 0.0)
        inv_rows.append(
            jnp.broadcast_to(jnp.sum(hit * position, axis=0, keepdims=True), (4, LANES))
        )
        has_rows.append(jnp.broadcast_to(jnp.sum(hit, axis=0, keepdims=True), (4, LANES)))
    inv_idx = jnp.concatenate(inv_rows, axis=0).astype(jnp.int32)
    inv_has = jnp.concatenate(has_rows, axis=0)

    def at_nodes(got):
        got = got + pltpu.roll(got, 4, 0)
        added = jnp.concatenate(
            [pick_lanes(got, inv_idx[0:8]), pick_lanes(got, inv_idx[8:16])], axis=0
        )
        return added * inv_has

    landed(5, len(arrays))
    weight = pw_ref[...]
    hi = weight.astype(BF16).astype(F32)
    pww[...] = jnp.concatenate(
        [hi, weight - hi, hi, jnp.zeros((LANES - depth, LANES), F32)], axis=0
    ).astype(BF16)
    jac = [jnp.broadcast_to(jac_ref[i : i + 1, :], (8, LANES)) for i in range(9)]
    lam = jnp.broadcast_to(lame_ref[0:1, :], (8, LANES))
    mu = jnp.broadcast_to(lame_ref[1:2, :], (8, LANES))

    def form_stiffness(m, carry):
        moments = jnp.dot(products[m], pww[...], preferred_element_type=F32)
        for p in range(2):
            for i in range(tiles):

                def moment(r, rp):
                    start = ((rp * 2 + p) * 3 + r) * padded + 8 * i
                    return moments[start : start + 8]

                half = [
                    [
                        jac[a] * moment(0, rp) + jac[3 + a] * moment(1, rp) + jac[6 + a] * moment(2, rp)
                        for rp in range(3)
                    ]
                    for a in range(3)
                ]
                full = [
                    [
                        jac[b] * half[a][0] + jac[3 + b] * half[a][1] + jac[6 + b] * half[a][2]
                        for b in range(3)
                    ]
                    for a in range(3)
                ]
                trace = mu * (full[0][0] + full[1][1] + full[2][2])
                for c in range(3):
                    for cp in range(3):
                        value = mu * full[cp][c] + lam * full[c][cp]
                        if c == cp:
                            value = value + trace
                        start = (p * 3 + cp) * 4 * padded + 32 * i + c
                        kmat[m, pl.ds(start, 8, stride=4), :] = value
        return carry

    group = 5 if pairs_el % 5 == 0 else 1

    def form_group(i, carry):
        for k in range(group):
            form_stiffness(i * group + k, carry)
        return carry

    lax.fori_loop(0, pairs_el // group, form_group, 0)

    first = first + at_nodes(shared_sum(0))
    axis_row = jnp.bitwise_and(row16, 3) < 3
    source = jnp.where(axis_row, first, 0.0)
    total = jnp.concatenate(
        [jnp.broadcast_to(first[4 * b + 3 : 4 * b + 4, :], (4, LANES)) for b in range(blocks)],
        axis=0,
    )
    half_inverse = jnp.where(axis_row, time_step / total, 0.0)

    spare = jnp.zeros((24 - nodes_el, LANES), jnp.int32)
    conn_low = jnp.concatenate([conn_low, spare], axis=0)
    conn_high = jnp.concatenate([conn_high, spare], axis=0)
    low = [conn_low[8 * i : 8 * i + 8, :] for i in range(3)]
    high = [conn_high[8 * i : 8 * i + 8, :] for i in range(3)]

    def at_elements(rows_of):
        out = []
        for i in range(3):
            acc = None
            for b in range(blocks):
                val = pick_lanes(jnp.broadcast_to(rows_of(b), (8, LANES)), low[i])
                acc = val if b == 0 else jnp.where(high[i] == b, val, acc)
            out.append(acc)
        return out

    def gather(u):
        return tuple(
            tuple(at_elements(lambda b: u[4 * b + c : 4 * b + c + 1, :])) for c in range(3)
        )

    def gradient(values):
        sides = []
        for c in range(3):
            rows = list(values[c]) + [jnp.zeros((8, LANES), F32)]
            hi, lo = split(jnp.concatenate(rows, axis=0))
            sides.append(jnp.concatenate([hi, lo, hi], axis=0))
        along = jnp.dot(
            w1[...], jnp.concatenate(sides, axis=1), preferred_element_type=F32
        )
        tensor = []
        for c in range(3):
            ref_dir = [
                along[r * points : (r + 1) * points, c * LANES : (c + 1) * LANES]
                for r in range(3)
            ]
            tensor.append(
                [
                    ref_dir[0] * jac_ref[e : e + 1, :]
                    + ref_dir[1] * jac_ref[3 + e : 4 + e, :]
                    + ref_dir[2] * jac_ref[6 + e : 7 + e, :]
                    for e in range(3)
                ]
            )
        return tensor

    def stiffness(values):
        for c in range(3):
            for i in range(tiles):
                start = c * padded + 8 * i
                at_el[start : start + 8, :] = values[c][i]
        sums = [None] * pairs_el
        for n in range(nodes_el):
            for cp in range(3):
                here = c_row(cp * padded + n)
                for j in range(pairs_el):
                    start = ((n % 2) * 3 + cp) * 4 * padded + 8 * j
                    term = kmat[n // 2, start : start + 8, :] * here
                    sums[j] = term if sums[j] is None else sums[j] + term
        return [pack(x) for x in sums]

    def c_row(i):
        return jnp.broadcast_to(at_el[i : i + 1, :], (8, LANES))

    def record(t):
        comps = [
            t[0][0],
            t[1][1],
            t[2][2],
            0.5 * (t[1][2] + t[2][1]),
            0.5 * (t[0][2] + t[2][0]),
            0.5 * (t[0][1] + t[1][0]),
        ]
        for c, value in enumerate(comps):
            snap[pl.ds(c, points, stride=8), :] = value

    def build_route():
        ranks = jnp.concatenate(
            [rank_ref[:, q * LANES : (q + 1) * LANES] for q in range(points)], axis=0
        )
        turned = jnp.concatenate(
            [ranks.astype(F32), jnp.zeros((LANES - points, LANES), F32)], axis=0
        ).T.astype(jnp.int32)
        upper = jnp.right_shift(ranks, 7)
        place_row = lax.broadcasted_iota(jnp.int32, (points, LANES), 0)
        lane_value = lax.broadcasted_iota(jnp.int32, (points, LANES), 1).astype(F32)
        sides = []
        for q in range(points):
            low = jnp.broadcast_to(turned[:, q : q + 1], (LANES, LANES))
            low = jnp.bitwise_and(low, LANES - 1)
            spread[q * LANES : (q + 1) * LANES, :] = jnp.where(low == lane, 1.0, 0.0).astype(BF16)
            mine_here = place_row == jnp.broadcast_to(upper[q : q + 1, :], (points, LANES))
            sides.append(
                jnp.concatenate(
                    [jnp.where(mine_here, float(q), 0.0), jnp.where(mine_here, lane_value, 0.0)],
                    axis=0,
                ).astype(BF16)
            )
        route[...] = jnp.dot(
            jnp.concatenate(sides, axis=1), spread[...], preferred_element_type=F32
        ).astype(jnp.int32)

    def in_order(k):
        origin = jnp.broadcast_to(route[pl.ds(k, 1), :], (8, LANES))
        at = jnp.broadcast_to(route[pl.ds(points + k, 1), :], (8, LANES))
        value = pick_lanes(snap[0:8, :], at)
        for q in range(1, points):
            value = jnp.where(origin == q, pick_lanes(snap[8 * q : 8 * q + 8, :], at), value)
        return value

    def keep(parity):
        for k in range(points):
            mixed[k, pl.ds(parity, 8, stride=2), :] = in_order(k)

    velocity = wav_ref[0] * source * half_inverse
    displace = time_step * velocity

    def mine(i):
        return pl.ds(pl.multiple_of(i * block, block), block)

    def parcel(chunk, i, column, target):
        return pltpu.make_async_remote_copy(
            src_ref=pair.at[chunk, :, mine(target)],
            dst_ref=pair_in.at[chunk, :, mine(column)],
            send_sem=out_send_sem.at[chunk, i],
            recv_sem=out_recv_sem.at[chunk, i],
            device_id=(g, target),
            device_id_type=MESH,
        )

    def dispatch(make, local):
        for i in range(1, writers):
            make(i, d, lax.rem(my_d + i, writers)).start()

        @pl.when(other_core)
        def _():
            make(0, d, my_d).start()

        pl.when(jnp.logical_not(other_core))(local)

    def collect(make):
        for i in range(1, writers):
            origin = lax.rem(my_d - i + writers, writers)
            make(i, along(origin), origin).wait_recv()
            make(i, d, lax.rem(my_d + i, writers)).wait_send()

        @pl.when(other_core)
        def _():
            make(0, d, my_d).wait_recv()
            make(0, d, my_d).wait_send()

    def close_pair(chunk):
        for k in range(points):
            pair[chunk, :, k * LANES : (k + 1) * LANES] = mixed[k].astype(BF16)

    def send_pair(chunk):
        def local():
            pair_in[chunk, :, mine(d)] = pair[chunk, :, mine(my_d)]

        dispatch(functools.partial(parcel, chunk), local)

    def send_last(chunk):
        each = block // LANES
        for i in [*range(1, writers, 2), *range(2, writers, 2), 0]:
            w = lax.rem(my_d + i, writers)
            for k in range(each):
                at = w * each + k
                mixed[at, pl.ds(1, 8, stride=2), :] = in_order(at)
                start = pl.multiple_of(at * LANES, LANES)
                pair[chunk, :, pl.ds(start, LANES)] = mixed[at].astype(BF16)
            if i:
                parcel(chunk, i, d, w).start()

        @pl.when(other_core)
        def _():
            parcel(chunk, 0, d, my_d).start()

        @pl.when(jnp.logical_not(other_core))
        def _():
            pair_in[chunk, :, mine(d)] = pair[chunk, :, mine(my_d)]

    def merge(chunk):
        collect(functools.partial(parcel, chunk))
        for c in range(6):
            out_ref[c, 2 * chunk : 2 * chunk + 2, :] = pair_in[chunk, 2 * c : 2 * c + 2, :]

    def launch(t, odd, values, got, displace, velocity, early, extra):
        packs = stiffness(values)
        send_shared(face_forces(packs), odd)
        departed(1 - odd)
        record(gradient(values))
        if got is not None:
            change = half_inverse * at_nodes(got)
            velocity = velocity - change
            displace = displace - time_step * change
        velocity = velocity + half_inverse * (wav_ref[t] * source - node_forces(packs))
        displace = displace + time_step * velocity
        values = gather(displace)
        extra()
        early()
        keep(1 - odd)
        return values, displace, velocity

    def nothing():
        return None

    state = launch(
        1, 1, gather(displace), None, displace, velocity, nothing, build_route
    )

    inv_f = inv_idx.astype(F32)
    place = [x.astype(jnp.int32) for x in at_elements(lambda b: inv_f[4 * b : 4 * b + 1, :])]
    coef = (-time_step) * half_inverse * inv_has
    coef = at_elements(lambda b: coef[4 * b : 4 * b + 1, :])

    def corrected(values, got):
        out = []
        for c in range(3):
            row = jnp.broadcast_to(got[c : c + 1, :], (8, LANES))
            out.append(
                tuple(values[c][i] + pick_lanes(row, place[i]) * coef[i] for i in range(3))
            )
        return tuple(out)

    def advance(t, odd, state, early):
        values, displace, velocity = state
        got = shared_sum(1 - odd)
        return launch(t, odd, corrected(values, got), got, displace, velocity, early, nothing)

    def two_steps(i, state):
        def early():
            pl.when(i >= 2)(lambda: send_pair(i - 2))

        state = advance(2 * i, 0, state, early)
        close_pair(i - 1)
        return advance(2 * i + 1, 1, state, nothing)

    state = lax.fori_loop(1, chunks, two_steps, state)
    send_pair(chunks - 2)
    for chunk in range(chunks - 2):
        merge(chunk)
    got = shared_sum(1)
    record(gradient(corrected(state[0], got)))
    if block % LANES:
        keep(1)
        close_pair(chunks - 1)
        send_pair(chunks - 1)
    else:
        send_last(chunks - 1)
    departed(1)
    merge(chunks - 2)
    merge(chunks - 1)


def solution(mesh):
    groups, writers = mesh.shape["grp"], mesh.shape["dom"]

    def shards(
        connect,
        interface_nodes,
        neighbours,
        point_rank,
        shape_grad,
        inverse_jacobian,
        lame_moduli,
        point_weights,
        mass_elem,
        source_pattern,
        wavelet,
    ):
        nodes_el, elements = connect.shape
        points = point_weights.shape[0]
        point_count = point_rank.shape[1]
        steps = wavelet.shape[0]
        padded = -(-nodes_el // 8) * 8
        vmem = pl.BlockSpec(memory_space=pltpu.VMEM)
        hbm = pl.BlockSpec(memory_space=pl.ANY)
        sharded = (
            connect,
            interface_nodes,
            neighbours,
            point_rank,
            inverse_jacobian,
            lame_moduli,
            point_weights,
            mass_elem,
            source_pattern,
        )
        ordered = pl.pallas_call(
            functools.partial(kernel, groups, writers, steps, nodes_el),
            out_shape=pltpu.VMEM((6, steps, point_count), BF16),
            in_specs=[hbm] * (len(sharded) + 2),
            out_specs=vmem,
            scratch_shapes=[pltpu.VMEM(a.shape, a.dtype) for a in sharded] * 2
            + [pltpu.VMEM(shape_grad.shape[::-1], F32), pltpu.SMEM(wavelet.shape, F32)]
            + [pltpu.SemaphoreType.DMA((len(sharded) + 2,))] * 3
            + [
                pltpu.VMEM((nodes_el // 2 * LANES, 2 * LANES), F8),
                pltpu.VMEM((nodes_el // 2 * LANES, 2 * LANES), BF16),
                pltpu.VMEM((nodes_el // 2 * (source_pattern.shape[1] // LANES) * 16, LANES), BF16),
                pltpu.VMEM((3, padded, LANES), F32),
                pltpu.VMEM((nodes_el // 2, 18 * padded, LANES), BF16),
                pltpu.VMEM((LANES, LANES), BF16),
                pltpu.VMEM((nodes_el // 2, 24 * padded, LANES), F32),
                pltpu.VMEM((3 * padded, LANES), F32),
                pltpu.VMEM((3 * points, 96), BF16),
                pltpu.VMEM((8 * points, LANES), F32),
                pltpu.VMEM((points * LANES, LANES), BF16),
                pltpu.VMEM((2 * points, LANES), jnp.int32),
                pltpu.VMEM((points, 16, LANES), F32),
                pltpu.VMEM((steps // 2, 16, point_count), BF16),
                pltpu.VMEM((steps // 2, 16, point_count), BF16),
                pltpu.VMEM((2, 8, LANES), F32),
                pltpu.VMEM((2, 4, 8, LANES), F32),
                pltpu.SemaphoreType.DMA((2, 4)),
                pltpu.SemaphoreType.DMA((2, 4)),
                pltpu.SemaphoreType.DMA((steps // 2, writers)),
                pltpu.SemaphoreType.DMA((steps // 2, writers)),
            ],
            compiler_params=pltpu.CompilerParams(
                collective_id=0, has_side_effects=True, vmem_limit_bytes=56 * 1024 * 1024
            ),
            name="window",
        )(
            *sharded,
            shape_grad.T,
            wavelet,
        )
        return ordered.transpose(1, 0, 2)

    placed = (
        P(None, ("grp", "dom")),
        P(("grp", "dom"), None, None),
        P(("grp", "dom"), None),
        P(("grp", "dom"), None),
        P(),
        P(None, ("grp", "dom")),
        P(None, ("grp", "dom")),
        P(None, ("grp", "dom")),
        P(None, ("grp", "dom")),
        P(None, ("grp", "dom")),
        P(),
    )
    return jax.shard_map(
        shards, mesh=mesh, in_specs=placed, out_specs=P(None, None, ("grp", "dom")), check_vma=False
    )
```

```python
import functools

import jax
import jax.numpy as jnp
from jax import lax
from jax.experimental import pallas as pl
from jax.experimental.pallas import tpu as pltpu
from jax.sharding import PartitionSpec as P

MESH = pl.DeviceIdType.MESH
F32 = jnp.float32
BF16 = jnp.bfloat16
F8 = jnp.float8_e4m3fn
time_step = 0.5
LANES = 128


def split(x):
    hi = x.astype(BF16)
    return hi, (x - hi.astype(F32)).astype(BF16)


def pick_lanes(x, idx):
    return jnp.take_along_axis(x, idx, axis=1, mode="promise_in_bounds")


def kernel(
    groups,
    writers,
    steps,
    nodes_el,
    conn_in,
    faces_in,
    nb_in,
    rank_in,
    jac_in,
    lame_in,
    pw_in,
    mass_in,
    src_in,
    gradt_in,
    wav_in,
    out_ref,
    conn_ref,
    faces_ref,
    nb_ref,
    rank_ref,
    jac_ref,
    lame_ref,
    pw_ref,
    mass_ref,
    src_ref,
    conn_own,
    faces_own,
    nb_own,
    rank_own,
    jac_own,
    lame_own,
    pw_own,
    mass_own,
    src_own,
    gradt_ref,
    wav_ref,
    move_sem,
    move_send_sem,
    move_recv_sem,
    at_face,
    at_node,
    hmask,
    basis,
    products,
    pww,
    kmat,
    at_el,
    w1,
    snap,
    spread,
    route,
    mixed,
    pair,
    pair_in,
    send,
    recv,
    send_sem,
    recv_sem,
    out_send_sem,
    out_recv_sem,
):
    my_g = lax.axis_index("grp")
    my_d = lax.axis_index("dom")
    points = pw_ref.shape[0]
    block = out_ref.shape[2] // writers
    blocks = src_ref.shape[1] // LANES

    def along(w):
        if writers % 4:
            return w
        return w + lax.rem(w // 2, 2) * (1 - 2 * lax.rem(w, 2))

    def across(g, w):
        if groups % 2:
            return g
        return g + lax.rem(w, 2) * (1 - 2 * lax.rem(g, 2))

    def host(g, w):
        return across(g, w), along(w)

    d = along(my_d)
    g = across(my_g, d)
    stays = (g == my_g) & (d == my_d)
    moves = jnp.logical_not(stays)
    other_core = g != my_g
    target = host(my_g, my_d)

    has = (g > 0, g < groups - 1, d > 0, d < writers - 1)
    where_to = (host(g - 1, d), host(g + 1, d), host(g, d - 1), host(g, d + 1))

    arrays = (
        (conn_in, conn_own, conn_ref),
        (faces_in, faces_own, faces_ref),
        (mass_in, mass_own, mass_ref),
        (src_in, src_own, src_ref),
        (nb_in, nb_own, nb_ref),
        (pw_in, pw_own, pw_ref),
        (jac_in, jac_own, jac_ref),
        (lame_in, lame_own, lame_ref),
        (rank_in, rank_own, rank_ref),
    )

    def fetch(i, kept):
        return pltpu.make_async_copy(
            arrays[i][0], arrays[i][2 if kept else 1], move_sem.at[i]
        )

    def move(i):
        return pltpu.make_async_remote_copy(
            src_ref=arrays[i][1],
            dst_ref=arrays[i][2],
            send_sem=move_send_sem.at[i],
            recv_sem=move_recv_sem.at[i],
            device_id=target,
            device_id_type=MESH,
        )

    recv[...] = jnp.zeros_like(recv)
    barrier = pltpu.get_barrier_semaphore()
    shared = (
        pltpu.make_async_copy(gradt_in, gradt_ref, move_sem.at[len(arrays)]),
        pltpu.make_async_copy(wav_in, wav_ref, move_sem.at[len(arrays) + 1]),
    )

    @pl.when(moves)
    def _():
        pl.semaphore_signal(barrier, inc=1, device_id=(g, d), device_id_type=MESH)

    for k in range(4):

        @pl.when(has[k])
        def _():
            pl.semaphore_signal(barrier, inc=1, device_id=where_to[k], device_id_type=MESH)

    near = writers <= 4
    for i in range(0 if near else writers):
        origin_d = lax.rem(my_d + i, writers)
        origin = (across(my_g, along(origin_d)), origin_d)

        def greet():
            pl.semaphore_signal(barrier, inc=1, device_id=origin, device_id_type=MESH)

        if i:
            greet()
        else:
            pl.when(other_core)(greet)

    @pl.when(stays)
    def _():
        for i in range(len(arrays)):
            fetch(i, True).start()

    @pl.when(moves)
    def _():
        for i in range(len(arrays)):
            fetch(i, False).start()

    for copy in shared:
        copy.start()
    expected = moves.astype(jnp.int32)
    if not near:
        expected = expected + other_core.astype(jnp.int32) + writers - 1
    for k in range(4):
        expected = expected + has[k].astype(jnp.int32)
    pl.semaphore_wait(barrier, expected)

    @pl.when(moves)
    def _():
        for i in range(len(arrays)):
            fetch(i, False).wait()
            move(i).start()

    def landed(lo, hi):
        @pl.when(stays)
        def _():
            for i in range(lo, hi):
                fetch(i, True).wait()

        @pl.when(moves)
        def _():
            for i in range(lo, hi):
                move(i).wait_recv()
                move(i).wait_send()


    lane = lax.broadcasted_iota(jnp.int32, (LANES, LANES), 1)
    row8 = lax.broadcasted_iota(jnp.int32, (8, LANES), 0)
    row16 = lax.broadcasted_iota(jnp.int32, (16, LANES), 0)
    pairs_el = nodes_el // 2
    padded = -(-nodes_el // 8) * 8
    tiles = padded // 8

    for copy in shared:
        copy.wait()
    gradt = gradt_ref[...]
    depth = 3 * points
    hi = gradt.astype(BF16).astype(F32)
    lo = gradt - hi
    gap = jnp.zeros((32 - nodes_el, depth), F32)
    tall = jnp.concatenate([hi, gap, hi, gap, lo, gap, jnp.zeros((32, depth), F32)], axis=0)
    tall = jnp.concatenate([tall, jnp.zeros((LANES, LANES - depth), F32)], axis=1)
    w1[...] = tall.T[0:depth, 0:96].astype(BF16)

    lanes = lax.broadcasted_iota(jnp.int32, (padded, LANES), 1)
    base = jnp.concatenate([gradt, jnp.zeros((padded - nodes_el, depth), F32)], axis=0)
    base = jnp.concatenate([base, jnp.zeros((padded, LANES - depth), F32)], axis=1)
    own_dir = []
    for r in range(3):
        x = pltpu.roll(base, LANES - r * points, 1) if r else base
        x = jnp.where(lanes < points, x, 0.0)
        x = x + pltpu.roll(x, points, 1) + pltpu.roll(x, 2 * points, 1)
        own_dir.append(x)
        basis[r] = x

    def multiply_pairs(m, carry):
        for rp in range(3):
            parts = []
            for p in range(2):
                other = basis[rp, pl.ds(2 * m + p, 1), :]
                for r in range(3):
                    product = own_dir[r] * other
                    high = product.astype(BF16).astype(F32)
                    parts.append(jnp.where(lanes < 2 * points, high, product - high))
            rows = 6 * padded
            products[m, rp * rows : (rp + 1) * rows, :] = jnp.concatenate(
                parts, axis=0
            ).astype(BF16)
        return carry

    lax.fori_loop(0, pairs_el, multiply_pairs, 0)

    def clear(m, carry):
        kmat[m] = jnp.zeros(kmat.shape[1:], F32)
        return carry

    lax.fori_loop(0, pairs_el, clear, 0)

    chunks = steps // 2
    snap[...] = jnp.zeros_like(snap)

    landed(0, 2)
    faces = faces_ref[0].astype(F32)
    face_row = jnp.concatenate([faces[k : k + 1, :] for k in range(4)], axis=1)
    face_swap = jnp.concatenate([faces[k ^ 1 : (k ^ 1) + 1, :] for k in range(4)], axis=1)
    face_swap = jnp.broadcast_to(face_swap.astype(jnp.int32), (LANES, LANES))
    face_low = jnp.bitwise_and(face_swap[0:8], LANES - 1)
    face_high = jnp.right_shift(face_swap[0:8], 7)

    columns = jnp.concatenate(
        [conn_ref[...].astype(F32), jnp.zeros((LANES - nodes_el, LANES), F32)], axis=0
    ).T.astype(jnp.int32)

    def column(n):
        return jnp.broadcast_to(columns[:, n : n + 1], (LANES, LANES))

    def spot(n):
        j, p = n // 2, n % 2
        return slice(j * LANES, (j + 1) * LANES), slice(p * LANES, (p + 1) * LANES)

    for n in range(nodes_el):
        at_face[spot(n)] = jnp.where(column(n) == face_swap, 1.0, 0.0).astype(F8)

    def pack(x):
        high = x.astype(BF16).astype(F32)
        return jnp.concatenate([high, x - high], axis=0).astype(BF16)

    def face_forces(packs):
        res = jnp.dot(
            jnp.concatenate(packs, axis=1), at_face[...], preferred_element_type=F32
        )
        res = res[0:8] + res[8:16]
        mixed = jnp.where(row8 < 4, res[:, 0:LANES], res[:, LANES:])
        return mixed + pltpu.roll(mixed, 4, 0)

    def node_forces(packs):
        sides = []
        for b in range(blocks):
            sides.append(
                jnp.concatenate(
                    [
                        packs[j] * hmask[(j * blocks + b) * 16 : (j * blocks + b + 1) * 16, :]
                        for j in range(pairs_el)
                    ],
                    axis=1,
                )
            )
        res = jnp.dot(
            jnp.concatenate(sides, axis=0), at_node[...], preferred_element_type=F32
        )
        halves = []
        for b in range(blocks):
            one = res[16 * b : 16 * b + 8] + res[16 * b + 8 : 16 * b + 16]
            even, odd = one[:, 0:LANES], one[:, LANES:]
            if b % 2:
                halves.append(pltpu.roll(even, 4, 0) + odd)
            else:
                halves.append(even + pltpu.roll(odd, 4, 0))
        return jnp.concatenate(
            [jnp.where(row8 < 4, halves[b], halves[b + 1]) for b in range(0, blocks, 2)],
            axis=0,
        )

    landed(2, 5)
    quarter = jnp.right_shift(lax.broadcasted_iota(jnp.int32, (8, LANES), 1), 5)
    nb = nb_ref[...].astype(F32)
    recv_mask = [jnp.where(quarter == k, nb[:, k : k + 1], 0.0) for k in range(4)]

    def copies(slot):
        return [
            pltpu.make_async_remote_copy(
                src_ref=send.at[slot, 0:4],
                dst_ref=recv.at[slot, k ^ 1, 0:4],
                send_sem=send_sem.at[slot, k],
                recv_sem=recv_sem.at[slot, k ^ 1],
                device_id=where_to[k],
                device_id_type=MESH,
            )
            for k in range(4)
        ]

    def arrivals(slot):
        return [
            pltpu.make_async_remote_copy(
                src_ref=send.at[slot, 0:4],
                dst_ref=recv.at[slot, k, 0:4],
                send_sem=send_sem.at[slot, k],
                recv_sem=recv_sem.at[slot, k],
                device_id=where_to[k],
                device_id_type=MESH,
            )
            for k in range(4)
        ]

    def send_shared(message, slot):
        send[slot] = message
        for k, copy in enumerate(copies(slot)):

            @pl.when(has[k])
            def _():
                copy.start()

    def departed(slot):
        for k, copy in enumerate(copies(slot)):
            pl.when(has[k])(copy.wait_send)

    def shared_sum(slot):
        for k, copy in enumerate(arrivals(slot)):

            @pl.when(has[k])
            def _():
                copy.wait_recv()

        got = recv[slot, 0] * recv_mask[0]
        for k in range(1, 4):
            got = got + recv[slot, k] * recv_mask[k]
        return got

    masses = []
    for n in range(0, nodes_el, 2):
        mass = jnp.where(row8 == 3, mass_ref[n : n + 1, :], 0.0)
        masses.append(pack(mass + jnp.where(row8 == 7, mass_ref[n + 1 : n + 2, :], 0.0)))
    src_rows = []
    for b in range(blocks):
        src_rows.append(src_ref[:, b * LANES : (b + 1) * LANES])
        src_rows.append(jnp.zeros((1, LANES), F32))
    at_faces = jnp.zeros((8, LANES), F32)
    for b in range(blocks):
        rows = jnp.concatenate([src_rows[2 * b], jnp.zeros((5, LANES), F32)], axis=0)
        at_faces = jnp.where(face_high == b, pick_lanes(rows, face_low), at_faces)
    send_shared(face_forces(masses) + at_faces, 0)

    conn_low = jnp.bitwise_and(conn_ref[...], LANES - 1)
    conn_high = jnp.right_shift(conn_ref[...], 7)
    for n in range(nodes_el):
        low_column = jnp.bitwise_and(column(n), LANES - 1)
        at_node[spot(n)] = jnp.where(low_column == lane, 1.0, 0.0).astype(BF16)
    for j in range(pairs_el):
        two = [
            jnp.broadcast_to(conn_high[n : n + 1, :], (4, LANES)) for n in (2 * j, 2 * j + 1)
        ]
        two = jnp.concatenate(two * 2, axis=0)
        for b in range(blocks):
            hmask[(j * blocks + b) * 16 : (j * blocks + b + 1) * 16, :] = jnp.where(
                two == b, 1.0, 0.0
            ).astype(BF16)
    first = node_forces(masses) + jnp.concatenate(src_rows, axis=0)

    face_col = jnp.broadcast_to(face_row, (LANES, LANES)).T
    position = lax.broadcasted_iota(jnp.int32, (LANES, LANES), 0).astype(F32)
    inv_rows = []
    has_rows = []
    for b in range(blocks):
        hit = jnp.where(face_col == (lane + b * LANES).astype(F32), 1.0, 0.0)
        inv_rows.append(
            jnp.broadcast_to(jnp.sum(hit * position, axis=0, keepdims=True), (4, LANES))
        )
        has_rows.append(jnp.broadcast_to(jnp.sum(hit, axis=0, keepdims=True), (4, LANES)))
    inv_idx = jnp.concatenate(inv_rows, axis=0).astype(jnp.int32)
    inv_has = jnp.concatenate(has_rows, axis=0)

    def at_nodes(got):
        got = got + pltpu.roll(got, 4, 0)
        added = jnp.concatenate(
            [pick_lanes(got, inv_idx[0:8]), pick_lanes(got, inv_idx[8:16])], axis=0
        )
        return added * inv_has

    landed(5, len(arrays))
    weight = pw_ref[...]
    hi = weight.astype(BF16).astype(F32)
    pww[...] = jnp.concatenate(
        [hi, weight - hi, hi, jnp.zeros((LANES - depth, LANES), F32)], axis=0
    ).astype(BF16)
    jac = [jnp.broadcast_to(jac_ref[i : i + 1, :], (8, LANES)) for i in range(9)]
    lam = jnp.broadcast_to(lame_ref[0:1, :], (8, LANES))
    mu = jnp.broadcast_to(lame_ref[1:2, :], (8, LANES))

    def form_stiffness(m, carry):
        moments = jnp.dot(products[m], pww[...], preferred_element_type=F32)
        for p in range(2):
            for i in range(tiles):

                def moment(r, rp):
                    start = ((rp * 2 + p) * 3 + r) * padded + 8 * i
                    return moments[start : start + 8]

                half = [
                    [
                        jac[a] * moment(0, rp) + jac[3 + a] * moment(1, rp) + jac[6 + a] * moment(2, rp)
                        for rp in range(3)
                    ]
                    for a in range(3)
                ]
                full = [
                    [
                        jac[b] * half[a][0] + jac[3 + b] * half[a][1] + jac[6 + b] * half[a][2]
                        for b in range(3)
                    ]
                    for a in range(3)
                ]
                trace = mu * (full[0][0] + full[1][1] + full[2][2])
                for c in range(3):
                    for cp in range(3):
                        value = mu * full[cp][c] + lam * full[c][cp]
                        if c == cp:
                            value = value + trace
                        start = (p * 3 + cp) * 4 * padded + 32 * i + c
                        kmat[m, pl.ds(start, 8, stride=4), :] = value
        return carry

    group = 5 if pairs_el % 5 == 0 else 1

    def form_group(i, carry):
        for k in range(group):
            form_stiffness(i * group + k, carry)
        return carry

    lax.fori_loop(0, pairs_el // group, form_group, 0)

    first = first + at_nodes(shared_sum(0))
    axis_row = jnp.bitwise_and(row16, 3) < 3
    source = jnp.where(axis_row, first, 0.0)
    total = jnp.concatenate(
        [jnp.broadcast_to(first[4 * b + 3 : 4 * b + 4, :], (4, LANES)) for b in range(blocks)],
        axis=0,
    )
    half_inverse = jnp.where(axis_row, time_step / total, 0.0)

    spare = jnp.zeros((24 - nodes_el, LANES), jnp.int32)
    conn_low = jnp.concatenate([conn_low, spare], axis=0)
    conn_high = jnp.concatenate([conn_high, spare], axis=0)
    low = [conn_low[8 * i : 8 * i + 8, :] for i in range(3)]
    high = [conn_high[8 * i : 8 * i + 8, :] for i in range(3)]

    def at_elements(rows_of):
        out = []
        for i in range(3):
            acc = None
            for b in range(blocks):
                val = pick_lanes(jnp.broadcast_to(rows_of(b), (8, LANES)), low[i])
                acc = val if b == 0 else jnp.where(high[i] == b, val, acc)
            out.append(acc)
        return out

    def gather(u):
        return tuple(
            tuple(at_elements(lambda b: u[4 * b + c : 4 * b + c + 1, :])) for c in range(3)
        )

    def gradient(values):
        sides = []
        for c in range(3):
            rows = list(values[c]) + [jnp.zeros((8, LANES), F32)]
            hi, lo = split(jnp.concatenate(rows, axis=0))
            sides.append(jnp.concatenate([hi, lo, hi], axis=0))
        along = jnp.dot(
            w1[...], jnp.concatenate(sides, axis=1), preferred_element_type=F32
        )
        tensor = []
        for c in range(3):
            ref_dir = [
                along[r * points : (r + 1) * points, c * LANES : (c + 1) * LANES]
                for r in range(3)
            ]
            tensor.append(
                [
                    ref_dir[0] * jac_ref[e : e + 1, :]
                    + ref_dir[1] * jac_ref[3 + e : 4 + e, :]
                    + ref_dir[2] * jac_ref[6 + e : 7 + e, :]
                    for e in range(3)
                ]
            )
        return tensor

    def stiffness(values):
        for c in range(3):
            for i in range(tiles):
                start = c * padded + 8 * i
                at_el[start : start + 8, :] = values[c][i]
        sums = [None] * pairs_el
        for n in range(nodes_el):
            for cp in range(3):
                here = c_row(cp * padded + n)
                for j in range(pairs_el):
                    start = ((n % 2) * 3 + cp) * 4 * padded + 8 * j
                    term = kmat[n // 2, start : start + 8, :] * here
                    sums[j] = term if sums[j] is None else sums[j] + term
        return [pack(x) for x in sums]

    def c_row(i):
        return jnp.broadcast_to(at_el[i : i + 1, :], (8, LANES))

    def record(t):
        comps = [
            t[0][0],
            t[1][1],
            t[2][2],
            0.5 * (t[1][2] + t[2][1]),
            0.5 * (t[0][2] + t[2][0]),
            0.5 * (t[0][1] + t[1][0]),
        ]
        for c, value in enumerate(comps):
            snap[pl.ds(c, points, stride=8), :] = value

    def build_route():
        ranks = jnp.concatenate(
            [rank_ref[:, q * LANES : (q + 1) * LANES] for q in range(points)], axis=0
        )
        turned = jnp.concatenate(
            [ranks.astype(F32), jnp.zeros((LANES - points, LANES), F32)], axis=0
        ).T.astype(jnp.int32)
        upper = jnp.right_shift(ranks, 7)
        place_row = lax.broadcasted_iota(jnp.int32, (points, LANES), 0)
        lane_value = lax.broadcasted_iota(jnp.int32, (points, LANES), 1).astype(F32)
        sides = []
        for q in range(points):
            low = jnp.broadcast_to(turned[:, q : q + 1], (LANES, LANES))
            low = jnp.bitwise_and(low, LANES - 1)
            spread[q * LANES : (q + 1) * LANES, :] = jnp.where(low == lane, 1.0, 0.0).astype(BF16)
            mine_here = place_row == jnp.broadcast_to(upper[q : q + 1, :], (points, LANES))
            sides.append(
                jnp.concatenate(
                    [jnp.where(mine_here, float(q), 0.0), jnp.where(mine_here, lane_value, 0.0)],
                    axis=0,
                ).astype(BF16)
            )
        route[...] = jnp.dot(
            jnp.concatenate(sides, axis=1), spread[...], preferred_element_type=F32
        ).astype(jnp.int32)

    def in_order(k):
        origin = jnp.broadcast_to(route[pl.ds(k, 1), :], (8, LANES))
        at = jnp.broadcast_to(route[pl.ds(points + k, 1), :], (8, LANES))
        value = pick_lanes(snap[0:8, :], at)
        for q in range(1, points):
            value = jnp.where(origin == q, pick_lanes(snap[8 * q : 8 * q + 8, :], at), value)
        return value

    def keep(parity):
        for k in range(points):
            mixed[k, pl.ds(parity, 8, stride=2), :] = in_order(k)

    velocity = wav_ref[0] * source * half_inverse
    displace = time_step * velocity

    def mine(i):
        return pl.ds(pl.multiple_of(i * block, block), block)

    def parcel(chunk, i, column, target):
        return pltpu.make_async_remote_copy(
            src_ref=pair.at[chunk, :, mine(target)],
            dst_ref=pair_in.at[chunk, :, mine(column)],
            send_sem=out_send_sem.at[chunk, i],
            recv_sem=out_recv_sem.at[chunk, i],
            device_id=(g, target),
            device_id_type=MESH,
        )

    def dispatch(make, local):
        for i in range(1, writers):
            make(i, d, lax.rem(my_d + i, writers)).start()

        @pl.when(other_core)
        def _():
            make(0, d, my_d).start()

        pl.when(jnp.logical_not(other_core))(local)

    def collect(make):
        for i in range(1, writers):
            origin = lax.rem(my_d - i + writers, writers)
            make(i, along(origin), origin).wait_recv()
            make(i, d, lax.rem(my_d + i, writers)).wait_send()

        @pl.when(other_core)
        def _():
            make(0, d, my_d).wait_recv()
            make(0, d, my_d).wait_send()

    def close_pair(chunk):
        for k in range(points):
            pair[chunk, :, k * LANES : (k + 1) * LANES] = mixed[k].astype(BF16)

    def send_pair(chunk):
        def local():
            pair_in[chunk, :, mine(d)] = pair[chunk, :, mine(my_d)]

        dispatch(functools.partial(parcel, chunk), local)

    def send_last(chunk):
        each = block // LANES
        for i in [*range(1, writers, 2), *range(2, writers, 2), 0]:
            w = lax.rem(my_d + i, writers)
            for k in range(each):
                at = w * each + k
                mixed[at, pl.ds(1, 8, stride=2), :] = in_order(at)
                start = pl.multiple_of(at * LANES, LANES)
                pair[chunk, :, pl.ds(start, LANES)] = mixed[at].astype(BF16)
            if i:
                parcel(chunk, i, d, w).start()

        @pl.when(other_core)
        def _():
            parcel(chunk, 0, d, my_d).start()

        @pl.when(jnp.logical_not(other_core))
        def _():
            pair_in[chunk, :, mine(d)] = pair[chunk, :, mine(my_d)]

    def merge(chunk):
        collect(functools.partial(parcel, chunk))
        for c in range(6):
            out_ref[c, 2 * chunk : 2 * chunk + 2, :] = pair_in[chunk, 2 * c : 2 * c + 2, :]

    def launch(t, odd, values, got, displace, velocity, early, extra):
        packs = stiffness(values)
        send_shared(face_forces(packs), odd)
        departed(1 - odd)
        record(gradient(values))
        if got is not None:
            change = half_inverse * at_nodes(got)
            velocity = velocity - change
            displace = displace - time_step * change
        velocity = velocity + half_inverse * (wav_ref[t] * source - node_forces(packs))
        displace = displace + time_step * velocity
        values = gather(displace)
        extra()
        early()
        keep(1 - odd)
        return values, displace, velocity

    def nothing():
        return None

    state = launch(
        1, 1, gather(displace), None, displace, velocity, nothing, build_route
    )

    inv_f = inv_idx.astype(F32)
    place = [x.astype(jnp.int32) for x in at_elements(lambda b: inv_f[4 * b : 4 * b + 1, :])]
    coef = (-time_step) * half_inverse * inv_has
    coef = at_elements(lambda b: coef[4 * b : 4 * b + 1, :])

    def corrected(values, got):
        out = []
        for c in range(3):
            row = jnp.broadcast_to(got[c : c + 1, :], (8, LANES))
            out.append(
                tuple(values[c][i] + pick_lanes(row, place[i]) * coef[i] for i in range(3))
            )
        return tuple(out)

    def advance(t, odd, state, early):
        values, displace, velocity = state
        got = shared_sum(1 - odd)
        return launch(t, odd, corrected(values, got), got, displace, velocity, early, nothing)

    def two_steps(i, state):
        def early():
            @pl.when((i >= 2) & (lax.rem(chunks - 1 - i, 2) == 0))
            def _():
                if chunks % 2:
                    pl.when(i >= 3)(lambda: send_pair(i - 3))
                else:
                    send_pair(i - 3)
                send_pair(i - 2)

        state = advance(2 * i, 0, state, early)
        close_pair(i - 1)
        return advance(2 * i + 1, 1, state, nothing)

    state = lax.fori_loop(1, chunks, two_steps, state)
    send_pair(chunks - 2)
    for chunk in range(chunks - 2):
        merge(chunk)
    got = shared_sum(1)
    record(gradient(corrected(state[0], got)))
    if block % LANES:
        keep(1)
        close_pair(chunks - 1)
        send_pair(chunks - 1)
    else:
        send_last(chunks - 1)
    departed(1)
    merge(chunks - 2)
    merge(chunks - 1)


def solution(mesh):
    groups, writers = mesh.shape["grp"], mesh.shape["dom"]

    def shards(
        connect,
        interface_nodes,
        neighbours,
        point_rank,
        shape_grad,
        inverse_jacobian,
        lame_moduli,
        point_weights,
        mass_elem,
        source_pattern,
        wavelet,
    ):
        nodes_el, elements = connect.shape
        points = point_weights.shape[0]
        point_count = point_rank.shape[1]
        steps = wavelet.shape[0]
        padded = -(-nodes_el // 8) * 8
        vmem = pl.BlockSpec(memory_space=pltpu.VMEM)
        hbm = pl.BlockSpec(memory_space=pl.ANY)
        sharded = (
            connect,
            interface_nodes,
            neighbours,
            point_rank,
            inverse_jacobian,
            lame_moduli,
            point_weights,
            mass_elem,
            source_pattern,
        )
        ordered = pl.pallas_call(
            functools.partial(kernel, groups, writers, steps, nodes_el),
            out_shape=pltpu.VMEM((6, steps, point_count), BF16),
            in_specs=[hbm] * (len(sharded) + 2),
            out_specs=vmem,
            scratch_shapes=[pltpu.VMEM(a.shape, a.dtype) for a in sharded] * 2
            + [pltpu.VMEM(shape_grad.shape[::-1], F32), pltpu.SMEM(wavelet.shape, F32)]
            + [pltpu.SemaphoreType.DMA((len(sharded) + 2,))] * 3
            + [
                pltpu.VMEM((nodes_el // 2 * LANES, 2 * LANES), F8),
                pltpu.VMEM((nodes_el // 2 * LANES, 2 * LANES), BF16),
                pltpu.VMEM((nodes_el // 2 * (source_pattern.shape[1] // LANES) * 16, LANES), BF16),
                pltpu.VMEM((3, padded, LANES), F32),
                pltpu.VMEM((nodes_el // 2, 18 * padded, LANES), BF16),
                pltpu.VMEM((LANES, LANES), BF16),
                pltpu.VMEM((nodes_el // 2, 24 * padded, LANES), F32),
                pltpu.VMEM((3 * padded, LANES), F32),
                pltpu.VMEM((3 * points, 96), BF16),
                pltpu.VMEM((8 * points, LANES), F32),
                pltpu.VMEM((points * LANES, LANES), BF16),
                pltpu.VMEM((2 * points, LANES), jnp.int32),
                pltpu.VMEM((points, 16, LANES), F32),
                pltpu.VMEM((steps // 2, 16, point_count), BF16),
                pltpu.VMEM((steps // 2, 16, point_count), BF16),
                pltpu.VMEM((2, 8, LANES), F32),
                pltpu.VMEM((2, 4, 8, LANES), F32),
                pltpu.SemaphoreType.DMA((2, 4)),
                pltpu.SemaphoreType.DMA((2, 4)),
                pltpu.SemaphoreType.DMA((steps // 2, writers)),
                pltpu.SemaphoreType.DMA((steps // 2, writers)),
            ],
            compiler_params=pltpu.CompilerParams(
                collective_id=0, has_side_effects=True, vmem_limit_bytes=56 * 1024 * 1024
            ),
            name="window",
        )(
            *sharded,
            shape_grad.T,
            wavelet,
        )
        return ordered.transpose(1, 0, 2)

    placed = (
        P(None, ("grp", "dom")),
        P(("grp", "dom"), None, None),
        P(("grp", "dom"), None),
        P(("grp", "dom"), None),
        P(),
        P(None, ("grp", "dom")),
        P(None, ("grp", "dom")),
        P(None, ("grp", "dom")),
        P(None, ("grp", "dom")),
        P(None, ("grp", "dom")),
        P(),
    )
    return jax.shard_map(
        shards, mesh=mesh, in_specs=placed, out_specs=P(None, None, ("grp", "dom")), check_vma=False
    )
```

```python
import functools

import jax
import jax.numpy as jnp
from jax import lax
from jax.experimental import pallas as pl
from jax.experimental.pallas import tpu as pltpu
from jax.sharding import PartitionSpec as P

MESH = pl.DeviceIdType.MESH
F32 = jnp.float32
BF16 = jnp.bfloat16
F8 = jnp.float8_e4m3fn
time_step = 0.5
LANES = 128


def split(x):
    hi = x.astype(BF16)
    return hi, (x - hi.astype(F32)).astype(BF16)


def pick_lanes(x, idx):
    return jnp.take_along_axis(x, idx, axis=1, mode="promise_in_bounds")


def kernel(
    groups,
    writers,
    steps,
    nodes_el,
    conn_in,
    faces_in,
    nb_in,
    rank_in,
    jac_in,
    lame_in,
    pw_in,
    mass_in,
    src_in,
    gradt_in,
    wav_in,
    out_ref,
    conn_ref,
    faces_ref,
    nb_ref,
    rank_ref,
    jac_ref,
    lame_ref,
    pw_ref,
    mass_ref,
    src_ref,
    conn_own,
    faces_own,
    nb_own,
    rank_own,
    jac_own,
    lame_own,
    pw_own,
    mass_own,
    src_own,
    gradt_ref,
    wav_ref,
    move_sem,
    move_send_sem,
    move_recv_sem,
    at_face,
    at_node,
    hmask,
    basis,
    products,
    pww,
    kmat,
    at_el,
    w1,
    snap,
    spread,
    route,
    mixed,
    pair,
    pair_in,
    send,
    recv,
    send_sem,
    recv_sem,
    out_send_sem,
    out_recv_sem,
):
    my_g = lax.axis_index("grp")
    my_d = lax.axis_index("dom")
    points = pw_ref.shape[0]
    block = out_ref.shape[2] // writers
    blocks = src_ref.shape[1] // LANES

    def along(w):
        if writers % 4:
            return w
        return w + lax.rem(w // 2, 2) * (1 - 2 * lax.rem(w, 2))

    def across(g, w):
        if groups % 2:
            return g
        return g + lax.rem(w, 2) * (1 - 2 * lax.rem(g, 2))

    def host(g, w):
        return across(g, w), along(w)

    d = along(my_d)
    g = across(my_g, d)
    stays = (g == my_g) & (d == my_d)
    moves = jnp.logical_not(stays)
    other_core = g != my_g
    target = host(my_g, my_d)

    has = (g > 0, g < groups - 1, d > 0, d < writers - 1)
    where_to = (host(g - 1, d), host(g + 1, d), host(g, d - 1), host(g, d + 1))

    arrays = (
        (conn_in, conn_own, conn_ref),
        (faces_in, faces_own, faces_ref),
        (mass_in, mass_own, mass_ref),
        (src_in, src_own, src_ref),
        (nb_in, nb_own, nb_ref),
        (pw_in, pw_own, pw_ref),
        (jac_in, jac_own, jac_ref),
        (lame_in, lame_own, lame_ref),
        (rank_in, rank_own, rank_ref),
    )

    def fetch(i, kept):
        return pltpu.make_async_copy(
            arrays[i][0], arrays[i][2 if kept else 1], move_sem.at[i]
        )

    def move(i):
        return pltpu.make_async_remote_copy(
            src_ref=arrays[i][1],
            dst_ref=arrays[i][2],
            send_sem=move_send_sem.at[i],
            recv_sem=move_recv_sem.at[i],
            device_id=target,
            device_id_type=MESH,
        )

    recv[...] = jnp.zeros_like(recv)
    barrier = pltpu.get_barrier_semaphore()
    shared = (
        pltpu.make_async_copy(gradt_in, gradt_ref, move_sem.at[len(arrays)]),
        pltpu.make_async_copy(wav_in, wav_ref, move_sem.at[len(arrays) + 1]),
    )

    @pl.when(moves)
    def _():
        pl.semaphore_signal(barrier, inc=1, device_id=(g, d), device_id_type=MESH)

    for k in range(4):

        @pl.when(has[k])
        def _():
            pl.semaphore_signal(barrier, inc=1, device_id=where_to[k], device_id_type=MESH)

    near = writers <= 4
    for i in range(0 if near else writers):
        origin_d = lax.rem(my_d + i, writers)
        origin = (across(my_g, along(origin_d)), origin_d)

        def greet():
            pl.semaphore_signal(barrier, inc=1, device_id=origin, device_id_type=MESH)

        if i:
            greet()
        else:
            pl.when(other_core)(greet)

    @pl.when(stays)
    def _():
        for i in range(len(arrays)):
            fetch(i, True).start()

    @pl.when(moves)
    def _():
        for i in range(len(arrays)):
            fetch(i, False).start()

    for copy in shared:
        copy.start()
    expected = moves.astype(jnp.int32)
    if not near:
        expected = expected + other_core.astype(jnp.int32) + writers - 1
    for k in range(4):
        expected = expected + has[k].astype(jnp.int32)
    pl.semaphore_wait(barrier, expected)

    @pl.when(moves)
    def _():
        for i in range(len(arrays)):
            fetch(i, False).wait()
            move(i).start()

    def landed(lo, hi):
        @pl.when(stays)
        def _():
            for i in range(lo, hi):
                fetch(i, True).wait()

        @pl.when(moves)
        def _():
            for i in range(lo, hi):
                move(i).wait_recv()
                move(i).wait_send()


    lane = lax.broadcasted_iota(jnp.int32, (LANES, LANES), 1)
    row8 = lax.broadcasted_iota(jnp.int32, (8, LANES), 0)
    row16 = lax.broadcasted_iota(jnp.int32, (16, LANES), 0)
    pairs_el = nodes_el // 2
    padded = -(-nodes_el // 8) * 8
    tiles = padded // 8

    for copy in shared:
        copy.wait()
    gradt = gradt_ref[...]
    depth = 3 * points
    hi = gradt.astype(BF16).astype(F32)
    lo = gradt - hi
    gap = jnp.zeros((32 - nodes_el, depth), F32)
    tall = jnp.concatenate([hi, gap, hi, gap, lo, gap, jnp.zeros((32, depth), F32)], axis=0)
    tall = jnp.concatenate([tall, jnp.zeros((LANES, LANES - depth), F32)], axis=1)
    w1[...] = tall.T[0:depth, 0:96].astype(BF16)

    lanes = lax.broadcasted_iota(jnp.int32, (padded, LANES), 1)
    base = jnp.concatenate([gradt, jnp.zeros((padded - nodes_el, depth), F32)], axis=0)
    base = jnp.concatenate([base, jnp.zeros((padded, LANES - depth), F32)], axis=1)
    own_dir = []
    for r in range(3):
        x = pltpu.roll(base, LANES - r * points, 1) if r else base
        x = jnp.where(lanes < points, x, 0.0)
        x = x + pltpu.roll(x, points, 1) + pltpu.roll(x, 2 * points, 1)
        own_dir.append(x)
        basis[r] = x

    def multiply_pairs(m, carry):
        for rp in range(3):
            parts = []
            for p in range(2):
                other = basis[rp, pl.ds(2 * m + p, 1), :]
                for r in range(3):
                    product = own_dir[r] * other
                    high = product.astype(BF16).astype(F32)
                    parts.append(jnp.where(lanes < 2 * points, high, product - high))
            rows = 6 * padded
            products[m, rp * rows : (rp + 1) * rows, :] = jnp.concatenate(
                parts, axis=0
            ).astype(BF16)
        return carry

    lax.fori_loop(0, pairs_el, multiply_pairs, 0)

    def clear(m, carry):
        kmat[m] = jnp.zeros(kmat.shape[1:], F32)
        return carry

    lax.fori_loop(0, pairs_el, clear, 0)

    chunks = steps // 2
    snap[...] = jnp.zeros_like(snap)

    landed(0, 2)
    faces = faces_ref[0].astype(F32)
    face_row = jnp.concatenate([faces[k : k + 1, :] for k in range(4)], axis=1)
    face_swap = jnp.concatenate([faces[k ^ 1 : (k ^ 1) + 1, :] for k in range(4)], axis=1)
    face_swap = jnp.broadcast_to(face_swap.astype(jnp.int32), (LANES, LANES))
    face_low = jnp.bitwise_and(face_swap[0:8], LANES - 1)
    face_high = jnp.right_shift(face_swap[0:8], 7)

    columns = jnp.concatenate(
        [conn_ref[...].astype(F32), jnp.zeros((LANES - nodes_el, LANES), F32)], axis=0
    ).T.astype(jnp.int32)

    def column(n):
        return jnp.broadcast_to(columns[:, n : n + 1], (LANES, LANES))

    def spot(n):
        j, p = n // 2, n % 2
        return slice(j * LANES, (j + 1) * LANES), slice(p * LANES, (p + 1) * LANES)

    for n in range(nodes_el):
        at_face[spot(n)] = jnp.where(column(n) == face_swap, 1.0, 0.0).astype(F8)

    def pack(x):
        high = x.astype(BF16).astype(F32)
        return jnp.concatenate([high, x - high], axis=0).astype(BF16)

    def face_forces(packs):
        res = jnp.dot(
            jnp.concatenate(packs, axis=1), at_face[...], preferred_element_type=F32
        )
        res = res[0:8] + res[8:16]
        mixed = jnp.where(row8 < 4, res[:, 0:LANES], res[:, LANES:])
        return mixed + pltpu.roll(mixed, 4, 0)

    def node_forces(packs):
        sides = []
        for b in range(blocks):
            sides.append(
                jnp.concatenate(
                    [
                        packs[j] * hmask[(j * blocks + b) * 16 : (j * blocks + b + 1) * 16, :]
                        for j in range(pairs_el)
                    ],
                    axis=1,
                )
            )
        res = jnp.dot(
            jnp.concatenate(sides, axis=0), at_node[...], preferred_element_type=F32
        )
        halves = []
        for b in range(blocks):
            one = res[16 * b : 16 * b + 8] + res[16 * b + 8 : 16 * b + 16]
            even, odd = one[:, 0:LANES], one[:, LANES:]
            if b % 2:
                halves.append(pltpu.roll(even, 4, 0) + odd)
            else:
                halves.append(even + pltpu.roll(odd, 4, 0))
        return jnp.concatenate(
            [jnp.where(row8 < 4, halves[b], halves[b + 1]) for b in range(0, blocks, 2)],
            axis=0,
        )

    landed(2, 5)
    quarter = jnp.right_shift(lax.broadcasted_iota(jnp.int32, (8, LANES), 1), 5)
    nb = nb_ref[...].astype(F32)
    recv_mask = [jnp.where(quarter == k, nb[:, k : k + 1], 0.0) for k in range(4)]

    def copies(slot):
        return [
            pltpu.make_async_remote_copy(
                src_ref=send.at[slot, 0:4],
                dst_ref=recv.at[slot, k ^ 1, 0:4],
                send_sem=send_sem.at[slot, k],
                recv_sem=recv_sem.at[slot, k ^ 1],
                device_id=where_to[k],
                device_id_type=MESH,
            )
            for k in range(4)
        ]

    def arrivals(slot):
        return [
            pltpu.make_async_remote_copy(
                src_ref=send.at[slot, 0:4],
                dst_ref=recv.at[slot, k, 0:4],
                send_sem=send_sem.at[slot, k],
                recv_sem=recv_sem.at[slot, k],
                device_id=where_to[k],
                device_id_type=MESH,
            )
            for k in range(4)
        ]

    def send_shared(message, slot):
        send[slot] = message
        for k, copy in enumerate(copies(slot)):

            @pl.when(has[k])
            def _():
                copy.start()

    def departed(slot):
        for k, copy in enumerate(copies(slot)):
            pl.when(has[k])(copy.wait_send)

    def shared_sum(slot):
        for k, copy in enumerate(arrivals(slot)):

            @pl.when(has[k])
            def _():
                copy.wait_recv()

        got = recv[slot, 0] * recv_mask[0]
        for k in range(1, 4):
            got = got + recv[slot, k] * recv_mask[k]
        return got

    masses = []
    for n in range(0, nodes_el, 2):
        mass = jnp.where(row8 == 3, mass_ref[n : n + 1, :], 0.0)
        masses.append(pack(mass + jnp.where(row8 == 7, mass_ref[n + 1 : n + 2, :], 0.0)))
    src_rows = []
    for b in range(blocks):
        src_rows.append(src_ref[:, b * LANES : (b + 1) * LANES])
        src_rows.append(jnp.zeros((1, LANES), F32))
    at_faces = jnp.zeros((8, LANES), F32)
    for b in range(blocks):
        rows = jnp.concatenate([src_rows[2 * b], jnp.zeros((5, LANES), F32)], axis=0)
        at_faces = jnp.where(face_high == b, pick_lanes(rows, face_low), at_faces)
    send_shared(face_forces(masses) + at_faces, 0)

    conn_low = jnp.bitwise_and(conn_ref[...], LANES - 1)
    conn_high = jnp.right_shift(conn_ref[...], 7)
    for n in range(nodes_el):
        low_column = jnp.bitwise_and(column(n), LANES - 1)
        at_node[spot(n)] = jnp.where(low_column == lane, 1.0, 0.0).astype(BF16)
    for j in range(pairs_el):
        two = [
            jnp.broadcast_to(conn_high[n : n + 1, :], (4, LANES)) for n in (2 * j, 2 * j + 1)
        ]
        two = jnp.concatenate(two * 2, axis=0)
        for b in range(blocks):
            hmask[(j * blocks + b) * 16 : (j * blocks + b + 1) * 16, :] = jnp.where(
                two == b, 1.0, 0.0
            ).astype(BF16)
    first = node_forces(masses) + jnp.concatenate(src_rows, axis=0)

    face_col = jnp.broadcast_to(face_row, (LANES, LANES)).T
    position = lax.broadcasted_iota(jnp.int32, (LANES, LANES), 0).astype(F32)
    inv_rows = []
    has_rows = []
    for b in range(blocks):
        hit = jnp.where(face_col == (lane + b * LANES).astype(F32), 1.0, 0.0)
        inv_rows.append(
            jnp.broadcast_to(jnp.sum(hit * position, axis=0, keepdims=True), (4, LANES))
        )
        has_rows.append(jnp.broadcast_to(jnp.sum(hit, axis=0, keepdims=True), (4, LANES)))
    inv_idx = jnp.concatenate(inv_rows, axis=0).astype(jnp.int32)
    inv_has = jnp.concatenate(has_rows, axis=0)

    def at_nodes(got):
        got = got + pltpu.roll(got, 4, 0)
        added = jnp.concatenate(
            [pick_lanes(got, inv_idx[0:8]), pick_lanes(got, inv_idx[8:16])], axis=0
        )
        return added * inv_has

    landed(5, len(arrays))
    weight = pw_ref[...]
    hi = weight.astype(BF16).astype(F32)
    pww[...] = jnp.concatenate(
        [hi, weight - hi, hi, jnp.zeros((LANES - depth, LANES), F32)], axis=0
    ).astype(BF16)
    jac = [jnp.broadcast_to(jac_ref[i : i + 1, :], (8, LANES)) for i in range(9)]
    lam = jnp.broadcast_to(lame_ref[0:1, :], (8, LANES))
    mu = jnp.broadcast_to(lame_ref[1:2, :], (8, LANES))

    def form_stiffness(m, carry):
        moments = jnp.dot(products[m], pww[...], preferred_element_type=F32)
        for p in range(2):
            for i in range(tiles):

                def moment(r, rp):
                    start = ((rp * 2 + p) * 3 + r) * padded + 8 * i
                    return moments[start : start + 8]

                half = [
                    [
                        jac[a] * moment(0, rp) + jac[3 + a] * moment(1, rp) + jac[6 + a] * moment(2, rp)
                        for rp in range(3)
                    ]
                    for a in range(3)
                ]
                full = [
                    [
                        jac[b] * half[a][0] + jac[3 + b] * half[a][1] + jac[6 + b] * half[a][2]
                        for b in range(3)
                    ]
                    for a in range(3)
                ]
                trace = mu * (full[0][0] + full[1][1] + full[2][2])
                for c in range(3):
                    for cp in range(3):
                        value = mu * full[cp][c] + lam * full[c][cp]
                        if c == cp:
                            value = value + trace
                        start = (p * 3 + cp) * 4 * padded + 32 * i + c
                        kmat[m, pl.ds(start, 8, stride=4), :] = value
        return carry

    group = 5 if pairs_el % 5 == 0 else 1

    def form_group(i, carry):
        for k in range(group):
            form_stiffness(i * group + k, carry)
        return carry

    lax.fori_loop(0, pairs_el // group, form_group, 0)

    first = first + at_nodes(shared_sum(0))
    axis_row = jnp.bitwise_and(row16, 3) < 3
    source = jnp.where(axis_row, first, 0.0)
    total = jnp.concatenate(
        [jnp.broadcast_to(first[4 * b + 3 : 4 * b + 4, :], (4, LANES)) for b in range(blocks)],
        axis=0,
    )
    half_inverse = jnp.where(axis_row, time_step / total, 0.0)

    spare = jnp.zeros((24 - nodes_el, LANES), jnp.int32)
    conn_low = jnp.concatenate([conn_low, spare], axis=0)
    conn_high = jnp.concatenate([conn_high, spare], axis=0)
    low = [conn_low[8 * i : 8 * i + 8, :] for i in range(3)]
    high = [conn_high[8 * i : 8 * i + 8, :] for i in range(3)]

    def at_elements(rows_of):
        out = []
        for i in range(3):
            acc = None
            for b in range(blocks):
                val = pick_lanes(jnp.broadcast_to(rows_of(b), (8, LANES)), low[i])
                acc = val if b == 0 else jnp.where(high[i] == b, val, acc)
            out.append(acc)
        return out

    def gather(u):
        return tuple(
            tuple(at_elements(lambda b: u[4 * b + c : 4 * b + c + 1, :])) for c in range(3)
        )

    def gradient(values):
        sides = []
        for c in range(3):
            rows = list(values[c]) + [jnp.zeros((8, LANES), F32)]
            hi, lo = split(jnp.concatenate(rows, axis=0))
            sides.append(jnp.concatenate([hi, lo, hi], axis=0))
        along = jnp.dot(
            w1[...], jnp.concatenate(sides, axis=1), preferred_element_type=F32
        )
        tensor = []
        for c in range(3):
            ref_dir = [
                along[r * points : (r + 1) * points, c * LANES : (c + 1) * LANES]
                for r in range(3)
            ]
            tensor.append(
                [
                    ref_dir[0] * jac_ref[e : e + 1, :]
                    + ref_dir[1] * jac_ref[3 + e : 4 + e, :]
                    + ref_dir[2] * jac_ref[6 + e : 7 + e, :]
                    for e in range(3)
                ]
            )
        return tensor

    def stiffness(values):
        for c in range(3):
            for i in range(tiles):
                start = c * padded + 8 * i
                at_el[start : start + 8, :] = values[c][i]
        sums = [None] * pairs_el
        for n in range(nodes_el):
            for cp in range(3):
                here = c_row(cp * padded + n)
                for j in range(pairs_el):
                    start = ((n % 2) * 3 + cp) * 4 * padded + 8 * j
                    term = kmat[n // 2, start : start + 8, :] * here
                    sums[j] = term if sums[j] is None else sums[j] + term
        return [pack(x) for x in sums]

    def c_row(i):
        return jnp.broadcast_to(at_el[i : i + 1, :], (8, LANES))

    def record(t):
        comps = [
            t[0][0],
            t[1][1],
            t[2][2],
            0.5 * (t[1][2] + t[2][1]),
            0.5 * (t[0][2] + t[2][0]),
            0.5 * (t[0][1] + t[1][0]),
        ]
        for c, value in enumerate(comps):
            snap[pl.ds(c, points, stride=8), :] = value

    def build_route():
        ranks = jnp.concatenate(
            [rank_ref[:, q * LANES : (q + 1) * LANES] for q in range(points)], axis=0
        )
        turned = jnp.concatenate(
            [ranks.astype(F32), jnp.zeros((LANES - points, LANES), F32)], axis=0
        ).T.astype(jnp.int32)
        upper = jnp.right_shift(ranks, 7)
        place_row = lax.broadcasted_iota(jnp.int32, (points, LANES), 0)
        lane_value = lax.broadcasted_iota(jnp.int32, (points, LANES), 1).astype(F32)
        sides = []
        for q in range(points):
            low = jnp.broadcast_to(turned[:, q : q + 1], (LANES, LANES))
            low = jnp.bitwise_and(low, LANES - 1)
            spread[q * LANES : (q + 1) * LANES, :] = jnp.where(low == lane, 1.0, 0.0).astype(BF16)
            mine_here = place_row == jnp.broadcast_to(upper[q : q + 1, :], (points, LANES))
            sides.append(
                jnp.concatenate(
                    [jnp.where(mine_here, float(q), 0.0), jnp.where(mine_here, lane_value, 0.0)],
                    axis=0,
                ).astype(BF16)
            )
        route[...] = jnp.dot(
            jnp.concatenate(sides, axis=1), spread[...], preferred_element_type=F32
        ).astype(jnp.int32)

    def in_order(k):
        origin = jnp.broadcast_to(route[pl.ds(k, 1), :], (8, LANES))
        at = jnp.broadcast_to(route[pl.ds(points + k, 1), :], (8, LANES))
        value = pick_lanes(snap[0:8, :], at)
        for q in range(1, points):
            value = jnp.where(origin == q, pick_lanes(snap[8 * q : 8 * q + 8, :], at), value)
        return value

    def keep(parity):
        for k in range(points):
            mixed[k, pl.ds(parity, 8, stride=2), :] = in_order(k)

    velocity = wav_ref[0] * source * half_inverse
    displace = time_step * velocity

    def mine(i):
        return pl.ds(pl.multiple_of(i * block, block), block)

    def parcel(chunk, i, column, target):
        return pltpu.make_async_remote_copy(
            src_ref=pair.at[chunk, :, mine(target)],
            dst_ref=pair_in.at[chunk, :, mine(column)],
            send_sem=out_send_sem.at[chunk, i],
            recv_sem=out_recv_sem.at[chunk, i],
            device_id=(g, target),
            device_id_type=MESH,
        )

    def dispatch(make, local):
        for i in range(1, writers):
            make(i, d, lax.rem(my_d + i, writers)).start()

        @pl.when(other_core)
        def _():
            make(0, d, my_d).start()

        pl.when(jnp.logical_not(other_core))(local)

    def collect(make):
        for i in range(1, writers):
            origin = lax.rem(my_d - i + writers, writers)
            make(i, along(origin), origin).wait_recv()
            make(i, d, lax.rem(my_d + i, writers)).wait_send()

        @pl.when(other_core)
        def _():
            make(0, d, my_d).wait_recv()
            make(0, d, my_d).wait_send()

    def close_pair(chunk):
        for k in range(points):
            pair[chunk, :, k * LANES : (k + 1) * LANES] = mixed[k].astype(BF16)

    def send_pair(chunk):
        def local():
            pair_in[chunk, :, mine(d)] = pair[chunk, :, mine(my_d)]

        dispatch(functools.partial(parcel, chunk), local)

    def send_last(chunk):
        each = block // LANES
        for i in [*range(1, writers, 2), *range(2, writers, 2), 0]:
            odd_pair = i % 2 and writers % 2 == 0
            i = jnp.where(lax.rem(my_d, 2) == 0, writers - i, i) if odd_pair else i
            w = lax.rem(my_d + i, writers)
            for k in range(each):
                at = w * each + k
                mixed[at, pl.ds(1, 8, stride=2), :] = in_order(at)
                start = pl.multiple_of(at * LANES, LANES)
                pair[chunk, :, pl.ds(start, LANES)] = mixed[at].astype(BF16)
            if odd_pair or i:
                parcel(chunk, i, d, w).start()

        @pl.when(other_core)
        def _():
            parcel(chunk, 0, d, my_d).start()

        @pl.when(jnp.logical_not(other_core))
        def _():
            pair_in[chunk, :, mine(d)] = pair[chunk, :, mine(my_d)]

    def merge(chunk):
        collect(functools.partial(parcel, chunk))
        for c in range(6):
            out_ref[c, 2 * chunk : 2 * chunk + 2, :] = pair_in[chunk, 2 * c : 2 * c + 2, :]

    def launch(t, odd, values, got, displace, velocity, early, extra):
        packs = stiffness(values)
        send_shared(face_forces(packs), odd)
        departed(1 - odd)
        record(gradient(values))
        if got is not None:
            change = half_inverse * at_nodes(got)
            velocity = velocity - change
            displace = displace - time_step * change
        velocity = velocity + half_inverse * (wav_ref[t] * source - node_forces(packs))
        displace = displace + time_step * velocity
        values = gather(displace)
        extra()
        early()
        keep(1 - odd)
        return values, displace, velocity

    def nothing():
        return None

    state = launch(
        1, 1, gather(displace), None, displace, velocity, nothing, build_route
    )

    inv_f = inv_idx.astype(F32)
    place = [x.astype(jnp.int32) for x in at_elements(lambda b: inv_f[4 * b : 4 * b + 1, :])]
    coef = (-time_step) * half_inverse * inv_has
    coef = at_elements(lambda b: coef[4 * b : 4 * b + 1, :])

    def corrected(values, got):
        out = []
        for c in range(3):
            row = jnp.broadcast_to(got[c : c + 1, :], (8, LANES))
            out.append(
                tuple(values[c][i] + pick_lanes(row, place[i]) * coef[i] for i in range(3))
            )
        return tuple(out)

    def advance(t, odd, state, early):
        values, displace, velocity = state
        got = shared_sum(1 - odd)
        return launch(t, odd, corrected(values, got), got, displace, velocity, early, nothing)

    def two_steps(i, state):
        def early():
            @pl.when((i >= 2) & (lax.rem(chunks - 1 - i, 2) == 0))
            def _():
                if chunks % 2:
                    pl.when(i >= 3)(lambda: send_pair(i - 3))
                else:
                    send_pair(i - 3)
                send_pair(i - 2)

        state = advance(2 * i, 0, state, early)
        close_pair(i - 1)
        return advance(2 * i + 1, 1, state, nothing)

    state = lax.fori_loop(1, chunks, two_steps, state)
    send_pair(chunks - 2)
    for chunk in range(chunks - 2):
        merge(chunk)
    got = shared_sum(1)
    record(gradient(corrected(state[0], got)))
    if block % LANES:
        keep(1)
        close_pair(chunks - 1)
        send_pair(chunks - 1)
    else:
        send_last(chunks - 1)
    departed(1)
    merge(chunks - 2)
    merge(chunks - 1)


def solution(mesh):
    groups, writers = mesh.shape["grp"], mesh.shape["dom"]

    def shards(
        connect,
        interface_nodes,
        neighbours,
        point_rank,
        shape_grad,
        inverse_jacobian,
        lame_moduli,
        point_weights,
        mass_elem,
        source_pattern,
        wavelet,
    ):
        nodes_el, elements = connect.shape
        points = point_weights.shape[0]
        point_count = point_rank.shape[1]
        steps = wavelet.shape[0]
        padded = -(-nodes_el // 8) * 8
        vmem = pl.BlockSpec(memory_space=pltpu.VMEM)
        hbm = pl.BlockSpec(memory_space=pl.ANY)
        sharded = (
            connect,
            interface_nodes,
            neighbours,
            point_rank,
            inverse_jacobian,
            lame_moduli,
            point_weights,
            mass_elem,
            source_pattern,
        )
        ordered = pl.pallas_call(
            functools.partial(kernel, groups, writers, steps, nodes_el),
            out_shape=pltpu.VMEM((6, steps, point_count), BF16),
            in_specs=[hbm] * (len(sharded) + 2),
            out_specs=vmem,
            scratch_shapes=[pltpu.VMEM(a.shape, a.dtype) for a in sharded] * 2
            + [pltpu.VMEM(shape_grad.shape[::-1], F32), pltpu.SMEM(wavelet.shape, F32)]
            + [pltpu.SemaphoreType.DMA((len(sharded) + 2,))] * 3
            + [
                pltpu.VMEM((nodes_el // 2 * LANES, 2 * LANES), F8),
                pltpu.VMEM((nodes_el // 2 * LANES, 2 * LANES), BF16),
                pltpu.VMEM((nodes_el // 2 * (source_pattern.shape[1] // LANES) * 16, LANES), BF16),
                pltpu.VMEM((3, padded, LANES), F32),
                pltpu.VMEM((nodes_el // 2, 18 * padded, LANES), BF16),
                pltpu.VMEM((LANES, LANES), BF16),
                pltpu.VMEM((nodes_el // 2, 24 * padded, LANES), F32),
                pltpu.VMEM((3 * padded, LANES), F32),
                pltpu.VMEM((3 * points, 96), BF16),
                pltpu.VMEM((8 * points, LANES), F32),
                pltpu.VMEM((points * LANES, LANES), BF16),
                pltpu.VMEM((2 * points, LANES), jnp.int32),
                pltpu.VMEM((points, 16, LANES), F32),
                pltpu.VMEM((steps // 2, 16, point_count), BF16),
                pltpu.VMEM((steps // 2, 16, point_count), BF16),
                pltpu.VMEM((2, 8, LANES), F32),
                pltpu.VMEM((2, 4, 8, LANES), F32),
                pltpu.SemaphoreType.DMA((2, 4)),
                pltpu.SemaphoreType.DMA((2, 4)),
                pltpu.SemaphoreType.DMA((steps // 2, writers)),
                pltpu.SemaphoreType.DMA((steps // 2, writers)),
            ],
            compiler_params=pltpu.CompilerParams(
                collective_id=0, has_side_effects=True, vmem_limit_bytes=56 * 1024 * 1024
            ),
            name="window",
        )(
            *sharded,
            shape_grad.T,
            wavelet,
        )
        return ordered.transpose(1, 0, 2)

    placed = (
        P(None, ("grp", "dom")),
        P(("grp", "dom"), None, None),
        P(("grp", "dom"), None),
        P(("grp", "dom"), None),
        P(),
        P(None, ("grp", "dom")),
        P(None, ("grp", "dom")),
        P(None, ("grp", "dom")),
        P(None, ("grp", "dom")),
        P(None, ("grp", "dom")),
        P(),
    )
    return jax.shard_map(
        shards, mesh=mesh, in_specs=placed, out_specs=P(None, None, ("grp", "dom")), check_vma=False
    )
```
